32 devices in a mesh: seq: 8 (over z, x), fsdp: 4 (over y, core).
Axes of the slice: x: 2, y: 2, z: 4, core: 2. Of those that a mesh axis runs over, the one named last changes fastest.
Arguments:
- block_input: bfloat16 [2, 4, 6144, 512], P(None, 'fsdp', 'seq'), may hold values from -6 to 6
- seq_ids: int32 [2, 4, 6144], P(None, 'fsdp', 'seq'), may hold values from 0 to 1, as said below
- random_features: bfloat16 [8, 64, 256], replicated, may hold values from -5 to 5
- ln1_gain: bfloat16 [512], P('fsdp'), may hold values from 0.099609375 to 1.8984375
- w_query: bfloat16 [512, 512], P('fsdp'), may hold values from -0.25 to 0.25
- w_key: bfloat16 [512, 512], P('fsdp'), may hold values from -0.25 to 0.25
- w_value: bfloat16 [512, 512], P('fsdp'), may hold values from -0.25 to 0.25
- w_out: bfloat16 [512, 512], P('fsdp'), may hold values from -1 to 1
- ln2_gain: bfloat16 [512], P('fsdp'), may hold values from 0.099609375 to 1.8984375
- w_up: bfloat16 [512, 2048], P('fsdp'), may hold values from -0.25 to 0.25
- w_down: bfloat16 [2048, 512], P('fsdp'), may hold values from -0.125 to 0.125
- cotangent: bfloat16 [2, 4, 6144, 512], P(None, 'fsdp', 'seq'), may hold values from -6 to 6
Outputs:
- block_output: bfloat16 [2, 4, 6144, 512], P(None, 'fsdp', 'seq')
- input_grad: bfloat16 [2, 4, 6144, 512], P(None, 'fsdp', 'seq')
- ln1_gain_grad: float32 [512], P('fsdp')
- w_query_grad: float32 [512, 512], P('fsdp')
- w_key_grad: float32 [512, 512], P('fsdp')
- w_value_grad: float32 [512, 512], P('fsdp')
- w_out_grad: float32 [512, 512], P('fsdp')
- ln2_gain_grad: float32 [512], P('fsdp')
- w_up_grad: float32 [512, 2048], P('fsdp')
- w_down_grad: float32 [2048, 512], P('fsdp')
The draws below stay inside these ranges and needn't reach their ends.
Inputs may be any that keep to these rules, and one draw needn't show every extreme that they name: `seq_ids`: along each group's tokens the ids never fall; each of the 2 sequences of a group holds 1536 tokens or more.
All inputs are finite; a program needn't handle non-finite values.
Results may differ from the reference program's by a relative error of at most 0.035.
Values may be sent and summed in bfloat16 or wider, within the bound.
A program may use at most 256 MiB of HBM per device.

```python
import jax
import jax.numpy as jnp
from jax import lax

D = 512
HEADS = 8
HEAD_DIM = 64
FEATS = 256
FF = 2048
MB = 2
SEQS = 2
GTOK = 6144
GROUPS = 4


def draw_seq_ids(key, part):
    least_tokens = GTOK // (2 * SEQS)
    spare_tokens = GTOK - SEQS * least_tokens
    cut_points = jax.random.randint(key, (MB, GROUPS, SEQS - 1), 0, spare_tokens + 1)
    cut_points = jnp.sort(cut_points, axis=-1)
    start_points = jnp.arange(1, SEQS, dtype=jnp.int32) * least_tokens
    boundaries = start_points[None, None, :] + cut_points
    positions = jnp.arange(GTOK, dtype=jnp.int32)
    passed = (positions[None, None, :, None] >= boundaries[:, :, None, :]).astype(jnp.int32)
    return jnp.sum(passed, axis=-1).astype(jnp.int32)


def level_of(key, extent, cuts, low, largest):
    loudness, own = 1.0, jax.random.fold_in(key, 6)
    for dim, blocks in cuts:
        heights = jnp.exp(jax.random.uniform(jax.random.fold_in(own, dim), (blocks,), jnp.float32, low / len(cuts), largest / len(cuts)))
        loudness = loudness * jnp.repeat(heights, extent[dim] // blocks).reshape([-1 if axis == dim else 1 for axis in range(len(extent))])
    return loudness


def normal_values(key, dims, width, most, cuts=(), kind=jnp.bfloat16):
    values = width * jax.random.normal(key, dims, jnp.float32)
    if cuts:
        values = values * level_of(key, dims, cuts, -0.22, 0.18)
    return jnp.clip(values, -most, most).astype(kind)


def setup_inputs(seed: int = 0) -> dict:
    arg_keys = jax.random.split(jax.random.key(seed), 13)
    block_input = normal_values(arg_keys[0], (MB, GROUPS, GTOK, D), 1.0, 6.0, ((1, 4), (2, 8)))
    seq_ids = draw_seq_ids(jax.random.fold_in(arg_keys[12], 71), 0)
    random_features = normal_values(arg_keys[2], (HEADS, HEAD_DIM, FEATS), 1.0, 5.0)
    ln1_gain = jnp.clip(1.0 + 0.18 * jax.random.normal(arg_keys[3], (D,), jnp.float32), 0.099609375, 1.8984375).astype(jnp.bfloat16)
    w_query = normal_values(arg_keys[4], (D, D), D ** -0.5, 0.25, ((0, 4),))
    w_key = normal_values(arg_keys[5], (D, D), D ** -0.5, 0.25, ((0, 4),))
    w_value = normal_values(arg_keys[6], (D, D), D ** -0.5, 0.25, ((0, 4),))
    w_out = normal_values(arg_keys[7], (D, D), (D // 16) ** -0.5, 1.0, ((0, 4),))
    ln2_gain = jnp.clip(1.0 + 0.18 * jax.random.normal(arg_keys[8], (D,), jnp.float32), 0.099609375, 1.8984375).astype(jnp.bfloat16)
    w_up = normal_values(arg_keys[9], (D, FF), D ** -0.5, 0.25, ((0, 4),))
    w_down = normal_values(arg_keys[10], (FF, D), FF ** -0.5, 0.125, ((0, 4),))
    cotangent = normal_values(arg_keys[11], (MB, GROUPS, GTOK, D), 1.0, 6.0, ((1, 4), (2, 8)))
    return dict(block_input=block_input, seq_ids=seq_ids, random_features=random_features, ln1_gain=ln1_gain, w_query=w_query, w_key=w_key, w_value=w_value, w_out=w_out, ln2_gain=ln2_gain, w_up=w_up, w_down=w_down, cotangent=cotangent)


@jax.custom_vjp
def low(v):
    return lax.optimization_barrier(v.astype(jnp.bfloat16)).astype(jnp.float32)

@jax.custom_vjp
def low_back(v):
    return v

def low_keep(v):
    return (low(v), None)

def low_pass(kept, grad):
    return (grad,)

def back_keep(v):
    return (v, None)

def back_low(kept, grad):
    return (low(grad),)
low.defvjp(low_keep, low_pass)
low_back.defvjp(back_keep, back_low)
NORM_EPS = 1e-05
TOP_PRECISION = lax.Precision.HIGHEST

def layer_norm(values, gain):
    center = values - lax.optimization_barrier(jnp.mean(values, axis=-1, keepdims=True))
    spread = lax.optimization_barrier(jnp.mean(center * center, axis=-1, keepdims=True))
    return center * lax.rsqrt(spread + NORM_EPS) * gain

def gelu_exact(values):
    return 0.5 * values * (1.0 + jax.scipy.special.erf(values * 0.7071067811865476))

def feature_map(scaled, rand_feats):
    inner = low_back(jnp.einsum('thd,hdm->thm', scaled, rand_feats, precision=TOP_PRECISION))
    square = 0.5 * lax.optimization_barrier(jnp.sum(scaled * scaled, axis=-1, keepdims=True))
    return low(jnp.exp(inner - square) * FEATS ** (-0.5))

def attend_all(ids, feature_query, feature_keys, value_reduced):

    def seq_step(carry, seq_index):
        numerator, denom = carry
        token_mask = (ids == seq_index).astype(jnp.float32)
        keys_after_mask = feature_keys * token_mask[:, None, None]
        key_value_summary = jnp.einsum('lsu,lsa->sua', keys_after_mask, value_reduced, precision=TOP_PRECISION)
        key_total = lax.optimization_barrier(jnp.sum(keys_after_mask, axis=0))
        numerator = numerator + token_mask[:, None, None] * jnp.einsum('avj,vjb->avb', feature_query, key_value_summary, precision=TOP_PRECISION)
        denom = denom + token_mask[:, None] * jnp.einsum('thm,hm->th', feature_query, key_total, precision=TOP_PRECISION)
        return ((numerator, denom), None)
    start = (jnp.zeros((GTOK, HEADS, HEAD_DIM), jnp.float32), jnp.zeros((GTOK, HEADS), jnp.float32))
    (numerator, denom), unused = lax.scan(jax.checkpoint(seq_step), start, jnp.arange(SEQS, dtype=jnp.int32))
    return (numerator, denom)

def one_group(tokens, ids, rand_feats, gain_one, w_query, w_key, w_value, w_out, gain_two, w_up, w_down):
    normed_in = low(layer_norm(tokens, gain_one))
    queries = low_back(jnp.dot(normed_in, w_query, precision=TOP_PRECISION))
    key_rows = low_back(jnp.dot(normed_in, w_key, precision=TOP_PRECISION))
    value_rows = low_back(jnp.dot(normed_in, w_value, precision=TOP_PRECISION))
    factor = HEAD_DIM ** (-0.25)
    scaled_query = low(queries * factor).reshape(GTOK, HEADS, HEAD_DIM)
    scaled_keys = low(key_rows * factor).reshape(GTOK, HEADS, HEAD_DIM)
    value_reduced = low(value_rows).reshape(GTOK, HEADS, HEAD_DIM)
    feature_query = feature_map(scaled_query, rand_feats)
    feature_keys = feature_map(scaled_keys, rand_feats)
    numerator, denom = attend_all(ids, feature_query, feature_keys, value_reduced)
    attended = low((numerator / denom[:, :, None]).reshape(GTOK, D))
    mixed = tokens + low_back(jnp.dot(attended, w_out, precision=TOP_PRECISION))
    normed_mid = low(layer_norm(mixed, gain_two))
    hidden_pre = low_back(jnp.dot(normed_mid, w_up, precision=TOP_PRECISION))
    hidden = low(gelu_exact(hidden_pre))
    branch = low_back(jnp.dot(hidden, w_down, precision=TOP_PRECISION))
    return mixed + branch

def reference(block_input, seq_ids, random_features, ln1_gain, w_query, w_key, w_value, w_out, ln2_gain, w_up, w_down, cotangent):
    tokens_all = block_input.astype(jnp.float32).reshape(MB * GROUPS, GTOK, D)
    ids_all = seq_ids.reshape(MB * GROUPS, GTOK).astype(jnp.int32)
    rand_feats = random_features.astype(jnp.float32)
    weights = (ln1_gain.astype(jnp.float32), w_query.astype(jnp.float32), w_key.astype(jnp.float32), w_value.astype(jnp.float32), w_out.astype(jnp.float32), ln2_gain.astype(jnp.float32), w_up.astype(jnp.float32), w_down.astype(jnp.float32))

    def forward(tokens, gain_one, wq_full, wk_full, wv_full, wo_full, gain_two, wu_full, wd_full):

        def group(item):
            return jax.checkpoint(one_group)(item[0], item[1], rand_feats, gain_one, wq_full, wk_full, wv_full, wo_full, gain_two, wu_full, wd_full)
        return lax.map(group, (tokens, ids_all))
    output, pullback = jax.vjp(forward, tokens_all, *weights)
    grads = pullback(cotangent.astype(jnp.float32).reshape(MB * GROUPS, GTOK, D))
    return (output.reshape(MB, GROUPS, GTOK, D).astype(jnp.bfloat16), grads[0].reshape(MB, GROUPS, GTOK, D).astype(jnp.bfloat16), grads[1], grads[2], grads[3], grads[4], grads[5], grads[6], grads[7], grads[8])
```

```python
import functools
import math

import jax
import jax.numpy as jnp
from jax import lax
from jax.experimental import pallas as pl
from jax.experimental.pallas import tpu as pltpu
from jax.sharding import PartitionSpec as P

EPS = 1e-05
TILE = 256
F32 = jnp.float32
BF16 = jnp.bfloat16
PAD = 16


def dot(a, b):
    return lax.dot_general(a, b, (((1,), (0,)), ((), ())), preferred_element_type=F32)


def dot_nt(a, b):
    return lax.dot_general(a, b, (((1,), (1,)), ((), ())), preferred_element_type=F32)


def norm_parts(v):
    c = v - jnp.mean(v, axis=-1, keepdims=True)
    r = lax.rsqrt(jnp.mean(c * c, axis=-1, keepdims=True) + EPS)
    return c * r, r


def norm_back(grad, normed, rescale, gain):
    e = grad * gain
    return rescale * (
        e
        - jnp.mean(e, axis=-1, keepdims=True)
        - normed * jnp.mean(e * normed, axis=-1, keepdims=True)
    )


def features(scaled, rbd_ref, feat_ref, feats):
    lane = lax.broadcasted_iota(jnp.int32, (scaled.shape[0], 128), 1)
    low = lane < 64
    log_scale = 0.5 * math.log(feats)
    as_float = scaled.astype(F32)
    for quad in range(scaled.shape[1] // 256):
        u = dot(scaled[:, 256 * quad : 256 * quad + 256], rbd_ref[quad])
        for pair in range(2):
            s = as_float[:, 256 * quad + 128 * pair : 256 * quad + 128 * pair + 128]
            s = s * s
            sq_a = jnp.sum(jnp.where(low, s, 0.0), axis=-1, keepdims=True)
            sq_b = jnp.sum(jnp.where(low, 0.0, s), axis=-1, keepdims=True)
            for k, sq in enumerate((sq_a, sq_b)):
                col = feats * (2 * pair + k)
                f = jnp.exp(u[:, col : col + feats] - (0.5 * sq + log_scale))
                base = feats * (4 * quad + 2 * pair + k)
                feat_ref[:, base : base + feats] = f.astype(BF16)


def summary_rows(rows, zrow, mask_t):
    z = mask_t if zrow is None else (mask_t.astype(F32) * zrow).astype(BF16)
    return jnp.concatenate([rows * mask_t[0:1], rows * mask_t[1:2], z], axis=0)


def key_kernel(x_ref, g_ref, wk_ref, wv_ref, rbd_ref, mt_ref, *refs, feats, factor, n_alias):
    a1_ref, ks_ref, vv_ref, fk_ref, p_ref, acc = refs[n_alias:]
    step = pl.program_id(0)

    @pl.when(step == 0)
    def _():
        acc[...] = jnp.zeros_like(acc)

    normed, _ = norm_parts(x_ref[...].astype(F32))
    a1 = (normed * g_ref[...].astype(F32)).astype(BF16)
    a1_ref[...] = a1
    ks = (dot(a1, wk_ref[...]) * factor).astype(BF16)
    ks_ref[...] = ks
    vv = dot(a1, wv_ref[...]).astype(BF16)
    vv_ref[...] = vv
    features(ks, rbd_ref, fk_ref, feats)
    vt = vv.T
    mask_t = mt_ref[...]
    for h in range(vv.shape[1] // 64):
        lt = summary_rows(vt[64 * h : 64 * h + 64], None, mask_t)
        acc[h] += dot(lt, fk_ref[:, feats * h : feats * h + feats])

    @pl.when(step == pl.num_programs(0) - 1)
    def _():
        p_ref[...] = acc[...].astype(BF16)


def query_kernel(a1_ref, wq_ref, rbd_ref, qs_ref, fq_ref, *, feats, factor):
    qs = (dot(a1_ref[...], wq_ref[...]) * factor).astype(BF16)
    qs_ref[...] = qs
    features(qs, rbd_ref, fq_ref, feats)


def mid_kernel(
    x_ref, dy_ref, fq_ref, qs_ref, last_ref, mt_ref, b_ref, wo_ref, g2_ref, wu_ref, wd_ref, rt_ref,
    *refs, feats, factor, n_alias,
):
    out_ref, att_ref, a2_ref, hid_ref, dpre_ref, dmid_ref, dq_ref, p_ref, gg_ref, acc = refs[n_alias:]
    step = pl.program_id(0)

    @pl.when(step == 0)
    def _():
        acc[...] = jnp.zeros_like(acc)
        gg_ref[...] = jnp.zeros_like(gg_ref)

    rows = x_ref.shape[0]
    pairs = x_ref.shape[1] // 128
    last = last_ref[...].astype(F32) > 0.5
    lane = lax.broadcasted_iota(jnp.int32, (rows, 128), 1)
    sel = jnp.logical_xor(lane < 64, last)

    def swap(v):
        return jnp.where(last, pltpu.roll(v, 64, 1), v)

    att_parts, inv_parts = [], []
    for p in range(pairs):
        base = 2 * feats * p
        a = dot_nt(fq_ref[:, base : base + feats], b_ref[2 * p])
        b = dot_nt(fq_ref[:, base + feats : base + 2 * feats], b_ref[2 * p + 1])
        num = jnp.where(sel, a[:, :128], b[:, :128])
        den = jnp.where(sel, a[:, 128:], b[:, 128:])
        inv = 1.0 / den
        att_parts.append(swap(num * inv))
        inv_parts.append(swap(inv))
    att = jnp.concatenate(att_parts, axis=1)
    inv = jnp.concatenate(inv_parts, axis=1)
    att_low = att.astype(BF16)
    att_ref[...] = att_low
    mixed = x_ref[...].astype(F32) + dot(att_low, wo_ref[...])
    normed, rescale = norm_parts(mixed)
    g2 = g2_ref[...].astype(F32)
    a2 = (normed * g2).astype(BF16)
    a2_ref[...] = a2
    dy = dy_ref[...]
    for j in range(wu_ref.shape[1] // 256):
        js = slice(256 * j, 256 * j + 256)
        pre = dot(a2, wu_ref[:, js])
        dh = dot_nt(dy, wd_ref[js, :])
        cdf = 0.5 * (1.0 + lax.erf(pre * 0.7071067811865476))
        slope = cdf + pre * jnp.exp(-0.5 * pre * pre) * 0.3989422804014327
        hid_ref[:, js] = (pre * cdf).astype(BF16)
        dpre_ref[:, js] = (dh * slope).astype(BF16)
    out_ref[...] = (mixed + dot(hid_ref[...], wd_ref[...])).astype(BF16)
    da2 = dot_nt(dpre_ref[...], wu_ref[...])
    gg_ref[...] += jnp.sum(da2 * normed, axis=0, keepdims=True)
    dmid = dy.astype(F32) + norm_back(da2, normed, rescale, g2)
    dmid_low = dmid.astype(BF16)
    dmid_ref[...] = dmid_low
    dnum = dot_nt(dmid_low, wo_ref[...]) * inv
    dpart = -dnum * att
    mask_t = mt_ref[...]
    for p in range(pairs):
        ps = slice(128 * p, 128 * p + 128)
        d, q = dnum[:, ps], dpart[:, ps]
        ds, qs = swap(d), swap(q)
        la = jnp.concatenate([jnp.where(sel, ds, 0.0), jnp.where(sel, qs, 0.0)], axis=1).astype(BF16)
        lb = jnp.concatenate([jnp.where(sel, 0.0, ds), jnp.where(sel, 0.0, qs)], axis=1).astype(BF16)
        base = 2 * feats * p
        fa = fq_ref[:, base : base + feats]
        fb = fq_ref[:, base + feats : base + 2 * feats]
        ga = (dot(la, b_ref[2 * p]) * fa.astype(F32)).astype(BF16)
        gb = (dot(lb, b_ref[2 * p + 1]) * fb.astype(F32)).astype(BF16)
        o = dot(jnp.concatenate([ga, gb], axis=1), rt_ref[p])
        dq_ref[:, ps] = (factor * (o[:, :128] - qs_ref[:, ps].astype(F32) * o[:, 128:])).astype(BF16)
        dt = d.astype(BF16).T
        qt = q.T
        for k, f in enumerate((fa, fb)):
            z = jnp.sum(qt[64 * k : 64 * k + 64], axis=0, keepdims=True)
            lt = summary_rows(dt[64 * k : 64 * k + 64], z, mask_t)
            acc[2 * p + k] += dot(lt, f)

    @pl.when(step == pl.num_programs(0) - 1)
    def _():
        p_ref[...] = acc[...].astype(BF16)


def second_kernel(
    x_ref, dmid_ref, fk_ref, ks_ref, vv_ref, last_ref, dq_ref, b_ref, g1_ref, wq_ref, wk_ref, wv_ref, rt_ref,
    *refs, feats, factor, n_alias,
):
    dx_ref, dk_ref, dv_ref, gg_ref = refs[n_alias:]
    step = pl.program_id(0)

    @pl.when(step == 0)
    def _():
        gg_ref[...] = jnp.zeros_like(gg_ref)

    rows = x_ref.shape[0]
    pairs = x_ref.shape[1] // 128
    last = last_ref[...].astype(F32) > 0.5
    lane = lax.broadcasted_iota(jnp.int32, (rows, 128), 1)
    sel = jnp.logical_xor(lane < 64, last)
    ones_a = jnp.where(sel, 1.0, 0.0).astype(BF16)
    ones_b = jnp.where(sel, 0.0, 1.0).astype(BF16)

    def swap(v):
        return jnp.where(last, pltpu.roll(v, 64, 1), v)

    for p in range(pairs):
        ps = slice(128 * p, 128 * p + 128)
        v = swap(vv_ref[:, ps].astype(F32))
        la = jnp.concatenate([jnp.where(sel, v, 0.0).astype(BF16), ones_a], axis=1)
        lb = jnp.concatenate([jnp.where(sel, 0.0, v).astype(BF16), ones_b], axis=1)
        base = 2 * feats * p
        fa = fk_ref[:, base : base + feats]
        fb = fk_ref[:, base + feats : base + 2 * feats]
        ga = (dot(la, b_ref[2 * p]) * fa.astype(F32)).astype(BF16)
        gb = (dot(lb, b_ref[2 * p + 1]) * fb.astype(F32)).astype(BF16)
        o = dot(jnp.concatenate([ga, gb], axis=1), rt_ref[p])
        dk_ref[:, ps] = (factor * (o[:, :128] - ks_ref[:, ps].astype(F32) * o[:, 128:])).astype(BF16)
        va = dot_nt(fa, b_ref[2 * p, :128])
        vb = dot_nt(fb, b_ref[2 * p + 1, :128])
        dv_ref[:, ps] = swap(jnp.where(sel, va, vb)).astype(BF16)
    da1 = dot_nt(dq_ref[...], wq_ref[...]) + dot_nt(dk_ref[...], wk_ref[...]) + dot_nt(dv_ref[...], wv_ref[...])
    normed, rescale = norm_parts(x_ref[...].astype(F32))
    gg_ref[...] += jnp.sum(da1 * normed, axis=0, keepdims=True)
    grad = norm_back(da1, normed, rescale, g1_ref[...].astype(F32))
    dx_ref[...] = (dmid_ref[...].astype(F32) + grad).astype(BF16)


def tile_spec(cols, off):
    return pl.BlockSpec((TILE, cols), lambda i: (i + off, 0))


def whole_spec(shape):
    zeros = (0,) * len(shape)
    return pl.BlockSpec(shape, lambda i: zeros, pipeline_mode=pl.Buffered(1))


def anyspec():
    return pl.BlockSpec(memory_space=pl.ANY)


def call(body, mb, tiles, tiled, wholes, mask_t, outs_tiled, outs_whole, scratch, previous, flops, name, **static):
    off = mb * tiles
    total = tiled[0].shape[0]
    in_specs = [tile_spec(a.shape[1], off) for a in tiled]
    args = list(tiled)
    for item in wholes:
        if item is mask_t:
            in_specs.append(pl.BlockSpec((PAD, TILE), lambda i: (0, i + off)))
        else:
            in_specs.append(whole_spec(item.shape))
        args.append(item)
    out_shape = [jax.ShapeDtypeStruct((total, c), BF16) for c in outs_tiled]
    out_specs = [tile_spec(c, off) for c in outs_tiled]
    for shape, dtype in outs_whole:
        out_shape.append(jax.ShapeDtypeStruct(shape, dtype))
        out_specs.append(pl.BlockSpec(shape, functools.partial(lambda n, i: (0,) * n, len(shape))))
    alias = {}
    if previous is not None:
        for k, a in enumerate(previous):
            alias[len(args)] = k
            args.append(a)
            in_specs.append(anyspec())
    n_alias = 0 if previous is None else len(previous)
    return pl.pallas_call(
        functools.partial(body, n_alias=n_alias, **static),
        grid=(tiles,),
        in_specs=in_specs,
        out_specs=out_specs,
        out_shape=out_shape,
        scratch_shapes=scratch,
        input_output_aliases=alias,
        compiler_params=pltpu.CompilerParams(dimension_semantics=("arbitrary",)),
        cost_estimate=pl.CostEstimate(flops=int(flops), bytes_accessed=1 << 20, transcendentals=0),
        name=name,
    )(*args)


def block_diag_features(rand):
    heads, dim, feats = rand.shape
    eye = jnp.eye(4, dtype=rand.dtype)
    quads = rand.reshape(heads // 4, 4, dim, feats)
    return jnp.einsum("qadf,ab->qadbf", quads, eye).reshape(heads // 4, 4 * dim, 4 * feats)


def back_features(rand):
    heads, dim, feats = rand.shape
    eye = jnp.eye(2, dtype=rand.dtype)
    pairs = rand.reshape(heads // 2, 2, dim, feats)
    left = jnp.einsum("padf,ab->pafbd", pairs, eye).reshape(heads // 2, 2 * feats, 2 * dim)
    right = jnp.broadcast_to(eye[None, :, None, :, None], (heads // 2, 2, feats, 2, dim))
    return jnp.concatenate([left, right.reshape(left.shape).astype(left.dtype)], axis=2)


def expand(pick, repeat):
    heads, _, feats = pick.shape
    first, second = pick[:, :64], pick[:, 64:128]
    z1, z2 = pick[:, 128:129], pick[:, 129:130]
    if repeat:
        z1, z2 = (jnp.broadcast_to(z, (heads, 64, feats)) for z in (z1, z2))
    else:
        z1, z2 = (jnp.pad(z, ((0, 0), (0, 63), (0, 0))) for z in (z1, z2))
    even = jnp.concatenate([first, second, z1, z2], axis=1)
    odd = jnp.concatenate([second, first, z2, z1], axis=1)
    parity = (jnp.arange(heads) % 2 == 0)[:, None, None]
    return jnp.where(parity, even, odd)


def place(local, ids, seqs):
    if seqs == 2:
        return local[:, None]
    slots = jnp.arange(seqs, dtype=jnp.int32)
    first = (slots == ids[0]).astype(BF16).reshape(1, seqs // 2, 2, 1, 1)
    last = (slots == ids[-1]).astype(BF16).reshape(1, seqs // 2, 2, 1, 1)
    heads, _, feats = local.shape
    rows = local[:, :128].reshape(heads, 1, 2, 64, feats)
    z = local[:, 128:130].reshape(heads, 1, 2, 1, feats)

    def put(v):
        return first * v[:, :, 0:1] + last * v[:, :, 1:2]

    body = put(rows).reshape(heads, seqs // 2, 128, feats)
    tail = jnp.pad(put(z).reshape(heads, seqs // 2, 2, feats), ((0, 0), (0, 0), (0, PAD - 2), (0, 0)))
    return jnp.concatenate([body, tail], axis=2)


def pick_two(dense, ids, seqs):
    if seqs == 2:
        return dense[:, 0]
    heads, _, _, feats = dense.shape
    rows = dense[:, :, :128].reshape(heads, seqs, 64, feats)
    z = dense[:, :, 128:130].reshape(heads, seqs, 1, feats)

    def get(k):
        return (lax.dynamic_index_in_dim(rows, k, 1, False), lax.dynamic_index_in_dim(z, k, 1, False))

    r1, z1 = get(ids[0])
    r2, z2 = get(ids[-1])
    return jnp.pad(jnp.concatenate([r1, r2, z1, z2], axis=1), ((0, 0), (0, PAD - 2), (0, 0)))


def sum_seq(dense):
    return lax.psum(dense, "seq")


def gather(w):
    return lax.all_gather(w, "fsdp", axis=0, tiled=True)


def per_device(block_input, seq_ids, rand, ln1_gain, w_query, w_key, w_value, w_out, ln2_gain, w_up, w_down, cotangent):
    micro, _, toks, width = block_input.shape
    heads, dim, feats = rand.shape
    hidden = w_up.shape[1]
    factor = dim ** (-0.25)
    seqs = max(1, lax.axis_size("seq") // 4)
    tiles = toks // TILE
    x = block_input.reshape(micro * toks, width)
    dy = cotangent.reshape(micro * toks, width)
    ids = seq_ids.reshape(micro, toks)
    last = (ids == (1 if seqs == 2 else ids[:, -1:])).reshape(-1)
    last_cols = jnp.broadcast_to(last.astype(BF16)[:, None], (micro * toks, 128))
    row = jnp.arange(PAD)[:, None]
    mask_t = jnp.where(row == 0, 1.0 - last.astype(F32), jnp.where(row == 1, last.astype(F32), 0.0)).astype(BF16)
    rbd = block_diag_features(rand)
    rt = back_features(rand)
    g1 = gather(ln1_gain).reshape(1, width)
    g2 = gather(ln2_gain).reshape(1, width)
    wq, wk, wv, wo, wu, wd = (gather(w) for w in (w_query, w_key, w_value, w_out, w_up, w_down))
    static = dict(feats=feats, factor=factor)
    rows = 128 + PAD
    summary = ((heads, rows, feats), BF16)
    acc = pltpu.VMEM((heads, rows, feats), F32)
    unit = 2.0 * toks * 256 * 256

    keep, sums = None, []
    for mb in range(micro):
        r = call(key_kernel, mb, tiles, [x], [g1, wk, wv, rbd, mask_t], mask_t,
                 [width, width, width, heads * feats], [summary], [acc], keep, 24 * unit, "keys", **static)
        keep = r[:4]
        sums.append(pick_two(sum_seq(place(r[4], ids[mb], seqs)), ids[mb], seqs))
    a1, ks, vv, fk = keep
    total = micro * toks
    qs, fq = pl.pallas_call(
        functools.partial(query_kernel, **static),
        grid=(micro * tiles,),
        in_specs=[tile_spec(width, 0), whole_spec(wq.shape), whole_spec(rbd.shape)],
        out_specs=[tile_spec(width, 0), tile_spec(heads * feats, 0)],
        out_shape=[jax.ShapeDtypeStruct((total, width), BF16), jax.ShapeDtypeStruct((total, heads * feats), BF16)],
        cost_estimate=pl.CostEstimate(flops=int(24 * unit), bytes_accessed=1 << 20, transcendentals=0),
        name="queries",
    )(a1, wq, rbd)
    keep, grads = None, []
    g2_grad = 0.0
    for mb in range(micro):
        b = expand(sums[mb], True)
        r = call(mid_kernel, mb, tiles, [x, dy, fq, qs, last_cols], [mask_t, b, wo, g2, wu, wd, rt], mask_t,
                 [width, width, width, hidden, hidden, width, width], [summary, ((1, width), F32)], [acc],
                 keep, 100 * unit, "mid", **static)
        keep = r[:7]
        g2_grad = g2_grad + r[8]
        grads.append(pick_two(sum_seq(place(r[7], ids[mb], seqs)), ids[mb], seqs))
    out, att, a2, hid, dpre, dmid, dq = keep
    keep = None
    g1_grad = 0.0
    for mb in range(micro):
        b = expand(grads[mb], False)
        r = call(second_kernel, mb, tiles, [x, dmid, fk, ks, vv, last_cols, dq], [b, g1, wq, wk, wv, rt], mask_t,
                 [width, width, width], [((1, width), F32)], [], keep, 44 * unit, "second", **static)
        keep = r[:3]
        g1_grad = g1_grad + r[3]
    dx, dk, dv = keep

    def weight_grad(left, right):
        return lax.dot_general(left, right, (((0,), (0,)), ((), ())), preferred_element_type=F32).astype(BF16)

    totals = (
        g1_grad.reshape(-1).astype(BF16),
        weight_grad(a1, dq),
        weight_grad(a1, dk),
        weight_grad(a1, dv),
        weight_grad(att, dmid),
        g2_grad.reshape(-1).astype(BF16),
        weight_grad(a2, dpre),
        weight_grad(hid, dy),
    )
    totals = [lax.psum_scatter(t, "fsdp", scatter_dimension=0, tiled=True) for t in totals]
    totals = [lax.psum(t, "seq").astype(F32) for t in totals]
    shape = block_input.shape
    return (out.reshape(shape), dx.reshape(shape), *totals)


def solution(mesh):
    tok = P(None, "fsdp", "seq", None)
    vec, mat = P("fsdp"), P("fsdp", None)
    return jax.shard_map(
        per_device,
        mesh=mesh,
        in_specs=(tok, P(None, "fsdp", "seq"), P(), vec, mat, mat, mat, mat, vec, mat, mat, tok),
        out_specs=(tok, tok, vec, mat, mat, mat, mat, vec, mat, mat),
        check_vma=False,
    )
```

```python
import functools
import math

import jax
import jax.numpy as jnp
from jax import lax
from jax.experimental import pallas as pl
from jax.experimental.pallas import tpu as pltpu
from jax.sharding import PartitionSpec as P

EPS = 1e-05
TILE = 256
F32 = jnp.float32
BF16 = jnp.bfloat16
PAD = 16


def dot(a, b):
    return lax.dot_general(a, b, (((1,), (0,)), ((), ())), preferred_element_type=F32)


def dot_nt(a, b):
    return lax.dot_general(a, b, (((1,), (1,)), ((), ())), preferred_element_type=F32)


def norm_parts(v):
    c = v - jnp.mean(v, axis=-1, keepdims=True)
    r = lax.rsqrt(jnp.mean(c * c, axis=-1, keepdims=True) + EPS)
    return c * r, r


def norm_back(grad, normed, rescale, gain):
    e = grad * gain
    return rescale * (
        e
        - jnp.mean(e, axis=-1, keepdims=True)
        - normed * jnp.mean(e * normed, axis=-1, keepdims=True)
    )


def features(scaled, rbd_ref, feat_ref, feats):
    lane = lax.broadcasted_iota(jnp.int32, (scaled.shape[0], 128), 1)
    low = lane < 64
    log_scale = 0.5 * math.log(feats)
    as_float = scaled.astype(F32)
    for quad in range(scaled.shape[1] // 256):
        u = dot(scaled[:, 256 * quad : 256 * quad + 256], rbd_ref[quad])
        for pair in range(2):
            s = as_float[:, 256 * quad + 128 * pair : 256 * quad + 128 * pair + 128]
            s = s * s
            sq_a = jnp.sum(jnp.where(low, s, 0.0), axis=-1, keepdims=True)
            sq_b = jnp.sum(jnp.where(low, 0.0, s), axis=-1, keepdims=True)
            for k, sq in enumerate((sq_a, sq_b)):
                col = feats * (2 * pair + k)
                f = jnp.exp(u[:, col : col + feats] - (0.5 * sq + log_scale))
                base = feats * (4 * quad + 2 * pair + k)
                feat_ref[:, base : base + feats] = f.astype(BF16)


def summary_rows(rows, zrow, mask_t):
    z = mask_t if zrow is None else (mask_t.astype(F32) * zrow).astype(BF16)
    return jnp.concatenate([rows * mask_t[0:1], rows * mask_t[1:2], z], axis=0)


MESH_ID = pl.DeviceIdType.MESH


def rows_at(index, size):
    return pl.ds(pl.multiple_of(index * size, size), size)


class Exchange:
    def __init__(self):
        self.s, self.f = lax.axis_index("seq"), lax.axis_index("fsdp")
        self.ns, self.nf = lax.axis_size("seq"), lax.axis_size("fsdp")
        self.ny = self.nf // 2
        self.y, self.c = self.f // 2, self.f % 2
        self.partner = self.y * 2 + (1 - self.c)
        self.pending = []

    def seq_peer(self, k):
        return ((self.s + k) % self.ns, self.f)

    def y_from(self, k):
        return ((self.y + self.ny - k) % self.ny) * 2 + self.c

    def y_to(self, k):
        return ((self.y + k) % self.ny) * 2 + self.c

    def barrier(self):
        sem = pltpu.get_barrier_semaphore()
        peers = [self.seq_peer(k) for k in range(1, self.ns)]
        peers += [(self.s, self.partner)] + [(self.s, self.y_to(k)) for k in range(1, self.ny)]
        for peer in peers:
            pl.semaphore_signal(sem, inc=1, device_id=peer, device_id_type=MESH_ID)
        pl.semaphore_wait(sem, len(peers))

    def copy(self, src, dst, send, recv, peer):
        return pltpu.make_async_remote_copy(
            src_ref=src, dst_ref=dst, send_sem=send, recv_sem=recv, device_id=peer, device_id_type=MESH_ID
        )

    def start(self, *args):
        c = self.copy(*args)
        c.start()
        self.pending.append(c)

    def drain(self):
        for c in self.pending:
            c.wait_send()
        self.pending = []


class Gather:
    def __init__(self, ex, shard, full, send, recv, local):
        self.ex, self.shard, self.full, self.send, self.recv = ex, shard, full, send, recv
        self.rows = shard.shape[0]
        self.own = pltpu.make_async_copy(shard, self.part(ex.f), local)

    def part(self, f):
        return self.full.at[rows_at(f, self.rows), :]

    def begin(self):
        ex = self.ex
        for k in range(1, ex.ny):
            ex.start(self.shard, self.part(ex.f), self.send.at[k], self.recv.at[k], (ex.s, ex.y_to(k)))
        ex.start(self.shard, self.part(ex.f), self.send.at[0], self.recv.at[0], (ex.s, ex.partner))
        self.own.start()

    def forward(self):
        ex = self.ex
        for k in range(1, ex.ny):
            part = self.part(ex.y_from(k))
            ex.copy(part, part, self.send.at[k], self.recv.at[k], (ex.s, ex.f)).wait_recv()
            j = ex.ny - 1 + k
            ex.start(part, part, self.send.at[j], self.recv.at[j], (ex.s, ex.partner))

    def finish(self):
        ex = self.ex
        part = self.part(ex.partner)
        ex.copy(part, part, self.send.at[0], self.recv.at[0], (ex.s, ex.f)).wait_recv()
        for k in range(1, ex.ny):
            j = ex.ny - 1 + k
            part = self.part(((ex.y + ex.ny - k) % ex.ny) * 2 + 1 - ex.c)
            ex.copy(part, part, self.send.at[j], self.recv.at[j], (ex.s, ex.f)).wait_recv()
        self.own.wait()


class Sum:
    def __init__(self, ex, out, got, full, sems):
        self.ex, self.out, self.got, self.full = ex, out, got, full
        self.s1, self.r1, self.s2, self.r2 = sems

    def scatter(self):
        ex = self.ex
        for k in range(1, ex.ns):
            peer = ex.seq_peer(k)
            ex.start(self.out.at[peer[0]], self.got.at[k - 1], self.s1.at[k - 1], self.r1.at[k - 1], peer)

    def reduce(self):
        ex = self.ex
        total = self.out[ex.s].astype(F32)
        for k in range(1, ex.ns):
            ex.copy(self.got.at[k - 1], self.got.at[k - 1], self.s1.at[k - 1], self.r1.at[k - 1], ex.seq_peer(k)).wait_recv()
            total = total + self.got[k - 1].astype(F32)
        return total.astype(BF16)

    def spread(self, total):
        ex = self.ex
        self.full[ex.s] = total
        mine = self.full.at[ex.s]
        for k in range(1, ex.ns):
            ex.start(mine, mine, self.s2.at[k - 1], self.r2.at[k - 1], ex.seq_peer(k))

    def finish(self):
        ex = self.ex
        for k in range(1, ex.ns):
            part = self.full.at[(ex.s + ex.ns - k) % ex.ns]
            ex.copy(part, part, self.s2.at[k - 1], self.r2.at[k - 1], ex.seq_peer(k)).wait_recv()


def mask_rows(ids, last_id):
    last = (ids == last_id).astype(F32)
    row = lax.broadcasted_iota(jnp.int32, (PAD, ids.shape[1]), 0)
    return jnp.where(row == 0, 1.0 - last, jnp.where(row == 1, last, 0.0)).astype(BF16)


def last_lanes(ids, last_id):
    last = (ids == last_id).astype(F32)
    return jnp.broadcast_to(last, (128, ids.shape[1])).T > 0.5


def put_chunks(acc_ref, out_ref, first_id, last_id, seqs):
    heads = acc_ref.shape[0]
    if seqs == 2:
        out_ref[...] = acc_ref[...].astype(BF16)
        return
    groups = seqs // 2

    def body(h, carry):
        a = acc_ref[h]
        v1, v2, z1, z2 = a[:64], a[64:128], a[128:129], a[129:130]
        row = lax.broadcasted_iota(jnp.int32, (PAD, a.shape[1]), 0)
        for g in range(groups):
            f0, f1 = (jnp.where(first_id == 2 * g + k, 1.0, 0.0) for k in range(2))
            l0, l1 = (jnp.where(last_id == 2 * g + k, 1.0, 0.0) for k in range(2))
            z = jnp.where(row == 0, f0 * z1 + l0 * z2, jnp.where(row == 1, f1 * z1 + l1 * z2, 0.0))
            out_ref[h * groups + g] = jnp.concatenate([f0 * v1 + l0 * v2, f1 * v1 + l1 * v2, z], axis=0).astype(BF16)
        return carry

    lax.fori_loop(0, heads, body, 0)


def take_slots(full_ref, h, first_id, last_id, seqs):
    if seqs == 2:
        a = full_ref[h].astype(F32)
        return a[:64], a[64:128], a[128:129], a[129:130]
    groups = seqs // 2
    picks = [None] * 4
    for g in range(groups):
        a = full_ref[h * groups + g].astype(F32)
        for k in range(2):
            rows, z = a[64 * k : 64 * k + 64], a[128 + k : 129 + k]
            for which, ident in enumerate((first_id, last_id)):
                hit = ident == 2 * g + k
                for slot, v in ((which, rows), (2 + which, z)):
                    term = jnp.where(hit, v, 0.0)
                    picks[slot] = term if picks[slot] is None else picks[slot] + term
    return picks


def build_b(full_ref, b_ref, first_id, last_id, seqs, repeat):
    for h in range(b_ref.shape[0]):
        r1, r2, z1, z2 = take_slots(full_ref, h, first_id, last_id, seqs)
        if h % 2:
            r1, r2, z1, z2 = r2, r1, z2, z1
        shape = r1.shape
        if repeat:
            z1, z2 = (jnp.broadcast_to(z, shape) for z in (z1, z2))
        else:
            top = lax.broadcasted_iota(jnp.int32, shape, 0) == 0
            z1, z2 = (jnp.where(top, jnp.broadcast_to(z, shape), 0.0) for z in (z1, z2))
        b_ref[h] = jnp.concatenate([r1, r2, z1, z2], axis=0).astype(BF16)


def build_features(rand_ref, rbd_ref, rt_ref):
    heads, dim, feats = rand_ref.shape
    rbd_ref[...] = jnp.zeros_like(rbd_ref)
    lane = lax.broadcasted_iota(jnp.int32, (feats, 128), 1)
    for h in range(heads):
        q, k = h // 4, h % 4
        rbd_ref[q, dim * k : dim * k + dim, feats * k : feats * k + feats] = rand_ref[h]
    for p in range(heads // 2):
        both = jnp.concatenate([rand_ref[2 * p], rand_ref[2 * p + 1]], axis=0).astype(F32).T
        for k in range(2):
            mine = (lane < 64) if k == 0 else (lane >= 64)
            left = jnp.where(mine, both, 0.0)
            right = jnp.where(mine, 1.0, 0.0)
            rt_ref[p, feats * k : feats * k + feats, :] = jnp.concatenate([left, right], axis=1).astype(BF16)


TILED_OUT = ("out", "att", "a2", "hid", "dpre", "dmid", "dq")


def front_kernel(
    x_ref, dy_ref, ids_ref, rand_ref, gains_in, wk_in, wv_in, wq_in, wo_in, wu_in, wd_in,
    out_o, att_o, a2_o, hid_o, dpre_o, dmid_o, dq_o, a1_o, ks_o, vv_o, fk_o, wq_o, wk_o, wv_o, p_o, gain_o, gg_o,
    a1, ks, vv, fk, qs, fq, t_out, t_att, t_a2, t_hid, t_dpre, t_dmid, t_dq,
    gains, wk, wv, wq, wo, wu, wd, rbd, rt, b_ref, acc, p_out, p_got, p_full,
    w_send, w_recv, w_local, r_send, r_recv, g_send, g_recv, o_sem, t_sem,
    *, micro, seqs, factor,
):
    ex = Exchange()
    heads, _, feats = rand_ref.shape
    total, width = x_ref.shape
    toks = total // micro
    tiles = toks // TILE
    pairs = width // 128
    ex.barrier()
    pieces = []
    for i, (shard, full) in enumerate(
        ((gains_in, gains), (wk_in, wk), (wv_in, wv), (wq_in, wq), (wo_in, wo), (wu_in, wu), (wd_in, wd))
    ):
        pieces.append(Gather(ex, shard, full, w_send.at[i], w_recv.at[i], w_local.at[i]))
    for piece in pieces:
        piece.begin()
    build_features(rand_ref, rbd, rt)
    for piece in pieces[:3]:
        piece.forward()
    for piece in pieces[:3]:
        piece.finish()
    gain_rows = gains.shape[0] // ex.nf
    both = gains[0:gain_rows, :].astype(F32)
    for f in range(1, ex.nf):
        both = both + gains[gain_rows * f : gain_rows * f + gain_rows, :].astype(F32)
    gain_o[...] = both.astype(BF16)
    g1, g2 = both[0:1], both[1:2]
    gg_o[...] = jnp.zeros_like(gg_o)

    def ident(mb):
        if seqs == 2:
            return 0, 1
        return ids_ref[mb : mb + 1, 0:1], ids_ref[mb : mb + 1, toks - 1 : toks]

    def ids_of(mb, t):
        return ids_ref[mb : mb + 1, pl.ds(pl.multiple_of(t * TILE, TILE), TILE)]

    outs = []

    def emit(src, dst, sem):
        c = pltpu.make_async_copy(src, dst, sem)
        c.start()
        outs.append(c)

    sums = [
        Sum(ex, p_out.at[mb], p_got.at[mb], p_full.at[mb], (r_send.at[mb], r_recv.at[mb], g_send.at[mb], g_recv.at[mb]))
        for mb in range(micro)
    ]
    for mb in range(micro):
        acc[...] = jnp.zeros_like(acc)
        first_id, last_id = ident(mb)

        def keys(t, carry, mb=mb, last_id=last_id):
            r = rows_at(t + mb * tiles, TILE)
            normed, _ = norm_parts(x_ref[r, :].astype(F32))
            low = (normed * g1).astype(BF16)
            a1[r, :] = low
            k = (dot(low, wk[...]) * factor).astype(BF16)
            ks[r, :] = k
            v = dot(low, wv[...]).astype(BF16)
            vv[r, :] = v
            features(k, rbd, fk.at[r, :], feats)
            vt = v.T
            mask_t = mask_rows(ids_of(mb, t), last_id)
            for h in range(heads):
                lt = summary_rows(vt[64 * h : 64 * h + 64], None, mask_t)
                acc[h] += dot(lt, fk[r, feats * h : feats * h + feats])
            return carry

        lax.fori_loop(0, tiles, keys, 0)
        put_chunks(acc, p_out.at[mb], first_id, last_id, seqs)
        sums[mb].scatter()
    for i, (src, dst) in enumerate(((a1, a1_o), (ks, ks_o), (vv, vv_o), (fk, fk_o))):
        emit(src, dst, o_sem.at[i])
    pieces[3].forward()
    pieces[3].finish()

    def queries(t, carry):
        r = rows_at(t, TILE)
        q = (dot(a1[r, :], wq[...]) * factor).astype(BF16)
        qs[r, :] = q
        features(q, rbd, fq.at[r, :], feats)
        return carry

    lax.fori_loop(0, micro * tiles, queries, 0)
    for mb in range(micro):
        sums[mb].spread(sums[mb].reduce())
    for piece in pieces[4:]:
        piece.forward()
    for piece in pieces[4:]:
        piece.finish()
    for i, (src, dst) in enumerate(((wq, wq_o), (wk, wk_o), (wv, wv_o))):
        emit(src, dst, o_sem.at[4 + i])
    tiled = ((t_out, out_o), (t_att, att_o), (t_a2, a2_o), (t_hid, hid_o), (t_dpre, dpre_o), (t_dmid, dmid_o), (t_dq, dq_o))

    def tile_copies(t, slot):
        r = rows_at(t, TILE)
        return [pltpu.make_async_copy(src.at[slot], dst.at[r, :], t_sem.at[slot, i]) for i, (src, dst) in enumerate(tiled)]

    for mb in range(micro):
        first_id, last_id = ident(mb)
        sums[mb].finish()
        build_b(p_full.at[mb], b_ref, first_id, last_id, seqs, True)
        acc[...] = jnp.zeros_like(acc)

        def mid(t, carry, mb=mb, last_id=last_id):
            g = t + mb * tiles
            slot = g % 2
            r = rows_at(g, TILE)

            @pl.when(g >= 2)
            def _():
                for c in tile_copies(g - 2, slot):
                    c.wait()

            ids = ids_of(mb, t)
            last = last_lanes(ids, last_id)
            mask_t = mask_rows(ids, last_id)
            lane = lax.broadcasted_iota(jnp.int32, (TILE, 128), 1)
            sel = jnp.logical_xor(lane < 64, last)

            def swap(v):
                return jnp.where(last, pltpu.roll(v, 64, 1), v)

            att_parts, inv_parts = [], []
            for p in range(pairs):
                base = 2 * feats * p
                a = dot_nt(fq[r, base : base + feats], b_ref[2 * p])
                b = dot_nt(fq[r, base + feats : base + 2 * feats], b_ref[2 * p + 1])
                inv = 1.0 / jnp.where(sel, a[:, 128:], b[:, 128:])
                att_parts.append(swap(jnp.where(sel, a[:, :128], b[:, :128]) * inv))
                inv_parts.append(swap(inv))
            att = jnp.concatenate(att_parts, axis=1)
            inv = jnp.concatenate(inv_parts, axis=1)
            att_low = att.astype(BF16)
            t_att[slot] = att_low
            mixed = x_ref[r, :].astype(F32) + dot(att_low, wo[...])
            normed, rescale = norm_parts(mixed)
            a2 = (normed * g2).astype(BF16)
            t_a2[slot] = a2
            dy = dy_ref[r, :]
            for j in range(wu.shape[1] // 256):
                js = slice(256 * j, 256 * j + 256)
                pre = dot(a2, wu[:, js])
                dh = dot_nt(dy, wd[js, :])
                cdf = 0.5 * (1.0 + lax.erf(pre * 0.7071067811865476))
                slope = cdf + pre * jnp.exp(-0.5 * pre * pre) * 0.3989422804014327
                t_hid[slot, :, js] = (pre * cdf).astype(BF16)
                t_dpre[slot, :, js] = (dh * slope).astype(BF16)
            t_out[slot] = (mixed + dot(t_hid[slot], wd[...])).astype(BF16)
            da2 = dot_nt(t_dpre[slot], wu[...])
            gg_o[...] += jnp.sum(da2 * normed, axis=0, keepdims=True)
            dmid = dy.astype(F32) + norm_back(da2, normed, rescale, g2)
            dmid_low = dmid.astype(BF16)
            t_dmid[slot] = dmid_low
            dnum = dot_nt(dmid_low, wo[...]) * inv
            dpart = -dnum * att
            for p in range(pairs):
                ps = slice(128 * p, 128 * p + 128)
                d, q = dnum[:, ps], dpart[:, ps]
                ds, dp = swap(d), swap(q)
                la = jnp.concatenate([jnp.where(sel, ds, 0.0), jnp.where(sel, dp, 0.0)], axis=1).astype(BF16)
                lb = jnp.concatenate([jnp.where(sel, 0.0, ds), jnp.where(sel, 0.0, dp)], axis=1).astype(BF16)
                base = 2 * feats * p
                fa = fq[r, base : base + feats]
                fb = fq[r, base + feats : base + 2 * feats]
                ga = (dot(la, b_ref[2 * p]) * fa.astype(F32)).astype(BF16)
                gb = (dot(lb, b_ref[2 * p + 1]) * fb.astype(F32)).astype(BF16)
                o = dot(jnp.concatenate([ga, gb], axis=1), rt[p])
                t_dq[slot, :, ps] = (factor * (o[:, :128] - qs[r, ps].astype(F32) * o[:, 128:])).astype(BF16)
                dt = d.astype(BF16).T
                qt = q.T
                for k, f in enumerate((fa, fb)):
                    z = jnp.sum(qt[64 * k : 64 * k + 64], axis=0, keepdims=True)
                    lt = summary_rows(dt[64 * k : 64 * k + 64], z, mask_t)
                    acc[2 * p + k] += dot(lt, f)
            for c in tile_copies(g, slot):
                c.start()
            return carry

        lax.fori_loop(0, tiles, mid, 0)
        put_chunks(acc, p_o.at[mb], first_id, last_id, seqs)
    last_tile = micro * tiles - 1
    for g in (last_tile - 1, last_tile):
        for c in tile_copies(g, g % 2):
            c.wait()
    for c in outs:
        c.wait()
    ex.drain()


def front(x, dy, ids, rand, gains, wk, wv, wq, wo, wu, wd, *, micro, seqs, nf, ns, factor):
    total, width = x.shape
    heads, _, feats = rand.shape
    hidden = wu.shape[1]
    rows = 128 + PAD
    chunks = heads * (seqs // 2)

    def bf(*shape):
        return jax.ShapeDtypeStruct(shape, BF16)

    hbm = pl.BlockSpec(memory_space=pl.ANY)
    vmem = pl.BlockSpec(memory_space=pltpu.VMEM)
    out_shape = [
        bf(total, width), bf(total, width), bf(total, width), bf(total, hidden), bf(total, hidden), bf(total, width),
        bf(total, width), bf(total, width), bf(total, width), bf(total, width), bf(total, heads * feats),
        bf(width, width), bf(width, width), bf(width, width), bf(micro, chunks, rows, feats),
        bf(PAD, width), jax.ShapeDtypeStruct((1, width), F32),
    ]
    v = pltpu.VMEM
    dma = pltpu.SemaphoreType.DMA
    scratch = [v((total, width), BF16)] * 3 + [v((total, heads * feats), BF16), v((total, width), BF16), v((total, heads * feats), BF16)]
    scratch += [v((2, TILE, width), BF16)] * 3 + [v((2, TILE, hidden), BF16)] * 2 + [v((2, TILE, width), BF16)] * 2
    scratch += [v((nf * PAD, width), BF16)] + [v((width, width), BF16)] * 4 + [v((width, hidden), BF16), v((hidden, width), BF16)]
    scratch += [v((heads // 4, 256, 4 * feats), BF16), v((heads // 2, 2 * feats, 256), BF16), v((heads, 256, feats), BF16)]
    scratch += [v((heads, rows, feats), F32), v((micro, chunks, rows, feats), BF16)]
    scratch += [v((micro, ns - 1, rows, feats), BF16), v((micro, ns, rows, feats), BF16)]
    kinds = nf - 1
    scratch += [dma((7, kinds)), dma((7, kinds)), dma((7,))] + [dma((micro, ns - 1))] * 4 + [dma((7,)), dma((2, 7))]
    return pl.pallas_call(
        functools.partial(front_kernel, micro=micro, seqs=seqs, factor=factor),
        in_specs=[vmem] * 4 + [hbm] * 7,
        out_specs=[hbm] * 14 + [vmem] * 3,
        out_shape=out_shape,
        scratch_shapes=scratch,
        compiler_params=pltpu.CompilerParams(collective_id=0, has_side_effects=True, vmem_limit_bytes=63 << 20),
        name="front",
    )(x, dy, ids, rand, gains, wk, wv, wq, wo, wu, wd)


def second_kernel(
    x_ref, dmid_ref, fk_ref, ks_ref, vv_ref, last_ref, dq_ref, b_ref, g1_ref, wq_ref, wk_ref, wv_ref, rt_ref,
    *refs, feats, factor, n_alias,
):
    dx_ref, dk_ref, dv_ref, gg_ref = refs[n_alias:]
    step = pl.program_id(0)

    @pl.when(step == 0)
    def _():
        gg_ref[...] = jnp.zeros_like(gg_ref)

    rows = x_ref.shape[0]
    pairs = x_ref.shape[1] // 128
    last = last_ref[...].astype(F32) > 0.5
    lane = lax.broadcasted_iota(jnp.int32, (rows, 128), 1)
    sel = jnp.logical_xor(lane < 64, last)
    ones_a = jnp.where(sel, 1.0, 0.0).astype(BF16)
    ones_b = jnp.where(sel, 0.0, 1.0).astype(BF16)

    def swap(v):
        return jnp.where(last, pltpu.roll(v, 64, 1), v)

    for p in range(pairs):
        ps = slice(128 * p, 128 * p + 128)
        v = swap(vv_ref[:, ps].astype(F32))
        la = jnp.concatenate([jnp.where(sel, v, 0.0).astype(BF16), ones_a], axis=1)
        lb = jnp.concatenate([jnp.where(sel, 0.0, v).astype(BF16), ones_b], axis=1)
        base = 2 * feats * p
        fa = fk_ref[:, base : base + feats]
        fb = fk_ref[:, base + feats : base + 2 * feats]
        ga = (dot(la, b_ref[2 * p]) * fa.astype(F32)).astype(BF16)
        gb = (dot(lb, b_ref[2 * p + 1]) * fb.astype(F32)).astype(BF16)
        o = dot(jnp.concatenate([ga, gb], axis=1), rt_ref[p])
        dk_ref[:, ps] = (factor * (o[:, :128] - ks_ref[:, ps].astype(F32) * o[:, 128:])).astype(BF16)
        va = dot_nt(fa, b_ref[2 * p, :128])
        vb = dot_nt(fb, b_ref[2 * p + 1, :128])
        dv_ref[:, ps] = swap(jnp.where(sel, va, vb)).astype(BF16)
    da1 = dot_nt(dq_ref[...], wq_ref[...]) + dot_nt(dk_ref[...], wk_ref[...]) + dot_nt(dv_ref[...], wv_ref[...])
    normed, rescale = norm_parts(x_ref[...].astype(F32))
    gg_ref[...] += jnp.sum(da1 * normed, axis=0, keepdims=True)
    grad = norm_back(da1, normed, rescale, g1_ref[...].astype(F32))
    dx_ref[...] = (dmid_ref[...].astype(F32) + grad).astype(BF16)


def tile_spec(cols, off):
    return pl.BlockSpec((TILE, cols), lambda i: (i + off, 0))


def whole_spec(shape):
    zeros = (0,) * len(shape)
    return pl.BlockSpec(shape, lambda i: zeros, pipeline_mode=pl.Buffered(1))


def anyspec():
    return pl.BlockSpec(memory_space=pl.ANY)


def call(body, mb, tiles, tiled, wholes, mask_t, outs_tiled, outs_whole, scratch, previous, flops, name, **static):
    off = mb * tiles
    total = tiled[0].shape[0]
    in_specs = [tile_spec(a.shape[1], off) for a in tiled]
    args = list(tiled)
    for item in wholes:
        if item is mask_t:
            in_specs.append(pl.BlockSpec((PAD, TILE), lambda i: (0, i + off)))
        else:
            in_specs.append(whole_spec(item.shape))
        args.append(item)
    out_shape = [jax.ShapeDtypeStruct((total, c), BF16) for c in outs_tiled]
    out_specs = [tile_spec(c, off) for c in outs_tiled]
    for shape, dtype in outs_whole:
        out_shape.append(jax.ShapeDtypeStruct(shape, dtype))
        out_specs.append(pl.BlockSpec(shape, functools.partial(lambda n, i: (0,) * n, len(shape))))
    alias = {}
    if previous is not None:
        for k, a in enumerate(previous):
            alias[len(args)] = k
            args.append(a)
            in_specs.append(anyspec())
    n_alias = 0 if previous is None else len(previous)
    return pl.pallas_call(
        functools.partial(body, n_alias=n_alias, **static),
        grid=(tiles,),
        in_specs=in_specs,
        out_specs=out_specs,
        out_shape=out_shape,
        scratch_shapes=scratch,
        input_output_aliases=alias,
        compiler_params=pltpu.CompilerParams(dimension_semantics=("arbitrary",)),
        cost_estimate=pl.CostEstimate(flops=int(flops), bytes_accessed=1 << 20, transcendentals=0),
        name=name,
    )(*args)


def back_features(rand):
    heads, dim, feats = rand.shape
    eye = jnp.eye(2, dtype=rand.dtype)
    pairs = rand.reshape(heads // 2, 2, dim, feats)
    left = jnp.einsum("padf,ab->pafbd", pairs, eye).reshape(heads // 2, 2 * feats, 2 * dim)
    right = jnp.broadcast_to(eye[None, :, None, :, None], (heads // 2, 2, feats, 2, dim))
    return jnp.concatenate([left, right.reshape(left.shape).astype(left.dtype)], axis=2)


def expand(pick, repeat):
    heads, _, feats = pick.shape
    first, second = pick[:, :64], pick[:, 64:128]
    z1, z2 = pick[:, 128:129], pick[:, 129:130]
    if repeat:
        z1, z2 = (jnp.broadcast_to(z, (heads, 64, feats)) for z in (z1, z2))
    else:
        z1, z2 = (jnp.pad(z, ((0, 0), (0, 63), (0, 0))) for z in (z1, z2))
    even = jnp.concatenate([first, second, z1, z2], axis=1)
    odd = jnp.concatenate([second, first, z2, z1], axis=1)
    parity = (jnp.arange(heads) % 2 == 0)[:, None, None]
    return jnp.where(parity, even, odd)


def place(local, ids, seqs):
    if seqs == 2:
        return local[:, None]
    slots = jnp.arange(seqs, dtype=jnp.int32)
    first = (slots == ids[0]).astype(BF16).reshape(1, seqs // 2, 2, 1, 1)
    last = (slots == ids[-1]).astype(BF16).reshape(1, seqs // 2, 2, 1, 1)
    heads, _, feats = local.shape
    rows = local[:, :128].reshape(heads, 1, 2, 64, feats)
    z = local[:, 128:130].reshape(heads, 1, 2, 1, feats)

    def put(v):
        return first * v[:, :, 0:1] + last * v[:, :, 1:2]

    body = put(rows).reshape(heads, seqs // 2, 128, feats)
    tail = jnp.pad(put(z).reshape(heads, seqs // 2, 2, feats), ((0, 0), (0, 0), (0, PAD - 2), (0, 0)))
    return jnp.concatenate([body, tail], axis=2)


def pick_two(dense, ids, seqs):
    if seqs == 2:
        return dense[:, 0]
    heads, _, _, feats = dense.shape
    rows = dense[:, :, :128].reshape(heads, seqs, 64, feats)
    z = dense[:, :, 128:130].reshape(heads, seqs, 1, feats)

    def get(k):
        return (lax.dynamic_index_in_dim(rows, k, 1, False), lax.dynamic_index_in_dim(z, k, 1, False))

    r1, z1 = get(ids[0])
    r2, z2 = get(ids[-1])
    return jnp.pad(jnp.concatenate([r1, r2, z1, z2], axis=1), ((0, 0), (0, PAD - 2), (0, 0)))


def sum_seq(dense):
    return lax.psum(dense, "seq")


def gather(w):
    return lax.all_gather(w, "fsdp", axis=0, tiled=True)


def per_device(block_input, seq_ids, rand, ln1_gain, w_query, w_key, w_value, w_out, ln2_gain, w_up, w_down, cotangent):
    micro, _, toks, width = block_input.shape
    heads, dim, feats = rand.shape
    factor = dim ** (-0.25)
    ns, nf = lax.axis_size("seq"), lax.axis_size("fsdp")
    seqs = max(2, ns // 4)
    tiles = toks // TILE
    x = block_input.reshape(micro * toks, width)
    dy = cotangent.reshape(micro * toks, width)
    ids = seq_ids.reshape(micro, toks)
    shard = ln1_gain.shape[0]
    mine = (jnp.arange(width) // shard == lax.axis_index("fsdp"))[None, :]
    row = jnp.arange(PAD)[:, None]
    gains = jnp.where(row == 0, jnp.tile(ln1_gain, nf)[None, :], jnp.tile(ln2_gain, nf)[None, :])
    gains = jnp.where(jnp.logical_and(mine, row < 2), gains, jnp.zeros_like(gains))
    out, att, a2, hid, dpre, dmid, dq, a1, ks, vv, fk, wq, wk, wv, parts, gains, g2_grad = front(
        x, dy, ids, rand, gains, w_key, w_value, w_query, w_out, w_up, w_down,
        micro=micro, seqs=seqs, nf=nf, ns=ns, factor=factor,
    )
    last = (ids == (1 if seqs == 2 else ids[:, -1:])).reshape(-1)
    last_cols = jnp.broadcast_to(last.astype(BF16)[:, None], (micro * toks, 128))
    rt = back_features(rand)
    g1 = gains[0:1]
    grads = []
    for mb in range(micro):
        dense = lax.psum(parts[mb], "seq").reshape(heads, seqs // 2, 128 + PAD, feats)
        grads.append(pick_two(dense, ids[mb], seqs))
    static = dict(feats=feats, factor=factor)
    unit = 2.0 * toks * 256 * 256
    keep = None
    g1_grad = 0.0
    for mb in range(micro):
        b = expand(grads[mb], False)
        r = call(second_kernel, mb, tiles, [x, dmid, fk, ks, vv, last_cols, dq], [b, g1, wq, wk, wv, rt], None,
                 [width, width, width], [((1, width), F32)], [], keep, 44 * unit, "second", **static)
        keep = r[:3]
        g1_grad = g1_grad + r[3]
    dx, dk, dv = keep

    def weight_grad(left, right):
        return lax.dot_general(left, right, (((0,), (0,)), ((), ())), preferred_element_type=F32).astype(BF16)

    totals = (
        g1_grad.reshape(-1).astype(BF16),
        weight_grad(a1, dq),
        weight_grad(a1, dk),
        weight_grad(a1, dv),
        weight_grad(att, dmid),
        g2_grad.reshape(-1).astype(BF16),
        weight_grad(a2, dpre),
        weight_grad(hid, dy),
    )
    totals = [lax.psum_scatter(t, "fsdp", scatter_dimension=0, tiled=True) for t in totals]
    totals = [lax.psum(t, "seq").astype(F32) for t in totals]
    shape = block_input.shape
    return (out.reshape(shape), dx.reshape(shape), *totals)


def solution(mesh):
    tok = P(None, "fsdp", "seq", None)
    vec, mat = P("fsdp"), P("fsdp", None)
    return jax.shard_map(
        per_device,
        mesh=mesh,
        in_specs=(tok, P(None, "fsdp", "seq"), P(), vec, mat, mat, mat, mat, vec, mat, mat, tok),
        out_specs=(tok, tok, vec, mat, mat, mat, mat, vec, mat, mat),
        check_vma=False,
    )
```

```python
import functools
import math

import jax
import jax.numpy as jnp
from jax import lax
from jax.experimental import pallas as pl
from jax.experimental.pallas import tpu as pltpu
from jax.sharding import PartitionSpec as P

EPS = 1e-05
TILE = 256
F32 = jnp.float32
BF16 = jnp.bfloat16
PAD = 16
SPREAD_AT = 3


def dot(a, b):
    return lax.dot_general(a, b, (((1,), (0,)), ((), ())), preferred_element_type=F32)


def dot_nt(a, b):
    return lax.dot_general(a, b, (((1,), (1,)), ((), ())), preferred_element_type=F32)


def norm_parts(v):
    c = v - jnp.mean(v, axis=-1, keepdims=True)
    r = lax.rsqrt(jnp.mean(c * c, axis=-1, keepdims=True) + EPS)
    return c * r, r


def norm_back(grad, normed, rescale, gain):
    e = grad * gain
    return rescale * (
        e
        - jnp.mean(e, axis=-1, keepdims=True)
        - normed * jnp.mean(e * normed, axis=-1, keepdims=True)
    )


def features(scaled, rbd_ref, feat_ref, feats):
    lane = lax.broadcasted_iota(jnp.int32, (scaled.shape[0], 128), 1)
    low = lane < 64
    log_scale = 0.5 * math.log(feats)
    as_float = scaled.astype(F32)
    for quad in range(scaled.shape[1] // 256):
        u = dot(scaled[:, 256 * quad : 256 * quad + 256], rbd_ref[quad])
        for pair in range(2):
            s = as_float[:, 256 * quad + 128 * pair : 256 * quad + 128 * pair + 128]
            s = s * s
            sq_a = jnp.sum(jnp.where(low, s, 0.0), axis=-1, keepdims=True)
            sq_b = jnp.sum(jnp.where(low, 0.0, s), axis=-1, keepdims=True)
            for k, sq in enumerate((sq_a, sq_b)):
                col = feats * (2 * pair + k)
                f = jnp.exp(u[:, col : col + feats] - (0.5 * sq + log_scale))
                base = feats * (4 * quad + 2 * pair + k)
                feat_ref[:, base : base + feats] = f.astype(BF16)


def summary_rows(rows, zrow, mask_t):
    z = mask_t if zrow is None else (mask_t.astype(F32) * zrow).astype(BF16)
    return jnp.concatenate([rows * mask_t[0:1], z, rows * mask_t[1:2]], axis=0)


MESH_ID = pl.DeviceIdType.MESH


def rows_at(index, size):
    return pl.ds(pl.multiple_of(index * size, size), size)


class Exchange:
    def __init__(self):
        self.s, self.f = lax.axis_index("seq"), lax.axis_index("fsdp")
        self.ns, self.nf = lax.axis_size("seq"), lax.axis_size("fsdp")
        self.ny = self.nf // 2
        self.y, self.c = self.f // 2, self.f % 2
        self.partner = self.y * 2 + (1 - self.c)
        self.pending = []

    def seq_peer(self, k):
        return ((self.s + k) % self.ns, self.f)

    def y_from(self, k):
        return ((self.y + self.ny - k) % self.ny) * 2 + self.c

    def y_to(self, k):
        return ((self.y + k) % self.ny) * 2 + self.c

    def barrier(self):
        sem = pltpu.get_barrier_semaphore()
        peers = [self.seq_peer(k) for k in range(1, self.ns)]
        peers += [(self.s, self.partner)] + [(self.s, self.y_to(k)) for k in range(1, self.ny)]
        for peer in peers:
            pl.semaphore_signal(sem, inc=1, device_id=peer, device_id_type=MESH_ID)
        pl.semaphore_wait(sem, len(peers))

    def copy(self, src, dst, send, recv, peer):
        return pltpu.make_async_remote_copy(
            src_ref=src, dst_ref=dst, send_sem=send, recv_sem=recv, device_id=peer, device_id_type=MESH_ID
        )

    def start(self, *args):
        c = self.copy(*args)
        c.start()
        self.pending.append(c)

    def drain(self):
        for c in self.pending:
            c.wait_send()
        self.pending = []


class Gather:
    def __init__(self, ex, shard, full, send, recv, local):
        self.ex, self.shard, self.full, self.send, self.recv = ex, shard, full, send, recv
        self.rows = shard.shape[0]
        self.own = pltpu.make_async_copy(shard, self.part(ex.f), local)

    def part(self, f):
        return self.full.at[rows_at(f, self.rows), :]

    def begin(self):
        ex = self.ex
        for k in range(1, ex.ny):
            ex.start(self.shard, self.part(ex.f), self.send.at[k], self.recv.at[k], (ex.s, ex.y_to(k)))
        ex.start(self.shard, self.part(ex.f), self.send.at[0], self.recv.at[0], (ex.s, ex.partner))
        self.own.start()

    def forward(self):
        ex = self.ex
        for k in range(1, ex.ny):
            part = self.part(ex.y_from(k))
            ex.copy(part, part, self.send.at[k], self.recv.at[k], (ex.s, ex.f)).wait_recv()
            j = ex.ny - 1 + k
            ex.start(part, part, self.send.at[j], self.recv.at[j], (ex.s, ex.partner))

    def finish(self):
        ex = self.ex
        part = self.part(ex.partner)
        ex.copy(part, part, self.send.at[0], self.recv.at[0], (ex.s, ex.f)).wait_recv()
        for k in range(1, ex.ny):
            j = ex.ny - 1 + k
            part = self.part(((ex.y + ex.ny - k) % ex.ny) * 2 + 1 - ex.c)
            ex.copy(part, part, self.send.at[j], self.recv.at[j], (ex.s, ex.f)).wait_recv()
        self.own.wait()


class Sum:
    def __init__(self, ex, out, got, full, sems, seqs):
        self.ex, self.out, self.got, self.full = ex, out, got, full
        self.s1, self.r1, self.s2, self.r2 = sems
        self.rows = out.shape[1]
        self.edge = ex.ns // (2 * seqs) if seqs == 2 else 0
        if self.edge:
            got[...] = jnp.zeros_like(got)
            full[...] = jnp.zeros_like(full)

    def by_place(self, place, body):
        if not self.edge:
            body(pl.ds(0, self.rows))
            return
        low, high = place < self.edge, place >= self.ex.ns - self.edge
        half = 64 + PAD

        @pl.when(low)
        def _():
            body(pl.ds(0, half))

        @pl.when(high)
        def _():
            body(pl.ds(64, half))

        @pl.when(jnp.logical_not(jnp.logical_or(low, high)))
        def _():
            body(pl.ds(0, self.rows))

    def others(self):
        return range(1, self.ex.ns)

    def scatter_copy(self, k, part):
        peer = self.ex.seq_peer(k)
        return self.ex.copy(self.out.at[peer[0], part], self.got.at[k - 1, part], self.s1.at[k - 1], self.r1.at[k - 1], peer)

    def spread_copy(self, k, index, part):
        ref = self.full.at[index, part]
        return self.ex.copy(ref, ref, self.s2.at[k - 1], self.r2.at[k - 1], self.ex.seq_peer(k))

    def scatter(self):
        self.by_place(self.ex.s, lambda part: [self.scatter_copy(k, part).start() for k in self.others()])

    def scatter_settle(self):
        self.by_place(self.ex.s, lambda part: [self.scatter_copy(k, part).wait_send() for k in self.others()])

    def from_place(self, k):
        return (self.ex.s + self.ex.ns - k) % self.ex.ns

    def reduce(self):
        ex = self.ex
        for k in self.others():
            self.by_place(self.from_place(k), lambda part, k=k: self.scatter_copy(k, part).wait_recv())
        total = self.out[ex.s].astype(F32)
        for k in self.others():
            total = total + self.got[k - 1].astype(F32)
        return total.astype(BF16)

    def spread(self, total):
        self.full[self.ex.s] = total
        for k in self.others():
            to = (self.ex.s + k) % self.ex.ns
            self.by_place(to, lambda part, k=k: self.spread_copy(k, self.ex.s, part).start())

    def spread_settle(self):
        for k in self.others():
            to = (self.ex.s + k) % self.ex.ns
            self.by_place(to, lambda part, k=k: self.spread_copy(k, self.ex.s, part).wait_send())

    def finish(self):
        self.by_place(
            self.ex.s, lambda part: [self.spread_copy(k, self.from_place(k), part).wait_recv() for k in self.others()]
        )


def mask_rows(ids, last_id):
    last = (ids == last_id).astype(F32)
    row = lax.broadcasted_iota(jnp.int32, (PAD, ids.shape[1]), 0)
    return jnp.where(row == 0, 1.0 - last, jnp.where(row == 1, last, 0.0)).astype(BF16)


def last_lanes(ids, last_id):
    last = (ids == last_id).astype(F32)
    return jnp.broadcast_to(last, (128, ids.shape[1])).T > 0.5


def put_chunks(acc_ref, out_ref, first_id, last_id, seqs):
    heads = acc_ref.shape[0]
    if seqs == 2:
        out_ref[...] = acc_ref[...].astype(BF16)
        return
    groups = seqs // 2

    def body(h, carry):
        a = acc_ref[h]
        v1, v2, z1, z2 = a[:64], a[64 + PAD :], a[64:65], a[65:66]
        row = lax.broadcasted_iota(jnp.int32, (PAD, a.shape[1]), 0)
        for g in range(groups):
            f0, f1 = (jnp.where(first_id == 2 * g + k, 1.0, 0.0) for k in range(2))
            l0, l1 = (jnp.where(last_id == 2 * g + k, 1.0, 0.0) for k in range(2))
            z = jnp.where(row == 0, f0 * z1 + l0 * z2, jnp.where(row == 1, f1 * z1 + l1 * z2, 0.0))
            out_ref[h * groups + g] = jnp.concatenate([f0 * v1 + l0 * v2, z, f1 * v1 + l1 * v2], axis=0).astype(BF16)
        return carry

    lax.fori_loop(0, heads, body, 0)


def take_slots(full_ref, h, first_id, last_id, seqs):
    if seqs == 2:
        a = full_ref[h].astype(F32)
        return a[:64], a[64 + PAD :], a[64:65], a[65:66]
    groups = seqs // 2
    picks = [None] * 4
    for g in range(groups):
        a = full_ref[h * groups + g].astype(F32)
        for k in range(2):
            rows, z = a[(64 + PAD) * k : (64 + PAD) * k + 64], a[64 + k : 65 + k]
            for which, ident in enumerate((first_id, last_id)):
                hit = ident == 2 * g + k
                for slot, v in ((which, rows), (2 + which, z)):
                    term = jnp.where(hit, v, 0.0)
                    picks[slot] = term if picks[slot] is None else picks[slot] + term
    return picks


def build_b(full_ref, b_ref, first_id, last_id, seqs, repeat):
    for h in range(b_ref.shape[0]):
        r1, r2, z1, z2 = take_slots(full_ref, h, first_id, last_id, seqs)
        if h % 2:
            r1, r2, z1, z2 = r2, r1, z2, z1
        shape = r1.shape
        if repeat:
            z1, z2 = (jnp.broadcast_to(z, shape) for z in (z1, z2))
        else:
            top = lax.broadcasted_iota(jnp.int32, shape, 0) == 0
            z1, z2 = (jnp.where(top, jnp.broadcast_to(z, shape), 0.0) for z in (z1, z2))
        b_ref[h] = jnp.concatenate([r1, r2, z1, z2], axis=0).astype(BF16)


def build_features(rand_ref, rbd_ref, rt_ref):
    heads, dim, feats = rand_ref.shape
    rbd_ref[...] = jnp.zeros_like(rbd_ref)
    lane = lax.broadcasted_iota(jnp.int32, (feats, 128), 1)
    for h in range(heads):
        q, k = h // 4, h % 4
        rbd_ref[q, dim * k : dim * k + dim, feats * k : feats * k + feats] = rand_ref[h]
    for p in range(heads // 2):
        both = jnp.concatenate([rand_ref[2 * p], rand_ref[2 * p + 1]], axis=0).astype(F32).T
        for k in range(2):
            mine = (lane < 64) if k == 0 else (lane >= 64)
            left = jnp.where(mine, both, 0.0)
            right = jnp.where(mine, 1.0, 0.0)
            rt_ref[p, feats * k : feats * k + feats, :] = jnp.concatenate([left, right], axis=1).astype(BF16)


TILED_OUT = ("out", "att", "a2", "hid", "dpre", "dmid", "dq")


def front_kernel(
    x_ref, dy_ref, ids_ref, rand_ref, gains_in, wk_in, wv_in, wq_in, wo_in, wu_in, wd_in,
    out_o, att_o, a2_o, hid_o, dpre_o, dmid_o, dq_o, a1_o, ks_o, vv_o, fk_o, wq_o, wk_o, wv_o, p_o, s_o, gain_o, gg_o,
    a1, ks, vv, fk, qs, fq, t_out, t_att, t_a2, t_hid, t_dpre, t_dmid, t_dq,
    gains, wk, wv, wq, wo, wu, wd, rbd, rt, b_ref, acc, p_out, p_got, p_full,
    w_send, w_recv, w_local, r_send, r_recv, g_send, g_recv, o_sem, t_sem,
    *, micro, seqs, factor,
):
    ex = Exchange()
    heads, _, feats = rand_ref.shape
    total, width = x_ref.shape
    toks = total // micro
    tiles = toks // TILE
    pairs = width // 128
    sums = [
        Sum(ex, p_out.at[mb], p_got.at[mb], p_full.at[mb], (r_send.at[mb], r_recv.at[mb], g_send.at[mb], g_recv.at[mb]), seqs)
        for mb in range(micro)
    ]
    ex.barrier()
    pieces = []
    for i, (shard, full) in enumerate(
        ((gains_in, gains), (wk_in, wk), (wv_in, wv), (wq_in, wq), (wo_in, wo), (wu_in, wu), (wd_in, wd))
    ):
        pieces.append(Gather(ex, shard, full, w_send.at[i], w_recv.at[i], w_local.at[i]))
    for piece in pieces:
        piece.begin()
    build_features(rand_ref, rbd, rt)
    for piece in pieces[:3]:
        piece.forward()
    for piece in pieces[:3]:
        piece.finish()
    gain_rows = gains.shape[0] // ex.nf
    both = gains[0:gain_rows, :].astype(F32)
    for f in range(1, ex.nf):
        both = both + gains[gain_rows * f : gain_rows * f + gain_rows, :].astype(F32)
    gain_o[...] = both.astype(BF16)
    g1, g2 = both[0:1], both[1:2]
    gg_o[...] = jnp.zeros_like(gg_o)

    def ident(mb):
        if seqs == 2:
            return 0, 1
        return ids_ref[mb : mb + 1, 0:1], ids_ref[mb : mb + 1, toks - 1 : toks]

    def ids_of(mb, t):
        return ids_ref[mb : mb + 1, pl.ds(pl.multiple_of(t * TILE, TILE), TILE)]

    outs = []

    def emit(src, dst, sem):
        c = pltpu.make_async_copy(src, dst, sem)
        c.start()
        outs.append(c)

    for mb in range(micro):
        acc[...] = jnp.zeros_like(acc)
        first_id, last_id = ident(mb)

        def keys(t, carry, mb=mb, last_id=last_id):
            r = rows_at(t + mb * tiles, TILE)
            normed, _ = norm_parts(x_ref[r, :].astype(F32))
            low = (normed * g1).astype(BF16)
            a1[r, :] = low
            k = (dot(low, wk[...]) * factor).astype(BF16)
            ks[r, :] = k
            v = dot(low, wv[...]).astype(BF16)
            vv[r, :] = v
            features(k, rbd, fk.at[r, :], feats)
            vt = v.T
            mask_t = mask_rows(ids_of(mb, t), last_id)
            for h in range(heads):
                lt = summary_rows(vt[64 * h : 64 * h + 64], None, mask_t)
                acc[h] += dot(lt, fk[r, feats * h : feats * h + feats])
            return carry

        lax.fori_loop(0, tiles, keys, 0)
        put_chunks(acc, p_out.at[mb], first_id, last_id, seqs)
        if mb == 0:
            sums[mb].scatter()
    for i, (src, dst) in enumerate(((a1, a1_o), (ks, ks_o), (vv, vv_o), (fk, fk_o))):
        emit(src, dst, o_sem.at[i])
    pieces[3].forward()
    pieces[3].finish()

    def queries(t, carry):
        r = rows_at(t, TILE)
        q = (dot(a1[r, :], wq[...]) * factor).astype(BF16)
        qs[r, :] = q
        features(q, rbd, fq.at[r, :], feats)
        return carry

    def queries_and_sums(t, carry):
        @pl.when(t == SPREAD_AT)
        def _():
            sums[0].spread(sums[0].reduce())
            for other in sums[1:]:
                other.scatter()

        return queries(t, carry)

    lax.fori_loop(0, micro * tiles, queries_and_sums, 0)
    for piece in pieces[4:]:
        piece.forward()
    for piece in pieces[4:]:
        piece.finish()
    for i, (src, dst) in enumerate(((wq, wq_o), (wk, wk_o), (wv, wv_o))):
        emit(src, dst, o_sem.at[4 + i])
    tiled = ((t_out, out_o), (t_att, att_o), (t_a2, a2_o), (t_hid, hid_o), (t_dpre, dpre_o), (t_dmid, dmid_o), (t_dq, dq_o))

    def tile_copies(t, slot):
        r = rows_at(t, TILE)
        return [pltpu.make_async_copy(src.at[slot], dst.at[r, :], t_sem.at[slot, i]) for i, (src, dst) in enumerate(tiled)]

    for mb in range(micro):
        first_id, last_id = ident(mb)
        sums[mb].finish()
        build_b(p_full.at[mb], b_ref, first_id, last_id, seqs, True)
        acc[...] = jnp.zeros_like(acc)

        def mid(t, carry, mb=mb, last_id=last_id):
            g = t + mb * tiles
            slot = g % 2
            r = rows_at(g, TILE)

            @pl.when(g >= 2)
            def _():
                for c in tile_copies(g - 2, slot):
                    c.wait()

            if mb == 0:

                @pl.when(t == 1)
                def _():
                    for other in sums[1:]:
                        other.spread(other.reduce())

            ids = ids_of(mb, t)
            last = last_lanes(ids, last_id)
            mask_t = mask_rows(ids, last_id)
            lane = lax.broadcasted_iota(jnp.int32, (TILE, 128), 1)
            sel = jnp.logical_xor(lane < 64, last)

            def swap(v):
                return jnp.where(last, pltpu.roll(v, 64, 1), v)

            att_parts, inv_parts = [], []
            for p in range(pairs):
                base = 2 * feats * p
                a = dot_nt(fq[r, base : base + feats], b_ref[2 * p])
                b = dot_nt(fq[r, base + feats : base + 2 * feats], b_ref[2 * p + 1])
                inv = 1.0 / jnp.where(sel, a[:, 128:], b[:, 128:])
                att_parts.append(swap(jnp.where(sel, a[:, :128], b[:, :128]) * inv))
                inv_parts.append(swap(inv))
            att = jnp.concatenate(att_parts, axis=1)
            inv = jnp.concatenate(inv_parts, axis=1)
            att_low = att.astype(BF16)
            t_att[slot] = att_low
            mixed = x_ref[r, :].astype(F32) + dot(att_low, wo[...])
            normed, rescale = norm_parts(mixed)
            a2 = (normed * g2).astype(BF16)
            t_a2[slot] = a2
            dy = dy_ref[r, :]
            for j in range(wu.shape[1] // 256):
                js = slice(256 * j, 256 * j + 256)
                pre = dot(a2, wu[:, js])
                dh = dot_nt(dy, wd[js, :])
                cdf = 0.5 * (1.0 + lax.erf(pre * 0.7071067811865476))
                slope = cdf + pre * jnp.exp(-0.5 * pre * pre) * 0.3989422804014327
                t_hid[slot, :, js] = (pre * cdf).astype(BF16)
                t_dpre[slot, :, js] = (dh * slope).astype(BF16)
            t_out[slot] = (mixed + dot(t_hid[slot], wd[...])).astype(BF16)
            da2 = dot_nt(t_dpre[slot], wu[...])
            gg_o[...] += jnp.sum(da2 * normed, axis=0, keepdims=True)
            dmid = dy.astype(F32) + norm_back(da2, normed, rescale, g2)
            dmid_low = dmid.astype(BF16)
            t_dmid[slot] = dmid_low
            dnum = dot_nt(dmid_low, wo[...]) * inv
            dpart = -dnum * att
            for p in range(pairs):
                ps = slice(128 * p, 128 * p + 128)
                d, q = dnum[:, ps], dpart[:, ps]
                ds, dp = swap(d), swap(q)
                la = jnp.concatenate([jnp.where(sel, ds, 0.0), jnp.where(sel, dp, 0.0)], axis=1).astype(BF16)
                lb = jnp.concatenate([jnp.where(sel, 0.0, ds), jnp.where(sel, 0.0, dp)], axis=1).astype(BF16)
                base = 2 * feats * p
                fa = fq[r, base : base + feats]
                fb = fq[r, base + feats : base + 2 * feats]
                ga = (dot(la, b_ref[2 * p]) * fa.astype(F32)).astype(BF16)
                gb = (dot(lb, b_ref[2 * p + 1]) * fb.astype(F32)).astype(BF16)
                o = dot(jnp.concatenate([ga, gb], axis=1), rt[p])
                t_dq[slot, :, ps] = (factor * (o[:, :128] - qs[r, ps].astype(F32) * o[:, 128:])).astype(BF16)
                dt = d.astype(BF16).T
                qt = q.T
                for k, f in enumerate((fa, fb)):
                    z = jnp.sum(qt[64 * k : 64 * k + 64], axis=0, keepdims=True)
                    lt = summary_rows(dt[64 * k : 64 * k + 64], z, mask_t)
                    acc[2 * p + k] += dot(lt, f)
            for c in tile_copies(g, slot):
                c.start()
            return carry

        lax.fori_loop(0, tiles, mid, 0)
        if mb == 0:
            sums[0].scatter_settle()
            put_chunks(acc, p_out.at[0], first_id, last_id, seqs)
            sums[0].scatter()
        else:
            put_chunks(acc, p_o.at[mb - 1], first_id, last_id, seqs)
    s_o[...] = sums[0].reduce()
    last_tile = micro * tiles - 1
    for g in (last_tile - 1, last_tile):
        for c in tile_copies(g, g % 2):
            c.wait()
    for c in outs:
        c.wait()
    for one in sums:
        one.scatter_settle()
        one.spread_settle()
    ex.drain()


def front(x, dy, ids, rand, gains, wk, wv, wq, wo, wu, wd, *, micro, seqs, nf, ns, factor):
    total, width = x.shape
    heads, _, feats = rand.shape
    hidden = wu.shape[1]
    rows = 128 + PAD
    chunks = heads * (seqs // 2)

    def bf(*shape):
        return jax.ShapeDtypeStruct(shape, BF16)

    hbm = pl.BlockSpec(memory_space=pl.ANY)
    vmem = pl.BlockSpec(memory_space=pltpu.VMEM)
    out_shape = [
        bf(total, width), bf(total, width), bf(total, width), bf(total, hidden), bf(total, hidden), bf(total, width),
        bf(total, width), bf(total, width), bf(total, width), bf(total, width), bf(total, heads * feats),
        bf(width, width), bf(width, width), bf(width, width), bf(micro - 1, chunks, rows, feats), bf(rows, feats),
        bf(PAD, width), jax.ShapeDtypeStruct((1, width), F32),
    ]
    v = pltpu.VMEM
    dma = pltpu.SemaphoreType.DMA
    scratch = [v((total, width), BF16)] * 3 + [v((total, heads * feats), BF16), v((total, width), BF16), v((total, heads * feats), BF16)]
    scratch += [v((2, TILE, width), BF16)] * 3 + [v((2, TILE, hidden), BF16)] * 2 + [v((2, TILE, width), BF16)] * 2
    scratch += [v((nf * PAD, width), BF16)] + [v((width, width), BF16)] * 4 + [v((width, hidden), BF16), v((hidden, width), BF16)]
    scratch += [v((heads // 4, 256, 4 * feats), BF16), v((heads // 2, 2 * feats, 256), BF16), v((heads, 256, feats), BF16)]
    scratch += [v((heads, rows, feats), F32), v((micro, chunks, rows, feats), BF16)]
    scratch += [v((micro, ns - 1, rows, feats), BF16), v((micro, ns, rows, feats), BF16)]
    kinds = nf - 1
    scratch += [dma((7, kinds)), dma((7, kinds)), dma((7,))] + [dma((micro, ns - 1))] * 4 + [dma((7,)), dma((2, 7))]
    return pl.pallas_call(
        functools.partial(front_kernel, micro=micro, seqs=seqs, factor=factor),
        in_specs=[vmem] * 4 + [hbm] * 7,
        out_specs=[hbm] * 14 + [vmem] * 4,
        out_shape=out_shape,
        scratch_shapes=scratch,
        compiler_params=pltpu.CompilerParams(collective_id=0, has_side_effects=True, vmem_limit_bytes=63 << 20),
        name="front",
    )(x, dy, ids, rand, gains, wk, wv, wq, wo, wu, wd)


class TwoLevel:
    def __init__(self, ex, out, got1, mid, got2, full, send, recv):
        self.ex, self.out, self.got1, self.mid, self.got2, self.full = ex, out, got1, mid, got2, full
        self.send, self.recv = send, recv
        self.slow = 4 if ex.ns % 4 == 0 else 1
        self.fast = ex.ns // self.slow
        self.z, self.x = ex.s // self.fast, ex.s % self.fast
        self.sent = []

    def device(self, z, x):
        return (z * self.fast + x, self.ex.f)

    def fast_copy(self, phase, k, src, dst):
        j = k - 1
        peer = self.device(self.z, (self.x + k) % self.fast)
        return self.ex.copy(src, dst, self.send.at[phase, j], self.recv.at[phase, j], peer)

    def slow_copy(self, phase, k, src, dst):
        j = k - 1
        peer = self.device((self.z + k) % self.slow, self.x)
        return self.ex.copy(src, dst, self.send.at[phase, j], self.recv.at[phase, j], peer)

    def start(self, c):
        c.start()
        self.ex.pending.append(c)

    def block(self, x):
        return pl.ds(x * self.slow, self.slow)

    def send1(self):
        for k in range(1, self.fast):
            src = self.out.at[self.block((self.x + k) % self.fast)]
            self.start(self.fast_copy(0, k, src, self.got1.at[k - 1]))

    def sum1(self):
        for k in range(1, self.fast):
            self.fast_copy(0, k, self.got1.at[k - 1], self.got1.at[k - 1]).wait_recv()
        total = self.out[self.block(self.x)].astype(F32)
        for k in range(1, self.fast):
            total = total + self.got1[k - 1].astype(F32)
        self.mid[...] = total.astype(BF16)
        for k in range(1, self.slow):
            self.start(self.slow_copy(1, k, self.mid.at[(self.z + k) % self.slow], self.got2.at[k - 1]))

    def sum2(self):
        for k in range(1, self.slow):
            self.slow_copy(1, k, self.got2.at[k - 1], self.got2.at[k - 1]).wait_recv()
        total = self.mid[self.z].astype(F32)
        for k in range(1, self.slow):
            total = total + self.got2[k - 1].astype(F32)
        at = self.x * self.slow + self.z
        self.full[at] = total.astype(BF16)
        for k in range(1, self.slow):
            self.start(self.slow_copy(2, k, self.full.at[at], self.full.at[at]))

    def send4(self):
        for k in range(1, self.slow):
            part = self.full.at[self.x * self.slow + (self.z + self.slow - k) % self.slow]
            self.slow_copy(2, k, part, part).wait_recv()
        mine = self.full.at[self.block(self.x)]
        for k in range(1, self.fast):
            self.start(self.fast_copy(3, k, mine, mine))

    def finish(self):
        for k in range(1, self.fast):
            part = self.full.at[self.block((self.x + self.fast - k) % self.fast)]
            self.fast_copy(3, k, part, part).wait_recv()


class Reduce:
    def __init__(self, ex, part, rc, ry, two, send, recv):
        self.ex, self.part, self.rc, self.ry, self.two, self.send, self.recv = ex, part, rc, ry, two, send, recv

    def core_copy(self, yy):
        ex = self.ex
        f = yy * 2 + (1 - ex.c)
        return ex.copy(self.part.at[f], self.rc.at[yy], self.send.at[yy], self.recv.at[yy], (ex.s, ex.partner))

    def core_send(self):
        for yy in range(self.ex.ny):
            c = self.core_copy(yy)
            c.start()
            self.ex.pending.append(c)

    def y_copy(self, k):
        ex = self.ex
        f = ex.y_to(k)
        j = ex.ny + k - 1
        return ex.copy(self.part.at[f], self.ry.at[k - 1], self.send.at[j], self.recv.at[j], (ex.s, f))

    def core_sum(self):
        ex = self.ex
        for yy in range(ex.ny):
            self.core_copy(yy).wait_recv()
            f = yy * 2 + ex.c
            self.part[f] = (self.part[f].astype(F32) + self.rc[yy].astype(F32)).astype(BF16)
        for k in range(1, ex.ny):
            c = self.y_copy(k)
            c.start()
            ex.pending.append(c)

    def y_sum(self):
        ex = self.ex
        for k in range(1, ex.ny):
            self.y_copy(k).wait_recv()
        total = self.part[ex.f].astype(F32)
        for k in range(1, ex.ny):
            total = total + self.ry[k - 1].astype(F32)
        self.two.out[...] = total.astype(BF16)
        self.two.send1()


def back_kernel(
    x_in, dy_in, hid_in, dpre_in, a2_in, att_in, dmid_in, dq_in, a1_in, ks_in, vv_in, fk_in, wq_in, wk_in, wv_in,
    ids_ref, rand_ref, gain_ref, gg_ref, s0_ref, p1_ref,
    dx_o, g1_o, g2_o, wq_g, wk_g, wv_g, wo_g, wu_g, wd_g,
    x, dy, blk, a2, att, dmid, dq, a1, ks, vv, fk, wq, wk, wv, dk, dv, tr, t_dx, rbd, rt, b_ref,
    p_got, p_full,
    part_d, rc_d, ry_d, out_d, got1_d, mid_d, got2_d, full_d,
    part_u, rc_u, ry_u, out_u, got1_u, mid_u, got2_u, full_u,
    part_q, rc_q, ry_q, out_q, got1_q, mid_q, got2_q, full_q,
    part_k, rc_k, ry_k, out_k, got1_k, mid_k, got2_k, full_k,
    gs, gr,
    l_sem, b_sem, x_sem, r_send, r_recv, g_send, g_recv, c_send, c_recv, t_send, t_recv, n_send, n_recv,
    *, micro, seqs, factor,
):
    ex = Exchange()
    heads, _, feats = rand_ref.shape
    total_rows, width = x.shape
    toks = total_rows // micro
    tiles = toks // TILE
    pairs = width // 128
    hidden = hid_in.shape[1]
    blocks = hidden // 512
    quarter = ex.ns // 4
    chunk = out_d.shape[1]
    shard = quarter * chunk
    sems = [(r_send, r_recv, g_send.at[mb], g_recv.at[mb]) for mb in range(2)]
    sums = [Sum(ex, p1_ref, p_got, p_full.at[mb], sems[mb], seqs) for mb in range(2)]

    loads = {}
    order = (
        ("dy", dy_in, dy), ("a2", a2_in, a2), ("att", att_in, att), ("dmid", dmid_in, dmid), ("a1", a1_in, a1), ("dq", dq_in, dq),
        ("vv", vv_in, vv), ("fk", fk_in, fk), ("ks", ks_in, ks), ("wq", wq_in, wq), ("wk", wk_in, wk), ("wv", wv_in, wv),
        ("x", x_in, x),
    )

    def block_copy(src, b):
        return pltpu.make_async_copy(src.at[:, pl.ds(pl.multiple_of(b * 512, 512), 512)], blk.at[b], b_sem.at[b])

    for i, (name, src, dst) in enumerate(order):
        loads[name] = pltpu.make_async_copy(src, dst, l_sem.at[i])
        loads[name].start()
        if name == "dy":
            for b in range(blocks):
                block_copy(hid_in, b).start()

    def need(*names):
        for name in names:
            loads.pop(name).wait()

    ex.barrier()
    sums[1].scatter()
    sums[0].spread(s0_ref[...])
    groups = []
    for i, refs in enumerate((
        (part_d, rc_d, ry_d, out_d, got1_d, mid_d, got2_d, full_d),
        (part_u, rc_u, ry_u, out_u, got1_u, mid_u, got2_u, full_u),
        (part_q, rc_q, ry_q, out_q, got1_q, mid_q, got2_q, full_q),
        (part_k, rc_k, ry_k, out_k, got1_k, mid_k, got2_k, full_k),
    )):
        two = TwoLevel(ex, *refs[3:], t_send.at[i], t_recv.at[i])
        groups.append(Reduce(ex, *refs[:3], two, c_send.at[i], c_recv.at[i]))
    down, up, query, key = groups
    build_features(rand_ref, rbd, rt)

    need("dy")
    tr[...] = dy[...].T

    def down_block(b, carry):
        block_copy(hid_in, b).wait()
        v = dot(tr[...], blk[b]).T
        n = 512 // chunk
        flat = part_d.at[b * n // ex.ns] if n == ex.ns else None
        v = v.reshape(n, chunk, width).astype(BF16)
        if flat is not None:
            flat[...] = v
        else:
            per = n // ex.ns
            for i in range(per):
                part_d[b * per + i] = v[i * ex.ns : (i + 1) * ex.ns]
        block_copy(dpre_in, b).start()
        return carry

    lax.fori_loop(0, blocks, down_block, 0)
    down.core_send()
    need("a2")
    tr[...] = a2[...].T

    def up_block(b, carry):
        block_copy(dpre_in, b).wait()
        v = dot(tr[...], blk[b])
        for f in range(ex.nf):
            one = v[f * shard : (f + 1) * shard].reshape(quarter, chunk, 512)
            part_u[f, pl.ds(b * quarter, quarter)] = one.astype(BF16)
        return carry

    lax.fori_loop(0, blocks, up_block, 0)
    up.core_send()
    sums[1].spread(sums[1].reduce())
    down.core_sum()

    def small(left_t, right, group, which):
        v = dot(left_t, right)
        for half in range(2):
            for f in range(ex.nf):
                one = v[f * shard : (f + 1) * shard, 256 * half : 256 * half + 256].reshape(quarter, chunk, 256)
                group.part[f, quarter * (2 * which + half) : quarter * (2 * which + half + 1)] = one.astype(BF16)

    need("att", "dmid")
    small(att[...].T, dmid[...], query, 1)
    need("a1", "dq")
    tr[...] = a1[...].T
    small(tr[...], dq[...], query, 0)
    query.core_send()
    up.core_sum()
    need("vv", "fk", "ks")

    def ident(mb):
        if seqs == 2:
            return 0, 1
        return ids_ref[mb : mb + 1, 0:1], ids_ref[mb : mb + 1, toks - 1 : toks]

    def kv_part(mb):
        first_id, last_id = ident(mb)
        build_b(p_full.at[mb], b_ref, first_id, last_id, seqs, False)

        def body(t, carry):
            r = rows_at(t + mb * tiles, TILE)
            ids = ids_ref[mb : mb + 1, pl.ds(pl.multiple_of(t * TILE, TILE), TILE)]
            last = last_lanes(ids, last_id)
            lane = lax.broadcasted_iota(jnp.int32, (TILE, 128), 1)
            sel = jnp.logical_xor(lane < 64, last)
            ones_a = jnp.where(sel, 1.0, 0.0).astype(BF16)
            ones_b = jnp.where(sel, 0.0, 1.0).astype(BF16)

            def swap(v):
                return jnp.where(last, pltpu.roll(v, 64, 1), v)

            for p in range(pairs):
                ps = slice(128 * p, 128 * p + 128)
                v = swap(vv[r, ps].astype(F32))
                la = jnp.concatenate([jnp.where(sel, v, 0.0).astype(BF16), ones_a], axis=1)
                lb = jnp.concatenate([jnp.where(sel, 0.0, v).astype(BF16), ones_b], axis=1)
                base = 2 * feats * p
                fa = fk[r, base : base + feats]
                fb = fk[r, base + feats : base + 2 * feats]
                ga = (dot(la, b_ref[2 * p]) * fa.astype(F32)).astype(BF16)
                gb = (dot(lb, b_ref[2 * p + 1]) * fb.astype(F32)).astype(BF16)
                o = dot(jnp.concatenate([ga, gb], axis=1), rt[p])
                dk[r, ps] = (factor * (o[:, :128] - ks[r, ps].astype(F32) * o[:, 128:])).astype(BF16)
                va = dot_nt(fa, b_ref[2 * p, :128])
                vb = dot_nt(fb, b_ref[2 * p + 1, :128])
                dv[r, ps] = swap(jnp.where(sel, va, vb)).astype(BF16)
            return carry

        lax.fori_loop(0, tiles, body, 0)

    g1 = gain_ref[0:1].astype(F32)
    gs[...] = jnp.zeros_like(gs)
    gs[0, 1:2, :] = gg_ref[...]

    def dx_copy(g, slot):
        return pltpu.make_async_copy(t_dx.at[slot], dx_o.at[rows_at(g, TILE), :], x_sem.at[slot])

    def x_part(mb):
        def body(t, carry):
            g = t + mb * tiles
            slot = g % 2
            r = rows_at(g, TILE)

            @pl.when(g >= 2)
            def _():
                dx_copy(g - 2, slot).wait()

            da1 = dot_nt(dq[r, :], wq[...]) + dot_nt(dk[r, :], wk[...]) + dot_nt(dv[r, :], wv[...])
            normed, rescale = norm_parts(x[r, :].astype(F32))
            gs[0, 0:1, :] += jnp.sum(da1 * normed, axis=0, keepdims=True)
            t_dx[slot] = (dmid[r, :].astype(F32) + norm_back(da1, normed, rescale, g1)).astype(BF16)
            dx_copy(g, slot).start()
            return carry

        lax.fori_loop(0, tiles, body, 0)

    sums[0].finish()
    kv_part(0)
    down.y_sum()
    query.core_sum()
    need("wq", "wk", "wv", "x")
    x_part(0)
    down.two.sum1()
    sums[1].finish()
    kv_part(1)
    small(tr[...], dk[...], key, 0)
    small(tr[...], dv[...], key, 1)
    key.core_send()
    up.y_sum()
    down.two.sum2()
    key.core_sum()
    query.y_sum()
    up.two.sum1()
    x_part(1)
    def gain_copy(level, j, peer):
        return ex.copy(gs.at[level], gr.at[j], n_send.at[j], n_recv.at[j], peer)

    def gain_level(level, jobs):
        for j, peer in jobs:
            gain_copy(level, j, peer).start()
        return jobs

    def gain_sum(level, jobs):
        total = gs[level]
        for j, peer in jobs:
            gain_copy(level, j, peer).wait_recv()
            total = total + gr[j]
        return total

    jobs0 = gain_level(0, [(0, (ex.s, ex.partner))])
    down.two.send4()
    key.y_sum()
    gs[1] = gain_sum(0, jobs0)
    jobs1 = gain_level(1, [(k, (ex.s, ex.y_to(k))) for k in range(1, ex.ny)])
    query.two.sum1()
    up.two.sum2()
    down.two.finish()
    wd_g[...] = full_d[...].astype(F32).reshape(wd_g.shape)
    gs[2] = gain_sum(1, jobs1)
    jobs2 = gain_level(2, [(ex.ny - 1 + k, ex.seq_peer(k)) for k in range(1, ex.ns)])
    key.two.sum1()
    query.two.sum2()
    up.two.send4()
    key.two.sum2()
    query.two.send4()
    up.two.finish()
    for b in range(blocks):
        wu_g[:, 512 * b : 512 * b + 512] = full_u[quarter * b : quarter * b + quarter].astype(F32).reshape(shard, 512)
    gains = gain_sum(2, jobs2)
    mine = jnp.zeros((gains.shape[0], shard), F32)
    for f in range(ex.nf):
        mine = mine + jnp.where(ex.f == f, gains[:, f * shard : f * shard + shard], 0.0)
    g1_o[...] = mine[0:1]
    g2_o[...] = mine[1:2]
    key.two.send4()

    def finish(group, full, refs):
        group.two.finish()
        for which, ref in enumerate(refs):
            for half in range(2):
                i = quarter * (2 * which + half)
                ref[:, 256 * half : 256 * half + 256] = full[i : i + quarter].astype(F32).reshape(shard, 256)

    finish(query, full_q, (wq_g, wo_g))
    finish(key, full_k, (wk_g, wv_g))
    last = micro * tiles - 1
    for g in (last - 1, last):
        dx_copy(g, g % 2).wait()
    for level, jobs in enumerate((jobs0, jobs1, jobs2)):
        for j, peer in jobs:
            gain_copy(level, j, peer).wait_send()
    sums[1].scatter_settle()
    for one in sums:
        one.spread_settle()
    ex.drain()


def back(big, small, *, micro, seqs, nf, ns, shard, factor):
    x, _, hid = big[:3]
    rand = small[1]
    total, width = x.shape
    heads, _, feats = rand.shape
    rows = 128 + PAD
    hidden = hid.shape[1]
    ny = nf // 2
    slow = 4 if ns % 4 == 0 else 1
    fast = ns // slow
    chunk = 4 * shard // ns
    hbm = pl.BlockSpec(memory_space=pl.ANY)
    vmem = pl.BlockSpec(memory_space=pltpu.VMEM)
    v = pltpu.VMEM
    dma = pltpu.SemaphoreType.DMA

    def f32(*shape):
        return jax.ShapeDtypeStruct(shape, F32)

    out_shape = [jax.ShapeDtypeStruct((total, width), BF16), f32(1, shard), f32(1, shard)]
    out_shape += [f32(shard, width)] * 4 + [f32(shard, hidden), f32(hidden // nf, width)]
    token = v((total, width), BF16)
    scratch = [token, token, v((hidden // 512, total, 512), BF16), token, token, token, token, token, token, token]
    scratch += [v((total, heads * feats), BF16)] + [v((width, width), BF16)] * 3 + [token, token, v((width, total), BF16)]
    scratch += [v((2, TILE, width), BF16), v((heads // 4, 256, 4 * feats), BF16), v((heads // 2, 2 * feats, 256), BF16)]
    scratch += [v((heads, 256, feats), BF16), v((ns - 1, rows, feats), BF16), v((2, ns, rows, feats), BF16)]
    for cols in (512, 512, 256, 256):
        scratch += [v((nf, ns, chunk, cols), BF16), v((ny, ns, chunk, cols), BF16), v((ny - 1, ns, chunk, cols), BF16)]
        scratch += [v((ns, chunk, cols), BF16), v((fast - 1, slow, chunk, cols), BF16), v((slow, chunk, cols), BF16)]
        scratch += [v((slow - 1, chunk, cols), BF16), v((ns, chunk, cols), BF16)]
    jobs = 1 + (ny - 1) + (ns - 1)
    scratch += [v((3, 8, width), F32), v((jobs, 8, width), F32)]
    peers = max(fast, slow) - 1
    scratch += [dma((13,)), dma((hidden // 512,)), dma((2,)), dma((ns - 1,)), dma((ns - 1,)), dma((2, ns - 1)), dma((2, ns - 1))]
    scratch += [dma((4, 2 * ny - 1))] * 2 + [dma((4, 4, peers))] * 2 + [dma((jobs,))] * 2
    return pl.pallas_call(
        functools.partial(back_kernel, micro=micro, seqs=seqs, factor=factor),
        in_specs=[hbm] * len(big) + [vmem] * len(small),
        out_specs=[hbm] + [vmem] * 8,
        out_shape=out_shape,
        scratch_shapes=scratch,
        compiler_params=pltpu.CompilerParams(collective_id=1, has_side_effects=True, vmem_limit_bytes=63 << 20),
        name="back",
    )(*big, *small)


def per_device(block_input, seq_ids, rand, ln1_gain, w_query, w_key, w_value, w_out, ln2_gain, w_up, w_down, cotangent):
    micro, _, toks, width = block_input.shape
    heads, dim, feats = rand.shape
    factor = dim ** (-0.25)
    ns, nf = lax.axis_size("seq"), lax.axis_size("fsdp")
    seqs = max(2, ns // 4)
    tiles = toks // TILE
    x = block_input.reshape(micro * toks, width)
    dy = cotangent.reshape(micro * toks, width)
    ids = seq_ids.reshape(micro, toks)
    shard = ln1_gain.shape[0]
    mine = (jnp.arange(width) // shard == lax.axis_index("fsdp"))[None, :]
    row = jnp.arange(PAD)[:, None]
    gains = jnp.where(row == 0, jnp.tile(ln1_gain, nf)[None, :], jnp.tile(ln2_gain, nf)[None, :])
    gains = jnp.where(jnp.logical_and(mine, row < 2), gains, jnp.zeros_like(gains))
    out, att, a2, hid, dpre, dmid, dq, a1, ks, vv, fk, wq, wk, wv, part, total, gains, gg = front(
        x, dy, ids, rand, gains, w_key, w_value, w_query, w_out, w_up, w_down,
        micro=micro, seqs=seqs, nf=nf, ns=ns, factor=factor,
    )
    dx, g1g, g2g, wqg, wkg, wvg, wog, wug, wdg = back(
        [x, dy, hid, dpre, a2, att, dmid, dq, a1, ks, vv, fk, wq, wk, wv],
        [ids, rand, gains, gg, total, part[0]],
        micro=micro, seqs=seqs, nf=nf, ns=ns, shard=shard, factor=factor,
    )
    shape = block_input.shape
    return (out.reshape(shape), dx.reshape(shape), g1g[0], wqg, wkg, wvg, wog, g2g[0], wug, wdg)


def solution(mesh):
    tok = P(None, "fsdp", "seq", None)
    vec, mat = P("fsdp"), P("fsdp", None)
    return jax.shard_map(
        per_device,
        mesh=mesh,
        in_specs=(tok, P(None, "fsdp", "seq"), P(), vec, mat, mat, mat, mat, vec, mat, mat, tok),
        out_specs=(tok, tok, vec, mat, mat, mat, mat, vec, mat, mat),
        check_vma=False,
    )
```

```python
import functools
import math

import jax
import jax.numpy as jnp
from jax import lax
from jax.experimental import pallas as pl
from jax.experimental.pallas import tpu as pltpu
from jax.sharding import PartitionSpec as P

EPS = 1e-05
TILE = 256
F32 = jnp.float32
BF16 = jnp.bfloat16
PAD = 16
SPREAD_AT = 3


def dot(a, b):
    return lax.dot_general(a, b, (((1,), (0,)), ((), ())), preferred_element_type=F32)


def dot_nt(a, b):
    return lax.dot_general(a, b, (((1,), (1,)), ((), ())), preferred_element_type=F32)


def norm_parts(v):
    c = v - jnp.mean(v, axis=-1, keepdims=True)
    r = lax.rsqrt(jnp.mean(c * c, axis=-1, keepdims=True) + EPS)
    return c * r, r


def norm_back(grad, normed, rescale, gain):
    e = grad * gain
    return rescale * (
        e
        - jnp.mean(e, axis=-1, keepdims=True)
        - normed * jnp.mean(e * normed, axis=-1, keepdims=True)
    )


def features(scaled, rbd_ref, feat_ref, feats):
    lane = lax.broadcasted_iota(jnp.int32, (scaled.shape[0], 128), 1)
    low = lane < 64
    log_scale = 0.5 * math.log(feats)
    as_float = scaled.astype(F32)
    for quad in range(scaled.shape[1] // 256):
        u = dot(scaled[:, 256 * quad : 256 * quad + 256], rbd_ref[quad])
        for pair in range(2):
            s = as_float[:, 256 * quad + 128 * pair : 256 * quad + 128 * pair + 128]
            s = s * s
            sq_a = jnp.sum(jnp.where(low, s, 0.0), axis=-1, keepdims=True)
            sq_b = jnp.sum(jnp.where(low, 0.0, s), axis=-1, keepdims=True)
            for k, sq in enumerate((sq_a, sq_b)):
                col = feats * (2 * pair + k)
                f = jnp.exp(u[:, col : col + feats] - (0.5 * sq + log_scale))
                base = feats * (4 * quad + 2 * pair + k)
                feat_ref[:, base : base + feats] = f.astype(BF16)


def summary_rows(rows, zrow, mask_t):
    z = mask_t if zrow is None else (mask_t.astype(F32) * zrow).astype(BF16)
    return jnp.concatenate([rows * mask_t[0:1], z, rows * mask_t[1:2]], axis=0)


MESH_ID = pl.DeviceIdType.MESH


def rows_at(index, size):
    return pl.ds(pl.multiple_of(index * size, size), size)


class Exchange:
    def __init__(self):
        self.s, self.f = lax.axis_index("seq"), lax.axis_index("fsdp")
        self.ns, self.nf = lax.axis_size("seq"), lax.axis_size("fsdp")
        self.ny = self.nf // 2
        self.y, self.c = self.f // 2, self.f % 2
        self.partner = self.y * 2 + (1 - self.c)
        self.pending = []

    def seq_peer(self, k):
        return ((self.s + k) % self.ns, self.f)

    def y_from(self, k):
        return ((self.y + self.ny - k) % self.ny) * 2 + self.c

    def y_to(self, k):
        return ((self.y + k) % self.ny) * 2 + self.c

    def greet(self):
        sem = pltpu.get_barrier_semaphore()
        peers = [self.seq_peer(k) for k in range(1, self.ns)]
        peers += [(self.s, self.partner)] + [(self.s, self.y_to(k)) for k in range(1, self.ny)]
        for peer in peers:
            pl.semaphore_signal(sem, inc=1, device_id=peer, device_id_type=MESH_ID)
        self.peers = len(peers)

    def meet(self):
        pl.semaphore_wait(pltpu.get_barrier_semaphore(), self.peers)

    def barrier(self):
        self.greet()
        self.meet()

    def copy(self, src, dst, send, recv, peer):
        return pltpu.make_async_remote_copy(
            src_ref=src, dst_ref=dst, send_sem=send, recv_sem=recv, device_id=peer, device_id_type=MESH_ID
        )

    def start(self, *args):
        self.launch(lambda: self.copy(*args))

    def launch(self, make):
        make().start()
        self.pending.append(make)

    def drain(self):
        for make in self.pending:
            make().wait_send()
        self.pending = []


class Gather:
    def __init__(self, ex, shard, full, send, recv, local):
        self.ex, self.shard, self.full, self.send, self.recv = ex, shard, full, send, recv
        self.rows = shard.shape[0]
        self.own = pltpu.make_async_copy(shard, self.part(ex.f), local)

    def part(self, f):
        return self.full.at[rows_at(f, self.rows), :]

    def begin(self):
        ex = self.ex
        for k in range(1, ex.ny):
            ex.start(self.shard, self.part(ex.f), self.send.at[k], self.recv.at[k], (ex.s, ex.y_to(k)))
        ex.start(self.shard, self.part(ex.f), self.send.at[0], self.recv.at[0], (ex.s, ex.partner))
        self.own.start()

    def forward(self):
        ex = self.ex
        for k in range(1, ex.ny):
            part = self.part(ex.y_from(k))
            ex.copy(part, part, self.send.at[k], self.recv.at[k], (ex.s, ex.f)).wait_recv()
            j = ex.ny - 1 + k
            ex.start(part, part, self.send.at[j], self.recv.at[j], (ex.s, ex.partner))

    def finish(self):
        ex = self.ex
        part = self.part(ex.partner)
        ex.copy(part, part, self.send.at[0], self.recv.at[0], (ex.s, ex.f)).wait_recv()
        for k in range(1, ex.ny):
            j = ex.ny - 1 + k
            part = self.part(((ex.y + ex.ny - k) % ex.ny) * 2 + 1 - ex.c)
            ex.copy(part, part, self.send.at[j], self.recv.at[j], (ex.s, ex.f)).wait_recv()
        self.own.wait()


class Sum:
    def __init__(self, ex, out, got, full, sems, seqs):
        self.ex, self.out, self.got, self.full = ex, out, got, full
        self.s1, self.r1, self.s2, self.r2 = sems
        self.sparse = seqs == 2
        self.edge = ex.ns // (2 * seqs)
        if self.sparse:
            got[...] = jnp.zeros_like(got)
            full[...] = jnp.zeros_like(full)

    def holds(self, chunk, device):
        return device < self.ex.ns - self.edge if chunk < self.ex.ns // 2 else device >= self.edge

    def chunks_of(self, device):
        return self.order(device, [o for o in range(self.ex.ns) if o != device and self.holds(o, device)])

    def devices_of(self, chunk):
        return self.order(chunk, [d for d in range(self.ex.ns) if d != chunk and self.holds(chunk, d)])

    def order(self, device, others):
        return sorted(others, key=lambda d: (-abs(d // 2 - device // 2), (d - device) % self.ex.ns))

    def each(self, peers, body):
        ex = self.ex
        if not self.sparse:
            for k in range(1, ex.ns):
                body((ex.s + k) % ex.ns)
            return
        for device in range(ex.ns):

            @pl.when(ex.s == device)
            def _(device=device):
                for peer in peers(device):
                    body(peer)

    def out_copy(self, peer):
        ex = self.ex
        return ex.copy(self.out.at[peer], self.got.at[ex.s], self.s1.at[peer], self.r1.at[ex.s], (peer, ex.f))

    def got_copy(self, peer):
        ref = self.got.at[peer]
        return self.ex.copy(ref, ref, self.s1.at[peer], self.r1.at[peer], (peer, self.ex.f))

    def spread_copy(self, peer):
        ex = self.ex
        ref = self.full.at[ex.s]
        return ex.copy(ref, ref, self.s2.at[peer], self.r2.at[ex.s], (peer, ex.f))

    def full_copy(self, peer):
        ref = self.full.at[peer]
        return self.ex.copy(ref, ref, self.s2.at[peer], self.r2.at[peer], (peer, self.ex.f))

    def scatter(self):
        self.each(self.chunks_of, lambda p: self.out_copy(p).start())

    def scatter_settle(self):
        self.each(self.chunks_of, lambda p: self.out_copy(p).wait_send())

    def reduce(self):
        ex = self.ex
        self.each(self.devices_of, lambda p: self.got_copy(p).wait_recv())
        total = self.out[ex.s].astype(F32)
        for k in range(ex.ns) if self.sparse else range(1, ex.ns):
            total = total + self.got[k if self.sparse else (ex.s + k) % ex.ns].astype(F32)
        return total.astype(BF16)

    def spread(self, total):
        self.full[self.ex.s] = total
        self.each(self.devices_of, lambda p: self.spread_copy(p).start())

    def spread_settle(self):
        self.each(self.devices_of, lambda p: self.spread_copy(p).wait_send())

    def finish(self):
        self.each(self.chunks_of, lambda p: self.full_copy(p).wait_recv())


def mask_rows(ids, last_id):
    last = (ids == last_id).astype(F32)
    row = lax.broadcasted_iota(jnp.int32, (PAD, ids.shape[1]), 0)
    return jnp.where(row == 0, 1.0 - last, jnp.where(row == 1, last, 0.0)).astype(BF16)


def last_lanes(ids, last_id):
    last = (ids == last_id).astype(F32)
    return jnp.broadcast_to(last, (128, ids.shape[1])).T > 0.5


def put_chunks(acc_ref, out_ref, first_id, last_id, seqs):
    heads = acc_ref.shape[0]
    if seqs == 2:
        owners = out_ref.shape[0] // 2
        per = heads // owners
        row = lax.broadcasted_iota(jnp.int32, (PAD, acc_ref.shape[2]), 0)
        for i in range(out_ref.shape[0]):
            slot, base = i // owners, per * (i % owners)
            at = (64 + PAD) * slot
            z = jnp.zeros(row.shape, F32)
            for j in range(per):
                z = jnp.where(row == j, acc_ref[base + j, 64 + slot : 65 + slot], z)
            rows = [acc_ref[base + j, at : at + 64] for j in range(per)]
            out_ref[i] = jnp.concatenate([*rows, z], axis=0).astype(BF16)
        return
    groups = seqs // 2

    def body(h, carry):
        a = acc_ref[h]
        v1, v2, z1, z2 = a[:64], a[64 + PAD :], a[64:65], a[65:66]
        row = lax.broadcasted_iota(jnp.int32, (PAD, a.shape[1]), 0)
        for g in range(groups):
            f0, f1 = (jnp.where(first_id == 2 * g + k, 1.0, 0.0) for k in range(2))
            l0, l1 = (jnp.where(last_id == 2 * g + k, 1.0, 0.0) for k in range(2))
            z = jnp.where(row == 0, f0 * z1 + l0 * z2, jnp.where(row == 1, f1 * z1 + l1 * z2, 0.0))
            out_ref[h * groups + g] = jnp.concatenate([f0 * v1 + l0 * v2, z, f1 * v1 + l1 * v2], axis=0).astype(BF16)
        return carry

    lax.fori_loop(0, heads, body, 0)


def take_slots(full_ref, h, heads, first_id, last_id, seqs):
    if seqs == 2:
        owners = full_ref.shape[0] // 2
        per = heads // owners
        j = h % per
        a, b = (full_ref[k * owners + h // per].astype(F32) for k in range(2))
        z = 64 * per + j
        return a[64 * j : 64 * j + 64], b[64 * j : 64 * j + 64], a[z : z + 1], b[z : z + 1]
    groups = seqs // 2
    picks = [None] * 4
    for g in range(groups):
        a = full_ref[h * groups + g].astype(F32)
        for k in range(2):
            rows, z = a[(64 + PAD) * k : (64 + PAD) * k + 64], a[64 + k : 65 + k]
            for which, ident in enumerate((first_id, last_id)):
                hit = ident == 2 * g + k
                for slot, v in ((which, rows), (2 + which, z)):
                    term = jnp.where(hit, v, 0.0)
                    picks[slot] = term if picks[slot] is None else picks[slot] + term
    return picks


def build_b(full_ref, b_ref, first_id, last_id, seqs, repeat):
    for h in range(b_ref.shape[0]):
        r1, r2, z1, z2 = take_slots(full_ref, h, b_ref.shape[0], first_id, last_id, seqs)
        if h % 2:
            r1, r2, z1, z2 = r2, r1, z2, z1
        shape = r1.shape
        if repeat:
            z1, z2 = (jnp.broadcast_to(z, shape) for z in (z1, z2))
        else:
            top = lax.broadcasted_iota(jnp.int32, shape, 0) == 0
            z1, z2 = (jnp.where(top, jnp.broadcast_to(z, shape), 0.0) for z in (z1, z2))
        b_ref[h] = jnp.concatenate([r1, r2, z1, z2], axis=0).astype(BF16)


def build_features(rand_ref, rbd_ref, rt_ref):
    heads, dim, feats = rand_ref.shape
    rbd_ref[...] = jnp.zeros_like(rbd_ref)
    lane = lax.broadcasted_iota(jnp.int32, (feats, 128), 1)
    for h in range(heads):
        q, k = h // 4, h % 4
        rbd_ref[q, dim * k : dim * k + dim, feats * k : feats * k + feats] = rand_ref[h]
    for p in range(heads // 2):
        both = jnp.concatenate([rand_ref[2 * p], rand_ref[2 * p + 1]], axis=0).astype(F32).T
        for k in range(2):
            mine = (lane < 64) if k == 0 else (lane >= 64)
            left = jnp.where(mine, both, 0.0)
            right = jnp.where(mine, 1.0, 0.0)
            rt_ref[p, feats * k : feats * k + feats, :] = jnp.concatenate([left, right], axis=1).astype(BF16)


TILED_OUT = ("out", "att", "a2", "hid", "dpre", "dmid", "dq")


def front_kernel(
    x_ref, dy_ref, ids_ref, rand_ref, g1_in, g2_in, wk_in, wv_in, wq_in, wo_in, wu_in, wd_in,
    out_o, att_o, a2_o, hid_o, dpre_o, dmid_o, dq_o, a1_o, ks_o, vv_o, fk_o, wq_o, wk_o, wv_o, p_o, s_o, gain_o, gg_o,
    a1, ks, vv, fk, qs, fq, t_out, t_att, t_a2, t_hid, t_dpre, t_dmid, t_dq,
    gains_in, gains, wk, wv, wq, wo, wu, wd, rbd, rt, b_ref, acc, p_out, p_got, p_full,
    w_send, w_recv, w_local, r_send, r_recv, g_send, g_recv, o_sem, t_sem,
    *, micro, seqs, factor,
):
    ex = Exchange()
    heads, _, feats = rand_ref.shape
    total, width = x_ref.shape
    toks = total // micro
    tiles = toks // TILE
    pairs = width // 128
    sums = [
        Sum(ex, p_out.at[mb], p_got.at[mb], p_full.at[mb], (r_send.at[mb], r_recv.at[mb], g_send.at[mb], g_recv.at[mb]), seqs)
        for mb in range(micro)
    ]
    place = lax.broadcasted_iota(jnp.int32, (1, width), 1) // g1_in.shape[1] == ex.f
    gains_in[...] = jnp.zeros_like(gains_in)
    for i, g in enumerate((g1_in, g2_in)):
        wide = jnp.concatenate([g[...].astype(F32)] * ex.nf, axis=1)
        gains_in[i : i + 1, :] = jnp.where(place, wide, 0.0).astype(BF16)
    ex.barrier()
    pieces = []
    for i, (shard, full) in enumerate(
        ((gains_in, gains), (wk_in, wk), (wv_in, wv), (wq_in, wq), (wo_in, wo), (wu_in, wu), (wd_in, wd))
    ):
        pieces.append(Gather(ex, shard, full, w_send.at[i], w_recv.at[i], w_local.at[i]))
    for piece in pieces:
        piece.begin()
    build_features(rand_ref, rbd, rt)
    for piece in pieces[:2]:
        piece.forward()
    for piece in pieces[:2]:
        piece.finish()
    gain_rows = gains.shape[0] // ex.nf
    both = gains[0:gain_rows, :].astype(F32)
    for f in range(1, ex.nf):
        both = both + gains[gain_rows * f : gain_rows * f + gain_rows, :].astype(F32)
    gain_o[...] = both.astype(BF16)
    g1, g2 = both[0:1], both[1:2]
    gg_o[...] = jnp.zeros_like(gg_o)

    def ident(mb):
        if seqs == 2:
            return 0, 1
        return ids_ref[mb, :, 0:1], ids_ref[mb, :, toks - 1 : toks]

    def ids_of(mb, t):
        return ids_ref[mb, :, pl.ds(pl.multiple_of(t * TILE, TILE), TILE)]

    outs = []

    def emit(src, dst, sem):
        c = pltpu.make_async_copy(src, dst, sem)
        c.start()
        outs.append(c)

    for mb in range(micro):
        acc[...] = jnp.zeros_like(acc)
        first_id, last_id = ident(mb)

        def keys(t, carry, mb=mb):
            r = rows_at(t + mb * tiles, TILE)
            normed, _ = norm_parts(x_ref[r, :].astype(F32))
            low = (normed * g1).astype(BF16)
            a1[r, :] = low
            k = (dot(low, wk[...]) * factor).astype(BF16)
            ks[r, :] = k
            features(k, rbd, fk.at[r, :], feats)
            return carry

        lax.fori_loop(0, tiles, keys, 0)
        if mb == 0:
            pieces[2].forward()
            pieces[2].finish()

        def values(t, carry, mb=mb, last_id=last_id):
            r = rows_at(t + mb * tiles, TILE)
            v = dot(a1[r, :], wv[...]).astype(BF16)
            vv[r, :] = v
            vt = v.T
            mask_t = mask_rows(ids_of(mb, t), last_id)
            for h in range(heads):
                lt = summary_rows(vt[64 * h : 64 * h + 64], None, mask_t)
                acc[h] += dot(lt, fk[r, feats * h : feats * h + feats])
            return carry

        lax.fori_loop(0, tiles, values, 0)
        put_chunks(acc, p_out.at[mb], first_id, last_id, seqs)
        if mb == 0:
            sums[mb].scatter()
    for i, (src, dst) in enumerate(((a1, a1_o), (ks, ks_o), (vv, vv_o), (fk, fk_o))):
        emit(src, dst, o_sem.at[i])
    pieces[3].forward()
    pieces[3].finish()

    def queries(t, carry):
        r = rows_at(t, TILE)
        q = (dot(a1[r, :], wq[...]) * factor).astype(BF16)
        qs[r, :] = q
        features(q, rbd, fq.at[r, :], feats)
        return carry

    def queries_and_sums(t, carry):
        @pl.when(t == SPREAD_AT)
        def _():
            sums[0].spread(sums[0].reduce())
            for other in sums[1:]:
                other.scatter()

        return queries(t, carry)

    lax.fori_loop(0, micro * tiles, queries_and_sums, 0)
    for piece in pieces[4:]:
        piece.forward()
    for piece in pieces[4:]:
        piece.finish()
    for i, (src, dst) in enumerate(((wq, wq_o), (wk, wk_o), (wv, wv_o))):
        emit(src, dst, o_sem.at[4 + i])
    tiled = ((t_out, out_o), (t_att, att_o), (t_a2, a2_o), (t_hid, hid_o), (t_dpre, dpre_o), (t_dmid, dmid_o), (t_dq, dq_o))

    def tile_copies(t, slot):
        r = rows_at(t, TILE)
        return [pltpu.make_async_copy(src.at[slot], dst.at[r, :], t_sem.at[slot, i]) for i, (src, dst) in enumerate(tiled)]

    for mb in range(micro):
        first_id, last_id = ident(mb)
        sums[mb].finish()
        build_b(p_full.at[mb], b_ref, first_id, last_id, seqs, True)
        acc[...] = jnp.zeros_like(acc)

        def mid(t, carry, mb=mb, last_id=last_id):
            g = t + mb * tiles
            slot = g % 2
            r = rows_at(g, TILE)

            @pl.when(g >= 2)
            def _():
                for c in tile_copies(g - 2, slot):
                    c.wait()

            if mb == 0:

                @pl.when(t == 1)
                def _():
                    for other in sums[1:]:
                        other.spread(other.reduce())

            if mb == 1:

                @pl.when(t == 1)
                def _():
                    sums[0].spread_settle()
                    sums[0].spread(sums[0].reduce())

            ids = ids_of(mb, t)
            last = last_lanes(ids, last_id)
            mask_t = mask_rows(ids, last_id)
            lane = lax.broadcasted_iota(jnp.int32, (TILE, 128), 1)
            sel = jnp.logical_xor(lane < 64, last)

            def swap(v):
                return jnp.where(last, pltpu.roll(v, 64, 1), v)

            att_parts, inv_parts = [], []
            for p in range(pairs):
                base = 2 * feats * p
                a = dot_nt(fq[r, base : base + feats], b_ref[2 * p])
                b = dot_nt(fq[r, base + feats : base + 2 * feats], b_ref[2 * p + 1])
                inv = 1.0 / jnp.where(sel, a[:, 128:], b[:, 128:])
                att_parts.append(swap(jnp.where(sel, a[:, :128], b[:, :128]) * inv))
                inv_parts.append(swap(inv))
            att = jnp.concatenate(att_parts, axis=1)
            inv = jnp.concatenate(inv_parts, axis=1)
            att_low = att.astype(BF16)
            t_att[slot] = att_low
            mixed = x_ref[r, :].astype(F32) + dot(att_low, wo[...])
            normed, rescale = norm_parts(mixed)
            a2 = (normed * g2).astype(BF16)
            t_a2[slot] = a2
            dy = dy_ref[r, :]
            for j in range(wu.shape[1] // 256):
                js = slice(256 * j, 256 * j + 256)
                pre = dot(a2, wu[:, js])
                dh = dot_nt(dy, wd[js, :])
                cdf = 0.5 * (1.0 + lax.erf(pre * 0.7071067811865476))
                slope = cdf + pre * jnp.exp(-0.5 * pre * pre) * 0.3989422804014327
                t_hid[slot, :, js] = (pre * cdf).astype(BF16)
                t_dpre[slot, :, js] = (dh * slope).astype(BF16)
            t_out[slot] = (mixed + dot(t_hid[slot], wd[...])).astype(BF16)
            da2 = dot_nt(t_dpre[slot], wu[...])
            gg_o[...] += jnp.sum(da2 * normed, axis=0, keepdims=True)
            dmid = dy.astype(F32) + norm_back(da2, normed, rescale, g2)
            dmid_low = dmid.astype(BF16)
            t_dmid[slot] = dmid_low
            dnum = dot_nt(dmid_low, wo[...]) * inv
            dpart = -dnum * att
            for p in range(pairs):
                ps = slice(128 * p, 128 * p + 128)
                d, q = dnum[:, ps], dpart[:, ps]
                ds, dp = swap(d), swap(q)
                la = jnp.concatenate([jnp.where(sel, ds, 0.0), jnp.where(sel, dp, 0.0)], axis=1).astype(BF16)
                lb = jnp.concatenate([jnp.where(sel, 0.0, ds), jnp.where(sel, 0.0, dp)], axis=1).astype(BF16)
                base = 2 * feats * p
                fa = fq[r, base : base + feats]
                fb = fq[r, base + feats : base + 2 * feats]
                ga = (dot(la, b_ref[2 * p]) * fa.astype(F32)).astype(BF16)
                gb = (dot(lb, b_ref[2 * p + 1]) * fb.astype(F32)).astype(BF16)
                o = dot(jnp.concatenate([ga, gb], axis=1), rt[p])
                t_dq[slot, :, ps] = (factor * (o[:, :128] - qs[r, ps].astype(F32) * o[:, 128:])).astype(BF16)
                dt = d.astype(BF16).T
                qt = q.T
                for k, f in enumerate((fa, fb)):
                    z = jnp.sum(qt[64 * k : 64 * k + 64], axis=0, keepdims=True)
                    lt = summary_rows(dt[64 * k : 64 * k + 64], z, mask_t)
                    acc[2 * p + k] += dot(lt, f)
            for c in tile_copies(g, slot):
                c.start()
            return carry

        lax.fori_loop(0, tiles, mid, 0)
        if mb == 0:
            sums[0].scatter_settle()
            put_chunks(acc, p_out.at[0], first_id, last_id, seqs)
            sums[0].scatter()
        else:
            put_chunks(acc, p_o.at[mb - 1], first_id, last_id, seqs)
    sums[0].finish()
    emit(p_full.at[0], s_o, o_sem.at[7])
    last_tile = micro * tiles - 1
    for g in (last_tile - 1, last_tile):
        for c in tile_copies(g, g % 2):
            c.wait()
    for c in outs:
        c.wait()
    for one in sums:
        one.scatter_settle()
        one.spread_settle()
    ex.drain()


def front(x, dy, ids, rand, g1, g2, wk, wv, wq, wo, wu, wd, *, micro, seqs, nf, ns, factor):
    total, width = x.shape
    heads, _, feats = rand.shape
    hidden = wu.shape[1]
    rows = 128 + PAD
    chunks = heads * (seqs // 2)

    def bf(*shape):
        return jax.ShapeDtypeStruct(shape, BF16)

    hbm = pl.BlockSpec(memory_space=pl.ANY)
    vmem = pl.BlockSpec(memory_space=pltpu.VMEM)
    out_shape = [
        bf(total, width), bf(total, width), bf(total, width), bf(total, hidden), bf(total, hidden), bf(total, width),
        bf(total, width), bf(total, width), bf(total, width), bf(total, width), bf(total, heads * feats),
        bf(width, width), bf(width, width), bf(width, width), bf(micro - 1, chunks, rows, feats), bf(ns, rows, feats),
        bf(PAD, width), jax.ShapeDtypeStruct((1, width), F32),
    ]
    v = pltpu.VMEM
    dma = pltpu.SemaphoreType.DMA
    scratch = [v((total, width), BF16)] * 3 + [v((total, heads * feats), BF16), v((total, width), BF16), v((total, heads * feats), BF16)]
    scratch += [v((2, TILE, width), BF16)] * 3 + [v((2, TILE, hidden), BF16)] * 2 + [v((2, TILE, width), BF16)] * 2
    scratch += [v((PAD, width), BF16), v((nf * PAD, width), BF16)] + [v((width, width), BF16)] * 4 + [v((width, hidden), BF16), v((hidden, width), BF16)]
    scratch += [v((heads // 4, 256, 4 * feats), BF16), v((heads // 2, 2 * feats, 256), BF16), v((heads, 256, feats), BF16)]
    scratch += [v((heads, rows, feats), F32), v((micro, chunks, rows, feats), BF16)]
    scratch += [v((micro, ns, rows, feats), BF16), v((micro, ns, rows, feats), BF16)]
    kinds = nf - 1
    scratch += [dma((7, kinds)), dma((7, kinds)), dma((7,))] + [dma((micro, ns))] * 4 + [dma((8,)), dma((2, 7))]
    return pl.pallas_call(
        functools.partial(front_kernel, micro=micro, seqs=seqs, factor=factor),
        in_specs=[vmem] * 6 + [hbm] * 6,
        out_specs=[hbm] * 14 + [vmem, hbm, vmem, vmem],
        out_shape=out_shape,
        scratch_shapes=scratch,
        compiler_params=pltpu.CompilerParams(collective_id=0, has_side_effects=True, vmem_limit_bytes=63 << 20),
        name="front",
    )(x, dy, ids, rand, g1, g2, wk, wv, wq, wo, wu, wd)


class SeqSum:
    def __init__(self, ex, refs, send, recv):
        self.ex, self.send, self.recv = ex, send, recv
        self.out, self.got1, self.mid, self.got2, self.full = refs
        self.fast = ex.ns // 4
        self.z, self.x = ex.s // self.fast, ex.s % self.fast

    def copy(self, phase, k, src, dst, z, x):
        return self.ex.copy(src, dst, self.send.at[phase, k - 1], self.recv.at[phase, k - 1], (z * self.fast + x, self.ex.f))

    def fast_copy(self, phase, k, src, dst):
        return self.copy(phase, k, src, dst, self.z, (self.x + k) % self.fast)

    def slow_copy(self, phase, k, src, dst):
        return self.copy(phase, k, src, dst, (self.z + k) % 4, self.x)

    def block(self, x):
        return pl.ds(x * 4, 4)

    def send1(self):
        for k in range(1, self.fast):

            def make(k=k):
                src = self.out.at[self.block((self.x + k) % self.fast)]
                return self.fast_copy(0, k, src, self.got1.at[k - 1])

            self.ex.launch(make)

    def sum1(self):
        for k in range(1, self.fast):
            self.fast_copy(0, k, self.got1.at[k - 1], self.got1.at[k - 1]).wait_recv()
        total = self.out[self.block(self.x)].astype(F32)
        for k in range(1, self.fast):
            total = total + self.got1[k - 1].astype(F32)
        self.mid[...] = total.astype(BF16)
        for k in (2, 1, 3):
            self.ex.launch(lambda k=k: self.slow_copy(1, k, self.mid.at[(self.z + k) % 4], self.got2.at[k - 1]))

    def sum2(self):
        for k in range(1, 4):
            self.slow_copy(1, k, self.got2.at[k - 1], self.got2.at[k - 1]).wait_recv()
        total = self.mid[self.z].astype(F32)
        for k in range(1, 4):
            total = total + self.got2[k - 1].astype(F32)
        self.full[self.x * 4 + self.z] = total.astype(BF16)
        for k in (2, 1, 3):

            def make(k=k):
                mine = self.full.at[self.x * 4 + self.z]
                return self.slow_copy(2, k, mine, mine)

            self.ex.launch(make)

    def send_fast(self):
        for k in range(1, 4):
            part = self.full.at[self.x * 4 + (self.z + 4 - k) % 4]
            self.slow_copy(2, k, part, part).wait_recv()
        for k in range(1, self.fast):

            def make(k=k):
                mine = self.full.at[self.block(self.x)]
                return self.fast_copy(3, k, mine, mine)

            self.ex.launch(make)

    def finish(self):
        for k in range(1, self.fast):
            part = self.full.at[self.block((self.x + self.fast - k) % self.fast)]
            self.fast_copy(3, k, part, part).wait_recv()


class Reduce:
    def __init__(self, ex, part, rc, ry, seq, send, recv):
        self.ex, self.part, self.rc, self.ry, self.seq, self.send, self.recv = ex, part, rc, ry, seq, send, recv
        self.steps = iter([self.core_sum, self.y_sum, seq.sum1, seq.sum2, seq.send_fast, seq.finish])

    def core_copy(self, yy):
        ex = self.ex
        f = yy * 2 + (1 - ex.c)
        return ex.copy(self.part.at[f], self.rc.at[yy], self.send.at[yy], self.recv.at[yy], (ex.s, ex.partner))

    def core_send(self):
        for yy in range(self.ex.ny):
            self.ex.launch(lambda yy=yy: self.core_copy(yy))

    def y_copy(self, k):
        ex = self.ex
        f = ex.y_to(k)
        j = ex.ny + k - 1
        return ex.copy(self.part.at[f], self.ry.at[k - 1], self.send.at[j], self.recv.at[j], (ex.s, f))

    def core_sum(self):
        ex = self.ex
        for k in range(1, ex.ny):
            yy = (ex.y + k) % ex.ny
            f = ex.y_to(k)
            self.core_copy(yy).wait_recv()
            self.part[f] = (self.part[f].astype(F32) + self.rc[yy].astype(F32)).astype(BF16)
            ex.launch(lambda k=k: self.y_copy(k))

    def y_sum(self):
        ex = self.ex
        self.core_copy(ex.y).wait_recv()
        total = self.part[ex.f].astype(F32) + self.rc[ex.y].astype(F32)
        for k in range(1, ex.ny):
            self.y_copy(k).wait_recv()
            total = total + self.ry[k - 1].astype(F32)
        self.seq.out[...] = total.astype(BF16)
        self.seq.send1()


PIECES = 6


def back_kernel(
    x_in, dy_in, hid_in, dpre_in, a2_in, att_in, dmid_in, dq_in, a1_in, ks_in, vv_in, fk_in, wq_in, wk_in, wv_in,
    ids_ref, rand_ref, gain_ref, gg_ref, p0_ref, p1_ref,
    dx_o, g1_o, g2_o, res_o,
    x, dy, blk, a2, att, dmid, dq, a1, ks, vv, fk, wq, wk, wv, dk, dv, tr, t_dx, rbd, rt, b_ref,
    p_got, p_full, part, rc, ry, s_out, s_got1, s_mid, s_got2,
    gs, gr,
    l_sem, b_sem, x_sem, r_send, r_recv, g_send, g_recv, c_send, c_recv, t_send, t_recv, n_send, n_recv,
    *, micro, seqs, factor,
):
    ex = Exchange()
    heads, _, feats = rand_ref.shape
    total_rows, width = x.shape
    toks = total_rows // micro
    tiles = toks // TILE
    pairs = width // 128
    hidden = hid_in.shape[1]
    blocks = hidden // 512
    quarter = ex.ns // 4
    chunk = res_o.shape[2]
    shard = quarter * chunk
    kv_sum = Sum(ex, p1_ref, p_got, p_full, (r_send, r_recv, g_send, g_recv), seqs)

    ex.greet()
    loads = {}
    order = (
        ("att", att_in, att), ("dmid", dmid_in, dmid), ("a1", a1_in, a1), ("dq", dq_in, dq), ("dy", dy_in, dy), ("a2", a2_in, a2),
        ("vv", vv_in, vv), ("fk", fk_in, fk), ("ks", ks_in, ks), ("wq", wq_in, wq), ("wk", wk_in, wk), ("wv", wv_in, wv),
        ("x", x_in, x),
    )

    def block_copy(src, b):
        return pltpu.make_async_copy(src.at[:, pl.ds(pl.multiple_of(b * 512, 512), 512)], blk.at[b], b_sem.at[b])

    for i, (name, src, dst) in enumerate(order):
        loads[name] = pltpu.make_async_copy(src, dst, l_sem.at[i])
        loads[name].start()
        if name == "dy":
            for b in range(blocks):
                block_copy(hid_in, b).start()

    def need(*names):
        for name in names:
            loads.pop(name).wait()

    ex.meet()
    kv_sum.scatter()
    pieces = []
    for i in range(PIECES):
        seq = SeqSum(ex, (s_out.at[i], s_got1.at[i], s_mid.at[i], s_got2.at[i], res_o.at[i]), t_send.at[i], t_recv.at[i])
        pieces.append(Reduce(ex, part.at[i], rc.at[i], ry.at[i], seq, c_send.at[i], c_recv.at[i]))
    q, d1, d2, u1, u2, k = pieces

    def go(*which):
        for one in which:
            next(one.steps)()

    def go_at(t, plan):
        for when, which in plan.items():

            @pl.when(t == when)
            def _(which=which):
                go(*which)

    def small(left_t, right, piece, which):
        v = dot(left_t, right)
        for half in range(2):
            for f in range(ex.nf):
                one = v[f * shard : (f + 1) * shard, 256 * half : 256 * half + 256].reshape(quarter, chunk, 256)
                piece.part[f, quarter * (2 * which + half) : quarter * (2 * which + half + 1)] = one.astype(BF16)

    need("att", "dmid")
    small(att[...].T, dmid[...], q, 1)
    need("a1", "dq")
    small(a1[...].T, dq[...], q, 0)
    q.core_send()
    need("dy")
    tr[...] = dy[...].T
    per = 512 // chunk // ex.ns

    def down_block(i, carry):
        b = (i + (ex.y + 1) % ex.ny * (blocks // ex.ny)) % blocks
        block_copy(hid_in, b).wait()
        v = dot(tr[...], blk[b]).T
        block_copy(dpre_in, b).start()
        for half, piece in enumerate((d1, d2)):
            one = v[:, 256 * half : 256 * half + 256].reshape(512 // chunk, chunk, 256).astype(BF16)
            for j in range(per):
                f = b * per + j
                piece.part[f] = one[j * ex.ns : (j + 1) * ex.ns]

                @pl.when(f % 2 != ex.c)
                def _(f=f, piece=piece):
                    piece.core_copy(f // 2).start()

        go_at(i, {1: (q,)})
        return carry

    lax.fori_loop(0, blocks, down_block, 0)
    for piece in (d1, d2):
        ex.pending += [lambda yy=yy, piece=piece: piece.core_copy(yy) for yy in range(ex.ny)]
    go(d1, d2)
    kv_sum.spread(kv_sum.reduce())
    build_features(rand_ref, rbd, rt)
    need("a2")
    tr[...] = a2[...].T

    def up_block(b, carry):
        block_copy(dpre_in, b).wait()
        v = dot(tr[...], blk[b])
        for half in range(2):
            for f in range(ex.nf):
                one = v[f * shard : (f + 1) * shard, 256 * half : 256 * half + 256].reshape(quarter, chunk, 256)
                part[3 + b // 2, f, pl.ds((b % 2 * 2 + half) * quarter, quarter)] = one.astype(BF16)

        @pl.when(b == 1)
        def _():
            u1.core_send()

        go_at(b, {2: (q,), 3: (u1,)})
        return carry

    lax.fori_loop(0, blocks, up_block, 0)
    u2.core_send()
    tr[...] = a1[...].T
    need("vv", "fk", "ks")

    def ident(mb):
        if seqs == 2:
            return 0, 1
        return ids_ref[mb, :, 0:1], ids_ref[mb, :, toks - 1 : toks]

    def kv_part(mb, full, plan):
        first_id, last_id = ident(mb)
        build_b(full, b_ref, first_id, last_id, seqs, False)

        def body(t, carry):
            r = rows_at(t + mb * tiles, TILE)
            ids = ids_ref[mb, :, pl.ds(pl.multiple_of(t * TILE, TILE), TILE)]
            last = last_lanes(ids, last_id)
            lane = lax.broadcasted_iota(jnp.int32, (TILE, 128), 1)
            sel = jnp.logical_xor(lane < 64, last)
            ones_a = jnp.where(sel, 1.0, 0.0).astype(BF16)
            ones_b = jnp.where(sel, 0.0, 1.0).astype(BF16)

            def swap(v):
                return jnp.where(last, pltpu.roll(v, 64, 1), v)

            for p in range(pairs):
                ps = slice(128 * p, 128 * p + 128)
                v = swap(vv[r, ps].astype(F32))
                la = jnp.concatenate([jnp.where(sel, v, 0.0).astype(BF16), ones_a], axis=1)
                lb = jnp.concatenate([jnp.where(sel, 0.0, v).astype(BF16), ones_b], axis=1)
                base = 2 * feats * p
                fa = fk[r, base : base + feats]
                fb = fk[r, base + feats : base + 2 * feats]
                ga = (dot(la, b_ref[2 * p]) * fa.astype(F32)).astype(BF16)
                gb = (dot(lb, b_ref[2 * p + 1]) * fb.astype(F32)).astype(BF16)
                o = dot(jnp.concatenate([ga, gb], axis=1), rt[p])
                dk[r, ps] = (factor * (o[:, :128] - ks[r, ps].astype(F32) * o[:, 128:])).astype(BF16)
                va = dot_nt(fa, b_ref[2 * p, :128])
                vb = dot_nt(fb, b_ref[2 * p + 1, :128])
                dv[r, ps] = swap(jnp.where(sel, va, vb)).astype(BF16)
            go_at(t, plan)
            return carry

        lax.fori_loop(0, tiles, body, 0)

    g1 = gain_ref[0:1].astype(F32)
    gs[...] = jnp.zeros_like(gs)
    gs[0, 1:2, :] = gg_ref[...]

    def dx_copy(g, slot):
        return pltpu.make_async_copy(t_dx.at[slot], dx_o.at[rows_at(g, TILE), :], x_sem.at[slot])

    def x_part(mb, plan):
        def body(t, carry):
            g = t + mb * tiles
            slot = g % 2
            r = rows_at(g, TILE)

            @pl.when(g >= 2)
            def _():
                dx_copy(g - 2, slot).wait()

            da1 = dot_nt(dq[r, :], wq[...]) + dot_nt(dk[r, :], wk[...]) + dot_nt(dv[r, :], wv[...])
            normed, rescale = norm_parts(x[r, :].astype(F32))
            gs[0, 0:1, :] += jnp.sum(da1 * normed, axis=0, keepdims=True)
            t_dx[slot] = (dmid[r, :].astype(F32) + norm_back(da1, normed, rescale, g1)).astype(BF16)
            dx_copy(g, slot).start()
            go_at(t, plan)
            return carry

        lax.fori_loop(0, tiles, body, 0)

    kv_part(0, p0_ref, {0: (u2,), 1: (d1, q), 2: ()})
    kv_sum.finish()
    kv_part(1, p_full, {1: (d1, d2, q)})
    small(tr[...], dk[...], k, 0)
    small(tr[...], dv[...], k, 1)
    k.core_send()
    go(u1, d2, d1)
    need("wq", "wk", "wv", "x")
    x_part(0, {1: (k, q), 2: (u1, u2)})
    x_part(1, {0: (d2,), 2: (q, d1)})
    def gain_copy(level, j, peer):
        return ex.copy(gs.at[level], gr.at[j], n_send.at[j], n_recv.at[j], peer)

    def gain_level(level, jobs):
        for j, peer in jobs:
            gain_copy(level, j, peer).start()
        return jobs

    def gain_sum(level, jobs):
        total = gs[level]
        for j, peer in jobs:
            gain_copy(level, j, peer).wait_recv()
            total = total + gr[j]
        return total

    jobs0 = gain_level(0, [(0, (ex.s, ex.partner))])
    go(k, u2, u1)
    gs[1] = gain_sum(0, jobs0)
    jobs1 = gain_level(1, [(k, (ex.s, ex.y_to(k))) for k in range(1, ex.ny)])
    go(d1, d2, k, u2)
    gs[2] = gain_sum(1, jobs1)
    jobs2 = gain_level(2, [(ex.ny - 1 + k, ex.seq_peer(k)) for k in range(1, ex.ns)])
    go(d2, u1, k, u1, u2)
    gains = gain_sum(2, jobs2)
    mine = jnp.zeros((gains.shape[0], shard), F32)
    for f in range(ex.nf):
        mine = mine + jnp.where(ex.f == f, gains[:, f * shard : f * shard + shard], 0.0)
    g1_o[...] = mine[0:1]
    g2_o[...] = mine[1:2]
    go(k, u2, k)
    for piece in pieces:
        assert next(piece.steps, None) is None
    last = micro * tiles - 1
    for g in (last - 1, last):
        dx_copy(g, g % 2).wait()
    for level, jobs in enumerate((jobs0, jobs1, jobs2)):
        for j, peer in jobs:
            gain_copy(level, j, peer).wait_send()
    kv_sum.scatter_settle()
    kv_sum.spread_settle()
    ex.drain()


def back(big, small, *, micro, seqs, nf, ns, shard, factor):
    x, _, hid = big[:3]
    rand = small[1]
    total, width = x.shape
    heads, _, feats = rand.shape
    rows = 128 + PAD
    hidden = hid.shape[1]
    ny = nf // 2
    slow = 4
    fast = ns // slow
    chunk = 4 * shard // ns
    hbm = pl.BlockSpec(memory_space=pl.ANY)
    vmem = pl.BlockSpec(memory_space=pltpu.VMEM)
    v = pltpu.VMEM
    dma = pltpu.SemaphoreType.DMA

    def f32(*shape):
        return jax.ShapeDtypeStruct(shape, F32)

    out_shape = [jax.ShapeDtypeStruct((total, width), BF16), f32(1, shard), f32(1, shard)]
    out_shape += [jax.ShapeDtypeStruct((PIECES, ns, chunk, 256), BF16)]
    token = v((total, width), BF16)
    scratch = [token, token, v((hidden // 512, total, 512), BF16), token, token, token, token, token, token, token]
    scratch += [v((total, heads * feats), BF16)] + [v((width, width), BF16)] * 3 + [token, token, v((width, total), BF16)]
    scratch += [v((2, TILE, width), BF16), v((heads // 4, 256, 4 * feats), BF16), v((heads // 2, 2 * feats, 256), BF16)]
    scratch += [v((heads, 256, feats), BF16), v((ns, rows, feats), BF16), v((ns, rows, feats), BF16)]
    for lead in ((nf, ns), (ny, ns), (ny - 1, ns), (ns,), (fast - 1, slow), (slow,), (slow - 1,)):
        scratch.append(v((PIECES, *lead, chunk, 256), BF16))
    jobs = 1 + (ny - 1) + (ns - 1)
    scratch += [v((3, 8, width), F32), v((jobs, 8, width), F32)]
    peers = max(fast, slow) - 1
    scratch += [dma((13,)), dma((hidden // 512,)), dma((2,)), *([dma((ns,))] * 4)]
    scratch += [dma((PIECES, 2 * ny - 1))] * 2 + [dma((PIECES, 4, peers))] * 2 + [dma((jobs,))] * 2
    return pl.pallas_call(
        functools.partial(back_kernel, micro=micro, seqs=seqs, factor=factor),
        in_specs=[hbm] * len(big) + [vmem] * len(small),
        out_specs=[hbm] + [vmem] * 3,
        out_shape=out_shape,
        scratch_shapes=scratch,
        compiler_params=pltpu.CompilerParams(collective_id=1, has_side_effects=True, vmem_limit_bytes=63 << 20),
        name="back",
    )(*big, *small)


def results_kernel(out, dx, q, d1, d2, u1, u2, k, g1, g2, out_o, dx_o, wq, wo, wk, wv, wu, wd, g1_o, g2_o):
    out_o[...] = out[...]
    dx_o[...] = dx[...]
    g1_o[...] = g1[...]
    g2_o[...] = g2[...]

    def wide(a):
        a = a.astype(F32)
        return a.reshape(a.shape[0] * a.shape[1], a.shape[2])

    wd[:, :256] = wide(d1[...])
    wd[:, 256:] = wide(d2[...])
    step = pl.program_id(0)

    def up(piece):
        half = piece.shape[0] // 2
        wu[:, :256] = wide(piece[:half])
        wu[:, 256:] = wide(piece[half:])

    @pl.when(step < 2)
    def _():
        wq[...] = wide(q[...])
        wk[...] = wide(k[...])
        up(u1)

    @pl.when(step >= 2)
    def _():
        wo[...] = wide(q[...])
        wv[...] = wide(k[...])
        up(u2)


def results(out, dx, res, g1, g2, shard):
    total, width = out.shape
    _, ns, chunk, cols = res.shape
    quarter = ns // 4
    rows = pl.BlockSpec((total // 4, width), lambda i: (i, 0))
    gain = pl.BlockSpec((1, shard), lambda i: (0, 0))

    def piece(g):
        return pl.BlockSpec((None, quarter, chunk, cols), lambda i: (g, i, 0, 0))

    def low(i):
        return jnp.minimum(i, 1)

    def high(i):
        return jnp.maximum(i - 2, 0)

    def wider(g, of):
        return pl.BlockSpec((None, 2 * quarter, chunk, cols), lambda i: (g, of(i), 0, 0))

    first = pl.BlockSpec((shard, cols), lambda i: (0, low(i)))
    second = pl.BlockSpec((shard, cols), lambda i: (0, high(i)))
    half = jax.ShapeDtypeStruct((shard, 2 * cols), F32)
    token = jax.ShapeDtypeStruct((total, width), BF16)
    gain_shape = jax.ShapeDtypeStruct((1, shard), F32)
    return pl.pallas_call(
        results_kernel,
        grid=(4,),
        in_specs=[rows, rows, piece(0), piece(1), piece(2), wider(3, low), wider(4, high), piece(5), gain, gain],
        out_specs=[rows, rows, first, second, first, second]
        + [pl.BlockSpec((shard, 2 * cols), lambda i: (0, i)), pl.BlockSpec((shard, 2 * cols), lambda i: (i, 0)), gain, gain],
        out_shape=[token, token, half, half, half, half]
        + [jax.ShapeDtypeStruct((shard, 8 * cols), F32), jax.ShapeDtypeStruct((4 * shard, 2 * cols), F32), gain_shape, gain_shape],
        name="results",
    )(out, dx, res, res, res, res, res, res, g1, g2)


def per_device(block_input, seq_ids, rand, ln1_gain, w_query, w_key, w_value, w_out, ln2_gain, w_up, w_down, cotangent):
    micro, _, toks, width = block_input.shape
    heads, dim, feats = rand.shape
    factor = dim ** (-0.25)
    ns, nf = lax.axis_size("seq"), lax.axis_size("fsdp")
    seqs = max(2, ns // 4)
    x = block_input.reshape(micro * toks, width)
    dy = cotangent.reshape(micro * toks, width)
    shard = ln1_gain.shape[0]
    out, att, a2, hid, dpre, dmid, dq, a1, ks, vv, fk, wq, wk, wv, part, total, gains, gg = front(
        x, dy, seq_ids, rand, ln1_gain.reshape(1, shard), ln2_gain.reshape(1, shard), w_key, w_value, w_query, w_out, w_up, w_down,
        micro=micro, seqs=seqs, nf=nf, ns=ns, factor=factor,
    )
    dx, g1g, g2g, res = back(
        [x, dy, hid, dpre, a2, att, dmid, dq, a1, ks, vv, fk, wq, wk, wv],
        [seq_ids, rand, gains, gg, total, part[0]],
        micro=micro, seqs=seqs, nf=nf, ns=ns, shard=shard, factor=factor,
    )
    shape = block_input.shape
    out, dx, wqg, wog, wkg, wvg, wug, wdg, g1g, g2g = results(out, dx, res, g1g, g2g, shard)
    return (out.reshape(shape), dx.reshape(shape), g1g[0], wqg, wkg, wvg, wog, g2g[0], wug, wdg)


def solution(mesh):
    tok = P(None, "fsdp", "seq", None)
    vec, mat = P("fsdp"), P("fsdp", None)
    return jax.shard_map(
        per_device,
        mesh=mesh,
        in_specs=(tok, P(None, "fsdp", "seq"), P(), vec, mat, mat, mat, mat, vec, mat, mat, tok),
        out_specs=(tok, tok, vec, mat, mat, mat, mat, vec, mat, mat),
        check_vma=False,
    )
```

```python
import functools
import math

import jax
import jax.numpy as jnp
from jax import lax
from jax.experimental import pallas as pl
from jax.experimental.pallas import tpu as pltpu
from jax.sharding import PartitionSpec as P

EPS = 1e-05
TILE = 256
F32 = jnp.float32
BF16 = jnp.bfloat16
PAD = 16
SCATTER_AT = 3
AR2_AT = 1


def dot(a, b):
    return lax.dot_general(a, b, (((1,), (0,)), ((), ())), preferred_element_type=F32)


def dot_nt(a, b):
    return lax.dot_general(a, b, (((1,), (1,)), ((), ())), preferred_element_type=F32)


def norm_parts(v):
    c = v - jnp.mean(v, axis=-1, keepdims=True)
    r = lax.rsqrt(jnp.mean(c * c, axis=-1, keepdims=True) + EPS)
    return c * r, r


def norm_back(grad, normed, rescale, gain):
    e = grad * gain
    return rescale * (
        e
        - jnp.mean(e, axis=-1, keepdims=True)
        - normed * jnp.mean(e * normed, axis=-1, keepdims=True)
    )


def features(scaled, rbd_ref, feat_ref, feats):
    lane = lax.broadcasted_iota(jnp.int32, (scaled.shape[0], 128), 1)
    low = lane < 64
    log_scale = 0.5 * math.log(feats)
    as_float = scaled.astype(F32)
    for quad in range(scaled.shape[1] // 256):
        u = dot(scaled[:, 256 * quad : 256 * quad + 256], rbd_ref[quad])
        for pair in range(2):
            s = as_float[:, 256 * quad + 128 * pair : 256 * quad + 128 * pair + 128]
            s = s * s
            sq_a = jnp.sum(jnp.where(low, s, 0.0), axis=-1, keepdims=True)
            sq_b = jnp.sum(jnp.where(low, 0.0, s), axis=-1, keepdims=True)
            for k, sq in enumerate((sq_a, sq_b)):
                col = feats * (2 * pair + k)
                f = jnp.exp(u[:, col : col + feats] - (0.5 * sq + log_scale))
                base = feats * (4 * quad + 2 * pair + k)
                feat_ref[:, base : base + feats] = f.astype(BF16)


def summary_rows(rows, zrow, mask_t):
    z = mask_t if zrow is None else (mask_t.astype(F32) * zrow).astype(BF16)
    return jnp.concatenate([rows * mask_t[0:1], z, rows * mask_t[1:2]], axis=0)


MESH_ID = pl.DeviceIdType.MESH


def rows_at(index, size):
    return pl.ds(pl.multiple_of(index * size, size), size)


class Exchange:
    def __init__(self):
        self.s, self.f = lax.axis_index("seq"), lax.axis_index("fsdp")
        self.ns, self.nf = lax.axis_size("seq"), lax.axis_size("fsdp")
        self.ny = self.nf // 2
        self.y, self.c = self.f // 2, self.f % 2
        self.partner = self.y * 2 + (1 - self.c)
        self.pending = []

    def seq_peer(self, k):
        return ((self.s + k) % self.ns, self.f)

    def y_from(self, k):
        return ((self.y + self.ny - k) % self.ny) * 2 + self.c

    def y_to(self, k):
        return ((self.y + k) % self.ny) * 2 + self.c

    def greet(self):
        sem = pltpu.get_barrier_semaphore()
        peers = [self.seq_peer(k) for k in range(1, self.ns)]
        peers += [(self.s, self.partner)] + [(self.s, self.y_to(k)) for k in range(1, self.ny)]
        for peer in peers:
            pl.semaphore_signal(sem, inc=1, device_id=peer, device_id_type=MESH_ID)
        self.peers = len(peers)

    def meet(self):
        pl.semaphore_wait(pltpu.get_barrier_semaphore(), self.peers)

    def barrier(self):
        self.greet()
        self.meet()

    def copy(self, src, dst, send, recv, peer):
        return pltpu.make_async_remote_copy(
            src_ref=src, dst_ref=dst, send_sem=send, recv_sem=recv, device_id=peer, device_id_type=MESH_ID
        )

    def start(self, *args):
        self.launch(lambda: self.copy(*args))

    def launch(self, make):
        make().start()
        self.pending.append(make)

    def drain(self):
        for make in self.pending:
            make().wait_send()
        self.pending = []


class Gather:
    def __init__(self, ex, shard, full, send, recv, local):
        self.ex, self.shard, self.full, self.send, self.recv = ex, shard, full, send, recv
        self.rows = shard.shape[0]
        self.own = pltpu.make_async_copy(shard, self.part(ex.f), local)

    def part(self, f):
        return self.full.at[rows_at(f, self.rows), :]

    def begin(self):
        ex = self.ex
        for k in range(1, ex.ny):
            ex.start(self.shard, self.part(ex.f), self.send.at[k], self.recv.at[k], (ex.s, ex.y_to(k)))
        ex.start(self.shard, self.part(ex.f), self.send.at[0], self.recv.at[0], (ex.s, ex.partner))
        self.own.start()

    def forward(self):
        ex = self.ex
        for k in range(1, ex.ny):
            part = self.part(ex.y_from(k))
            ex.copy(part, part, self.send.at[k], self.recv.at[k], (ex.s, ex.f)).wait_recv()
            j = ex.ny - 1 + k
            ex.start(part, part, self.send.at[j], self.recv.at[j], (ex.s, ex.partner))

    def finish(self):
        ex = self.ex
        part = self.part(ex.partner)
        ex.copy(part, part, self.send.at[0], self.recv.at[0], (ex.s, ex.f)).wait_recv()
        for k in range(1, ex.ny):
            j = ex.ny - 1 + k
            part = self.part(((ex.y + ex.ny - k) % ex.ny) * 2 + 1 - ex.c)
            ex.copy(part, part, self.send.at[j], self.recv.at[j], (ex.s, ex.f)).wait_recv()
        self.own.wait()


class Sum:
    def __init__(self, ex, out, got, full, sems, seqs):
        self.ex, self.out, self.got, self.full = ex, out, got, full
        self.s1, self.r1, self.s2, self.r2 = sems
        self.sparse = seqs == 2
        self.edge = ex.ns // (2 * seqs)
        if self.sparse:
            got[...] = jnp.zeros_like(got)
            full[...] = jnp.zeros_like(full)

    def holds(self, chunk, device):
        return device < self.ex.ns - self.edge if chunk < self.ex.ns // 2 else device >= self.edge

    def chunks_of(self, device):
        return self.order(device, [o for o in range(self.ex.ns) if o != device and self.holds(o, device)])

    def devices_of(self, chunk):
        return self.order(chunk, [d for d in range(self.ex.ns) if d != chunk and self.holds(chunk, d)])

    def order(self, device, others):
        return sorted(others, key=lambda d: (-abs(d // 2 - device // 2), (d - device) % self.ex.ns))

    def each(self, peers, body):
        ex = self.ex
        if not self.sparse:
            for k in range(1, ex.ns):
                body((ex.s + k) % ex.ns)
            return
        for device in range(ex.ns):

            @pl.when(ex.s == device)
            def _(device=device):
                for peer in peers(device):
                    body(peer)

    def out_copy(self, peer):
        ex = self.ex
        return ex.copy(self.out.at[peer], self.got.at[ex.s], self.s1.at[peer], self.r1.at[ex.s], (peer, ex.f))

    def got_copy(self, peer):
        ref = self.got.at[peer]
        return self.ex.copy(ref, ref, self.s1.at[peer], self.r1.at[peer], (peer, self.ex.f))

    def spread_copy(self, peer):
        ex = self.ex
        ref = self.full.at[ex.s]
        return ex.copy(ref, ref, self.s2.at[peer], self.r2.at[ex.s], (peer, ex.f))

    def full_copy(self, peer):
        ref = self.full.at[peer]
        return self.ex.copy(ref, ref, self.s2.at[peer], self.r2.at[peer], (peer, self.ex.f))

    def scatter(self):
        self.each(self.chunks_of, lambda p: self.out_copy(p).start())

    def scatter_settle(self):
        self.each(self.chunks_of, lambda p: self.out_copy(p).wait_send())

    def reduce(self):
        ex = self.ex
        self.each(self.devices_of, lambda p: self.got_copy(p).wait_recv())
        total = self.out[ex.s].astype(F32)
        for k in range(ex.ns) if self.sparse else range(1, ex.ns):
            total = total + self.got[k if self.sparse else (ex.s + k) % ex.ns].astype(F32)
        return total.astype(BF16)

    def spread(self, total):
        self.full[self.ex.s] = total
        self.each(self.devices_of, lambda p: self.spread_copy(p).start())

    def spread_settle(self):
        self.each(self.devices_of, lambda p: self.spread_copy(p).wait_send())

    def finish(self):
        self.each(self.chunks_of, lambda p: self.full_copy(p).wait_recv())


def mask_rows(ids, last_id):
    last = (ids == last_id).astype(F32)
    row = lax.broadcasted_iota(jnp.int32, (PAD, ids.shape[1]), 0)
    return jnp.where(row == 0, 1.0 - last, jnp.where(row == 1, last, 0.0)).astype(BF16)


def last_lanes(ids, last_id):
    last = (ids == last_id).astype(F32)
    return jnp.broadcast_to(last, (128, ids.shape[1])).T > 0.5


def put_chunks(acc_ref, out_ref, first_id, last_id, seqs):
    heads = acc_ref.shape[0]
    if seqs == 2:
        owners = out_ref.shape[0] // 2
        per = heads // owners
        row = lax.broadcasted_iota(jnp.int32, (PAD, acc_ref.shape[2]), 0)
        for i in range(out_ref.shape[0]):
            slot, base = i // owners, per * (i % owners)
            at = (64 + PAD) * slot
            z = jnp.zeros(row.shape, F32)
            for j in range(per):
                z = jnp.where(row == j, acc_ref[base + j, 64 + slot : 65 + slot], z)
            rows = [acc_ref[base + j, at : at + 64] for j in range(per)]
            out_ref[i] = jnp.concatenate([*rows, z], axis=0).astype(BF16)
        return
    groups = seqs // 2

    def body(h, carry):
        a = acc_ref[h]
        v1, v2, z1, z2 = a[:64], a[64 + PAD :], a[64:65], a[65:66]
        row = lax.broadcasted_iota(jnp.int32, (PAD, a.shape[1]), 0)
        for g in range(groups):
            f0, f1 = (jnp.where(first_id == 2 * g + k, 1.0, 0.0) for k in range(2))
            l0, l1 = (jnp.where(last_id == 2 * g + k, 1.0, 0.0) for k in range(2))
            z = jnp.where(row == 0, f0 * z1 + l0 * z2, jnp.where(row == 1, f1 * z1 + l1 * z2, 0.0))
            out_ref[h * groups + g] = jnp.concatenate([f0 * v1 + l0 * v2, z, f1 * v1 + l1 * v2], axis=0).astype(BF16)
        return carry

    lax.fori_loop(0, heads, body, 0)


def take_slots(full_ref, h, heads, first_id, last_id, seqs):
    if seqs == 2:
        owners = full_ref.shape[0] // 2
        per = heads // owners
        j = h % per
        a, b = (full_ref[k * owners + h // per].astype(F32) for k in range(2))
        z = 64 * per + j
        return a[64 * j : 64 * j + 64], b[64 * j : 64 * j + 64], a[z : z + 1], b[z : z + 1]
    groups = seqs // 2
    picks = [None] * 4
    for g in range(groups):
        a = full_ref[h * groups + g].astype(F32)
        for k in range(2):
            rows, z = a[(64 + PAD) * k : (64 + PAD) * k + 64], a[64 + k : 65 + k]
            for which, ident in enumerate((first_id, last_id)):
                hit = ident == 2 * g + k
                for slot, v in ((which, rows), (2 + which, z)):
                    term = jnp.where(hit, v, 0.0)
                    picks[slot] = term if picks[slot] is None else picks[slot] + term
    return picks


def build_b(full_ref, b_ref, first_id, last_id, seqs, repeat):
    for h in range(b_ref.shape[0]):
        r1, r2, z1, z2 = take_slots(full_ref, h, b_ref.shape[0], first_id, last_id, seqs)
        if h % 2:
            r1, r2, z1, z2 = r2, r1, z2, z1
        shape = r1.shape
        if repeat:
            z1, z2 = (jnp.broadcast_to(z, shape) for z in (z1, z2))
        else:
            top = lax.broadcasted_iota(jnp.int32, shape, 0) == 0
            z1, z2 = (jnp.where(top, jnp.broadcast_to(z, shape), 0.0) for z in (z1, z2))
        b_ref[h] = jnp.concatenate([r1, r2, z1, z2], axis=0).astype(BF16)


def build_features(rand_ref, rbd_ref, rt_ref):
    heads, dim, feats = rand_ref.shape
    rbd_ref[...] = jnp.zeros_like(rbd_ref)
    lane = lax.broadcasted_iota(jnp.int32, (feats, 128), 1)
    for h in range(heads):
        q, k = h // 4, h % 4
        rbd_ref[q, dim * k : dim * k + dim, feats * k : feats * k + feats] = rand_ref[h]
    for p in range(heads // 2):
        both = jnp.concatenate([rand_ref[2 * p], rand_ref[2 * p + 1]], axis=0).astype(F32).T
        for k in range(2):
            mine = (lane < 64) if k == 0 else (lane >= 64)
            left = jnp.where(mine, both, 0.0)
            right = jnp.where(mine, 1.0, 0.0)
            rt_ref[p, feats * k : feats * k + feats, :] = jnp.concatenate([left, right], axis=1).astype(BF16)


TILED_OUT = ("out", "att", "a2", "hid", "dpre", "dmid", "dq")


def front_kernel(
    x_in, dy_in, ids_ref, rand_ref, g1_in, g2_in, wk_in, wv_in, wq_in, wo_in, wu_in, wd_in,
    out_o, att_o, a2_o, hid_o, dpre_o, dmid_o, dq_o, a1_o, ks_o, vv_o, fk_o, wq_o, wk_o, wv_o, p_o, s_o, gain_o, gg_o,
    x_ref, dy_ref,
    a1, ks, vv, fk, qs, fq, t_out, t_att, t_a2, t_hid, t_dpre, t_dmid, t_dq, att_s, inv_s, mix_s,
    gains_in, gains, wk, wv, wq, wo, wu, wd, rbd, rt, b_ref, acc, p_out, p_got, p_full,
    w_send, w_recv, w_local, r_send, r_recv, g_send, g_recv, o_sem, t_sem,
    *, micro, seqs, factor,
):
    ex = Exchange()
    heads, _, feats = rand_ref.shape
    total, width = x_in.shape
    x_load = pltpu.make_async_copy(x_in, x_ref, o_sem.at[8])
    dy_load = pltpu.make_async_copy(dy_in, dy_ref, o_sem.at[9])
    x_load.start()
    dy_load.start()
    toks = total // micro
    tiles = toks // TILE
    pairs = width // 128
    sums = [
        Sum(ex, p_out.at[mb], p_got.at[mb], p_full.at[mb], (r_send.at[mb], r_recv.at[mb], g_send.at[mb], g_recv.at[mb]), seqs)
        for mb in range(micro)
    ]
    ex.greet()
    place = lax.broadcasted_iota(jnp.int32, (1, width), 1) // g1_in.shape[1] == ex.f
    gains_in[...] = jnp.zeros_like(gains_in)
    for i, g in enumerate((g1_in, g2_in)):
        wide = jnp.concatenate([g[...].astype(F32)] * ex.nf, axis=1)
        gains_in[i : i + 1, :] = jnp.where(place, wide, 0.0).astype(BF16)
    ex.meet()
    pieces = []
    for i, (shard, full) in enumerate(
        ((gains_in, gains), (wk_in, wk), (wv_in, wv), (wq_in, wq), (wo_in, wo), (wd_in, wd), (wu_in, wu))
    ):
        pieces.append(Gather(ex, shard, full, w_send.at[i], w_recv.at[i], w_local.at[i]))
    for piece in pieces:
        piece.begin()
    build_features(rand_ref, rbd, rt)
    for piece in pieces[:2]:
        piece.forward()
    for piece in pieces[:2]:
        piece.finish()
    gain_rows = gains.shape[0] // ex.nf
    both = gains[0:gain_rows, :].astype(F32)
    for f in range(1, ex.nf):
        both = both + gains[gain_rows * f : gain_rows * f + gain_rows, :].astype(F32)
    gain_o[...] = both.astype(BF16)
    g1, g2 = both[0:1], both[1:2]
    gg_o[...] = jnp.zeros_like(gg_o)
    x_load.wait()

    def ident(mb):
        if seqs == 2:
            return 0, 1
        return ids_ref[mb, :, 0:1], ids_ref[mb, :, toks - 1 : toks]

    def ids_of(mb, t):
        return ids_ref[mb, :, pl.ds(pl.multiple_of(t * TILE, TILE), TILE)]

    outs = []

    def emit(src, dst, sem):
        c = pltpu.make_async_copy(src, dst, sem)
        c.start()
        outs.append(c)

    for mb in range(micro):
        acc[...] = jnp.zeros_like(acc)
        first_id, last_id = ident(mb)

        def keys(t, carry, mb=mb):
            r = rows_at(t + mb * tiles, TILE)
            normed, _ = norm_parts(x_ref[r, :].astype(F32))
            low = (normed * g1).astype(BF16)
            a1[r, :] = low
            k = (dot(low, wk[...]) * factor).astype(BF16)
            ks[r, :] = k
            features(k, rbd, fk.at[r, :], feats)
            return carry

        lax.fori_loop(0, tiles, keys, 0)
        if mb == 0:
            pieces[2].forward()
            pieces[2].finish()

        def values(t, carry, mb=mb, last_id=last_id):
            r = rows_at(t + mb * tiles, TILE)
            v = dot(a1[r, :], wv[...]).astype(BF16)
            vv[r, :] = v
            vt = v.T
            mask_t = mask_rows(ids_of(mb, t), last_id)
            for h in range(heads):
                lt = summary_rows(vt[64 * h : 64 * h + 64], None, mask_t)
                acc[h] += dot(lt, fk[r, feats * h : feats * h + feats])
            return carry

        lax.fori_loop(0, tiles, values, 0)
        put_chunks(acc, p_out.at[mb], first_id, last_id, seqs)
        if mb == 0:
            sums[mb].scatter()
    for i, (src, dst) in enumerate(((a1, a1_o), (ks, ks_o), (vv, vv_o), (fk, fk_o))):
        emit(src, dst, o_sem.at[i])
    fk_out = outs.pop()
    pieces[3].forward()
    pieces[3].finish()
    sums[0].spread(sums[0].reduce())

    def queries(t, carry):
        r = rows_at(t, TILE)
        q = (dot(a1[r, :], wq[...]) * factor).astype(BF16)
        qs[r, :] = q
        features(q, rbd, fq.at[r, :], feats)
        return carry

    def queries_and_sums(t, carry):
        @pl.when(t == SCATTER_AT)
        def _():
            for other in sums[1:]:
                other.scatter()

        return queries(t, carry)

    lax.fori_loop(0, micro * tiles, queries_and_sums, 0)
    for piece in pieces[4:6]:
        piece.forward()
    for piece in pieces[4:6]:
        piece.finish()

    dy_load.wait()
    fk_out.wait()
    dh = fk

    def hidden_grads(t, carry):
        r = rows_at(t, TILE)
        dy = dy_ref[r, :]
        for j in range(wd.shape[0] // 256):
            js = slice(256 * j, 256 * j + 256)
            dh[r, js] = dot_nt(dy, wd[js, :]).astype(BF16)
        return carry

    lax.fori_loop(0, micro * tiles, hidden_grads, 0)
    for i, (src, dst) in enumerate(((wq, wq_o), (wk, wk_o), (wv, wv_o))):
        emit(src, dst, o_sem.at[4 + i])
    tiled = ((t_out, out_o), (t_att, att_o), (t_a2, a2_o), (t_hid, hid_o), (t_dpre, dpre_o), (t_dmid, dmid_o), (t_dq, dq_o))

    def tile_copies(t, slot):
        r = rows_at(t, TILE)
        return [pltpu.make_async_copy(src.at[slot], dst.at[r, :], t_sem.at[slot, i]) for i, (src, dst) in enumerate(tiled)]

    for mb in range(micro):
        first_id, last_id = ident(mb)
        sums[mb].finish()
        build_b(p_full.at[mb], b_ref, first_id, last_id, seqs, True)
        acc[...] = jnp.zeros_like(acc)

        def attend(t, carry, mb=mb, last_id=last_id):
            r = rows_at(t + mb * tiles, TILE)
            own = rows_at(t, TILE)
            last = last_lanes(ids_of(mb, t), last_id)
            lane = lax.broadcasted_iota(jnp.int32, (TILE, 128), 1)
            sel = jnp.logical_xor(lane < 64, last)

            def swap(v):
                return jnp.where(last, pltpu.roll(v, 64, 1), v)

            for p in range(pairs):
                base = 2 * feats * p
                ps = slice(128 * p, 128 * p + 128)
                a = dot_nt(fq[r, base : base + feats], b_ref[2 * p])
                b = dot_nt(fq[r, base + feats : base + 2 * feats], b_ref[2 * p + 1])
                inv = 1.0 / jnp.where(sel, a[:, 128:], b[:, 128:])
                att_s[own, ps] = swap(jnp.where(sel, a[:, :128], b[:, :128]) * inv)
                inv_s[own, ps] = swap(inv)
            mix_s[own, :] = x_ref[r, :].astype(F32) + dot(att_s[own, :].astype(BF16), wo[...])
            return carry

        def mid(t, carry, mb=mb, last_id=last_id):
            g = t + mb * tiles
            slot = g % 2
            r = rows_at(g, TILE)

            @pl.when(g >= 2)
            def _():
                for c in tile_copies(g - 2, slot):
                    c.wait()

            if mb == 1:

                @pl.when(t == AR2_AT)
                def _():
                    sums[0].spread_settle()
                    sums[0].spread(sums[0].reduce())

            ids = ids_of(mb, t)
            last = last_lanes(ids, last_id)
            mask_t = mask_rows(ids, last_id)
            lane = lax.broadcasted_iota(jnp.int32, (TILE, 128), 1)
            sel = jnp.logical_xor(lane < 64, last)

            def swap(v):
                return jnp.where(last, pltpu.roll(v, 64, 1), v)

            own = rows_at(t, TILE)
            att, inv, mixed = att_s[own, :], inv_s[own, :], mix_s[own, :]
            t_att[slot] = att.astype(BF16)
            normed, rescale = norm_parts(mixed)
            a2 = (normed * g2).astype(BF16)
            t_a2[slot] = a2
            dy = dy_ref[r, :]
            for j in range(wu.shape[1] // 256):
                js = slice(256 * j, 256 * j + 256)
                pre = dot(a2, wu[:, js])
                cdf = 0.5 * (1.0 + lax.erf(pre * 0.7071067811865476))
                slope = cdf + pre * jnp.exp(-0.5 * pre * pre) * 0.3989422804014327
                t_hid[slot, :, js] = (pre * cdf).astype(BF16)
                t_dpre[slot, :, js] = (dh[r, js].astype(F32) * slope).astype(BF16)
            t_out[slot] = (mixed + dot(t_hid[slot], wd[...])).astype(BF16)
            da2 = dot_nt(t_dpre[slot], wu[...])
            gg_o[...] += jnp.sum(da2 * normed, axis=0, keepdims=True)
            dmid = dy.astype(F32) + norm_back(da2, normed, rescale, g2)
            dmid_low = dmid.astype(BF16)
            t_dmid[slot] = dmid_low
            dnum = dot_nt(dmid_low, wo[...]) * inv
            dpart = -dnum * att
            for p in range(pairs):
                ps = slice(128 * p, 128 * p + 128)
                d, q = dnum[:, ps], dpart[:, ps]
                ds, dp = swap(d), swap(q)
                la = jnp.concatenate([jnp.where(sel, ds, 0.0), jnp.where(sel, dp, 0.0)], axis=1).astype(BF16)
                lb = jnp.concatenate([jnp.where(sel, 0.0, ds), jnp.where(sel, 0.0, dp)], axis=1).astype(BF16)
                base = 2 * feats * p
                fa = fq[r, base : base + feats]
                fb = fq[r, base + feats : base + 2 * feats]
                ga = (dot(la, b_ref[2 * p]) * fa.astype(F32)).astype(BF16)
                gb = (dot(lb, b_ref[2 * p + 1]) * fb.astype(F32)).astype(BF16)
                o = dot(jnp.concatenate([ga, gb], axis=1), rt[p])
                t_dq[slot, :, ps] = (factor * (o[:, :128] - qs[r, ps].astype(F32) * o[:, 128:])).astype(BF16)
                dt = d.astype(BF16).T
                qt = q.T
                for k, f in enumerate((fa, fb)):
                    z = jnp.sum(qt[64 * k : 64 * k + 64], axis=0, keepdims=True)
                    lt = summary_rows(dt[64 * k : 64 * k + 64], z, mask_t)
                    acc[2 * p + k] += dot(lt, f)
            for c in tile_copies(g, slot):
                c.start()
            return carry

        lax.fori_loop(0, tiles, attend, 0)
        if mb == 0:
            for other in sums[1:]:
                other.spread(other.reduce())
            pieces[6].forward()
            pieces[6].finish()
        lax.fori_loop(0, tiles, mid, 0)
        if mb == 0:
            sums[0].scatter_settle()
            put_chunks(acc, p_out.at[0], first_id, last_id, seqs)
            sums[0].scatter()
        else:
            put_chunks(acc, p_o.at[mb - 1], first_id, last_id, seqs)
    sums[0].finish()
    emit(p_full.at[0], s_o, o_sem.at[7])
    last_tile = micro * tiles - 1
    for g in (last_tile - 1, last_tile):
        for c in tile_copies(g, g % 2):
            c.wait()
    for c in outs:
        c.wait()
    for one in sums:
        one.scatter_settle()
        one.spread_settle()
    ex.drain()


def front(x, dy, ids, rand, g1, g2, wk, wv, wq, wo, wu, wd, *, micro, seqs, nf, ns, factor):
    total, width = x.shape
    heads, _, feats = rand.shape
    hidden = wu.shape[1]
    rows = 128 + PAD
    chunks = heads * (seqs // 2)

    def bf(*shape):
        return jax.ShapeDtypeStruct(shape, BF16)

    hbm = pl.BlockSpec(memory_space=pl.ANY)
    vmem = pl.BlockSpec(memory_space=pltpu.VMEM)
    out_shape = [
        bf(total, width), bf(total, width), bf(total, width), bf(total, hidden), bf(total, hidden), bf(total, width),
        bf(total, width), bf(total, width), bf(total, width), bf(total, width), bf(total, heads * feats),
        bf(width, width), bf(width, width), bf(width, width), bf(micro - 1, chunks, rows, feats), bf(ns, rows, feats),
        bf(PAD, width), jax.ShapeDtypeStruct((1, width), F32),
    ]
    v = pltpu.VMEM
    dma = pltpu.SemaphoreType.DMA
    scratch = [v((total, width), BF16)] * 5 + [v((total, heads * feats), BF16), v((total, width), BF16), v((total, heads * feats), BF16)]
    scratch += [v((2, TILE, width), BF16)] * 3 + [v((2, TILE, hidden), BF16)] * 2 + [v((2, TILE, width), BF16)] * 2
    scratch += [v((total // micro, width), F32)] * 3
    scratch += [v((PAD, width), BF16), v((nf * PAD, width), BF16)] + [v((width, width), BF16)] * 4 + [v((width, hidden), BF16), v((hidden, width), BF16)]
    scratch += [v((heads // 4, 256, 4 * feats), BF16), v((heads // 2, 2 * feats, 256), BF16), v((heads, 256, feats), BF16)]
    scratch += [v((heads, rows, feats), F32), v((micro, chunks, rows, feats), BF16)]
    scratch += [v((micro, ns, rows, feats), BF16), v((micro, ns, rows, feats), BF16)]
    kinds = nf - 1
    scratch += [dma((7, kinds)), dma((7, kinds)), dma((7,))] + [dma((micro, ns))] * 4 + [dma((10,)), dma((2, 7))]
    return pl.pallas_call(
        functools.partial(front_kernel, micro=micro, seqs=seqs, factor=factor),
        in_specs=[hbm] * 2 + [vmem] * 4 + [hbm] * 6,
        out_specs=[hbm] * 14 + [vmem, hbm, vmem, vmem],
        out_shape=out_shape,
        scratch_shapes=scratch,
        compiler_params=pltpu.CompilerParams(collective_id=0, has_side_effects=True, vmem_limit_bytes=63 << 20),
        name="front",
    )(x, dy, ids, rand, g1, g2, wk, wv, wq, wo, wu, wd)


class SeqSum:
    def __init__(self, ex, refs, send, recv):
        self.ex, self.send, self.recv = ex, send, recv
        self.out, self.got1, self.mid, self.got2, self.full = refs
        self.fast = ex.ns // 4
        self.z, self.x = ex.s // self.fast, ex.s % self.fast

    def copy(self, phase, k, src, dst, z, x):
        return self.ex.copy(src, dst, self.send.at[phase, k - 1], self.recv.at[phase, k - 1], (z * self.fast + x, self.ex.f))

    def fast_copy(self, phase, k, src, dst):
        return self.copy(phase, k, src, dst, self.z, (self.x + k) % self.fast)

    def slow_copy(self, phase, k, src, dst):
        return self.copy(phase, k, src, dst, (self.z + k) % 4, self.x)

    def block(self, x):
        return pl.ds(x * 4, 4)

    def send1(self):
        for k in range(1, self.fast):

            def make(k=k):
                src = self.out.at[self.block((self.x + k) % self.fast)]
                return self.fast_copy(0, k, src, self.got1.at[k - 1])

            self.ex.launch(make)

    def sum1(self):
        for k in range(1, self.fast):
            self.fast_copy(0, k, self.got1.at[k - 1], self.got1.at[k - 1]).wait_recv()
        total = self.out[self.block(self.x)].astype(F32)
        for k in range(1, self.fast):
            total = total + self.got1[k - 1].astype(F32)
        self.mid[...] = total.astype(BF16)
        for k in (2, 1, 3):
            self.ex.launch(lambda k=k: self.slow_copy(1, k, self.mid.at[(self.z + k) % 4], self.got2.at[k - 1]))

    def sum2(self):
        for k in range(1, 4):
            self.slow_copy(1, k, self.got2.at[k - 1], self.got2.at[k - 1]).wait_recv()
        total = self.mid[self.z].astype(F32)
        for k in range(1, 4):
            total = total + self.got2[k - 1].astype(F32)
        self.full[self.x * 4 + self.z] = total.astype(BF16)
        for k in (2, 1, 3):

            def make(k=k):
                mine = self.full.at[self.x * 4 + self.z]
                return self.slow_copy(2, k, mine, mine)

            self.ex.launch(make)

    def send_fast(self):
        for k in range(1, 4):
            part = self.full.at[self.x * 4 + (self.z + 4 - k) % 4]
            self.slow_copy(2, k, part, part).wait_recv()
        for k in range(1, self.fast):

            def make(k=k):
                mine = self.full.at[self.block(self.x)]
                return self.fast_copy(3, k, mine, mine)

            self.ex.launch(make)

    def finish(self):
        for k in range(1, self.fast):
            part = self.full.at[self.block((self.x + self.fast - k) % self.fast)]
            self.fast_copy(3, k, part, part).wait_recv()


class Reduce:
    def __init__(self, ex, part, rc, ry, seq, send, recv):
        self.ex, self.part, self.rc, self.ry, self.seq, self.send, self.recv = ex, part, rc, ry, seq, send, recv
        self.steps = iter([self.core_sum, self.y_sum, seq.sum1, seq.sum2, seq.send_fast, seq.finish])

    def core_copy(self, yy):
        ex = self.ex
        f = yy * 2 + (1 - ex.c)
        return ex.copy(self.part.at[f], self.rc.at[yy], self.send.at[yy], self.recv.at[yy], (ex.s, ex.partner))

    def core_send(self):
        for yy in range(self.ex.ny):
            self.ex.launch(lambda yy=yy: self.core_copy(yy))

    def y_copy(self, k):
        ex = self.ex
        f = ex.y_to(k)
        j = ex.ny + k - 1
        return ex.copy(self.part.at[f], self.ry.at[k - 1], self.send.at[j], self.recv.at[j], (ex.s, f))

    def core_sum(self):
        ex = self.ex
        for k in range(1, ex.ny):
            yy = (ex.y + k) % ex.ny
            f = ex.y_to(k)
            self.core_copy(yy).wait_recv()
            self.part[f] = (self.part[f].astype(F32) + self.rc[yy].astype(F32)).astype(BF16)
            ex.launch(lambda k=k: self.y_copy(k))

    def y_sum(self):
        ex = self.ex
        self.core_copy(ex.y).wait_recv()
        total = self.part[ex.f].astype(F32) + self.rc[ex.y].astype(F32)
        for k in range(1, ex.ny):
            self.y_copy(k).wait_recv()
            total = total + self.ry[k - 1].astype(F32)
        self.seq.out[...] = total.astype(BF16)
        self.seq.send1()


PIECES = 6


def back_kernel(
    x_in, dy_in, hid_in, dpre_in, a2_in, att_in, dmid_in, dq_in, a1_in, ks_in, vv_in, fk_in, wq_in, wk_in, wv_in,
    ids_ref, rand_ref, gain_ref, gg_ref, p0_ref, p1_ref,
    dx_o, g1_o, g2_o, res_o,
    x, dy, blk, a2, att, dmid, dq, a1, ks, vv, fk, wq, wk, wv, dk, dv, tr, t_dx, rbd, rt, b_ref,
    p_got, p_full, part, rc, ry, s_out, s_got1, s_mid, s_got2,
    gs, gr,
    l_sem, b_sem, x_sem, r_send, r_recv, g_send, g_recv, c_send, c_recv, t_send, t_recv, n_send, n_recv,
    *, micro, seqs, factor,
):
    ex = Exchange()
    heads, _, feats = rand_ref.shape
    total_rows, width = x.shape
    toks = total_rows // micro
    tiles = toks // TILE
    pairs = width // 128
    hidden = hid_in.shape[1]
    blocks = hidden // 512
    quarter = ex.ns // 4
    chunk = res_o.shape[2]
    shard = quarter * chunk
    kv_sum = Sum(ex, p1_ref, p_got, p_full, (r_send, r_recv, g_send, g_recv), seqs)

    ex.greet()
    loads = {}
    order = (
        ("att", att_in, att), ("dmid", dmid_in, dmid), ("a1", a1_in, a1), ("dq", dq_in, dq), ("dy", dy_in, dy), ("a2", a2_in, a2),
        ("vv", vv_in, vv), ("fk", fk_in, fk), ("ks", ks_in, ks), ("wq", wq_in, wq), ("wk", wk_in, wk), ("wv", wv_in, wv),
        ("x", x_in, x),
    )

    def block_copy(src, b):
        return pltpu.make_async_copy(src.at[:, pl.ds(pl.multiple_of(b * 512, 512), 512)], blk.at[b], b_sem.at[b])

    for i, (name, src, dst) in enumerate(order):
        loads[name] = pltpu.make_async_copy(src, dst, l_sem.at[i])
        loads[name].start()
        if name == "dy":
            for b in range(blocks):
                block_copy(hid_in, b).start()

    def need(*names):
        for name in names:
            loads.pop(name).wait()

    ex.meet()
    kv_sum.scatter()
    pieces = []
    for i in range(PIECES):
        seq = SeqSum(ex, (s_out.at[i], s_got1.at[i], s_mid.at[i], s_got2.at[i], res_o.at[i]), t_send.at[i], t_recv.at[i])
        pieces.append(Reduce(ex, part.at[i], rc.at[i], ry.at[i], seq, c_send.at[i], c_recv.at[i]))
    q, d1, d2, u1, u2, k = pieces

    def go(*which):
        for one in which:
            next(one.steps)()

    def go_at(t, plan):
        for when, which in plan.items():

            @pl.when(t == when)
            def _(which=which):
                go(*which)

    def small(left_t, right, piece, which):
        v = dot(left_t, right)
        for half in range(2):
            for f in range(ex.nf):
                one = v[f * shard : (f + 1) * shard, 256 * half : 256 * half + 256].reshape(quarter, chunk, 256)
                piece.part[f, quarter * (2 * which + half) : quarter * (2 * which + half + 1)] = one.astype(BF16)

    need("att", "dmid")
    small(att[...].T, dmid[...], q, 1)
    need("a1", "dq")
    small(a1[...].T, dq[...], q, 0)
    q.core_send()
    need("dy")
    tr[...] = dy[...].T
    per = 512 // chunk // ex.ns

    def down_block(i, carry):
        b = (i + (ex.y + 1) % ex.ny * (blocks // ex.ny)) % blocks
        block_copy(hid_in, b).wait()
        v = dot(tr[...], blk[b]).T
        block_copy(dpre_in, b).start()
        for half, piece in enumerate((d1, d2)):
            one = v[:, 256 * half : 256 * half + 256].reshape(512 // chunk, chunk, 256).astype(BF16)
            for j in range(per):
                f = b * per + j
                piece.part[f] = one[j * ex.ns : (j + 1) * ex.ns]

                @pl.when(f % 2 != ex.c)
                def _(f=f, piece=piece):
                    piece.core_copy(f // 2).start()

        go_at(i, {1: (q,)})
        return carry

    lax.fori_loop(0, blocks, down_block, 0)
    for piece in (d1, d2):
        ex.pending += [lambda yy=yy, piece=piece: piece.core_copy(yy) for yy in range(ex.ny)]
    kv_sum.spread(kv_sum.reduce())
    go(d1, d2)
    build_features(rand_ref, rbd, rt)
    need("a2")
    tr[...] = a2[...].T

    def up_block(b, carry):
        block_copy(dpre_in, b).wait()
        v = dot(tr[...], blk[b])
        for half in range(2):
            for f in range(ex.nf):
                one = v[f * shard : (f + 1) * shard, 256 * half : 256 * half + 256].reshape(quarter, chunk, 256)
                part[3 + b // 2, f, pl.ds((b % 2 * 2 + half) * quarter, quarter)] = one.astype(BF16)

        @pl.when(b == 1)
        def _():
            u1.core_send()

        go_at(b, {2: (q,), 3: (u1,)})
        return carry

    lax.fori_loop(0, blocks, up_block, 0)
    u2.core_send()
    tr[...] = a1[...].T
    need("vv", "fk", "ks")

    def ident(mb):
        if seqs == 2:
            return 0, 1
        return ids_ref[mb, :, 0:1], ids_ref[mb, :, toks - 1 : toks]

    def kv_part(mb, full, plan):
        first_id, last_id = ident(mb)
        build_b(full, b_ref, first_id, last_id, seqs, False)

        def body(t, carry):
            r = rows_at(t + mb * tiles, TILE)
            ids = ids_ref[mb, :, pl.ds(pl.multiple_of(t * TILE, TILE), TILE)]
            last = last_lanes(ids, last_id)
            lane = lax.broadcasted_iota(jnp.int32, (TILE, 128), 1)
            sel = jnp.logical_xor(lane < 64, last)
            ones_a = jnp.where(sel, 1.0, 0.0).astype(BF16)
            ones_b = jnp.where(sel, 0.0, 1.0).astype(BF16)

            def swap(v):
                return jnp.where(last, pltpu.roll(v, 64, 1), v)

            for p in range(pairs):
                ps = slice(128 * p, 128 * p + 128)
                v = swap(vv[r, ps].astype(F32))
                la = jnp.concatenate([jnp.where(sel, v, 0.0).astype(BF16), ones_a], axis=1)
                lb = jnp.concatenate([jnp.where(sel, 0.0, v).astype(BF16), ones_b], axis=1)
                base = 2 * feats * p
                fa = fk[r, base : base + feats]
                fb = fk[r, base + feats : base + 2 * feats]
                ga = (dot(la, b_ref[2 * p]) * fa.astype(F32)).astype(BF16)
                gb = (dot(lb, b_ref[2 * p + 1]) * fb.astype(F32)).astype(BF16)
                o = dot(jnp.concatenate([ga, gb], axis=1), rt[p])
                dk[r, ps] = (factor * (o[:, :128] - ks[r, ps].astype(F32) * o[:, 128:])).astype(BF16)
                va = dot_nt(fa, b_ref[2 * p, :128])
                vb = dot_nt(fb, b_ref[2 * p + 1, :128])
                dv[r, ps] = swap(jnp.where(sel, va, vb)).astype(BF16)
            go_at(t, plan)
            return carry

        lax.fori_loop(0, tiles, body, 0)

    g1 = gain_ref[0:1].astype(F32)
    gs[...] = jnp.zeros_like(gs)
    gs[0, 1:2, :] = gg_ref[...]

    def dx_copy(g, slot):
        return pltpu.make_async_copy(t_dx.at[slot], dx_o.at[rows_at(g, TILE), :], x_sem.at[slot])

    def x_part(mb, plan):
        def body(t, carry):
            g = t + mb * tiles
            slot = g % 2
            r = rows_at(g, TILE)

            @pl.when(g >= 2)
            def _():
                dx_copy(g - 2, slot).wait()

            da1 = dot_nt(dq[r, :], wq[...]) + dot_nt(dk[r, :], wk[...]) + dot_nt(dv[r, :], wv[...])
            normed, rescale = norm_parts(x[r, :].astype(F32))
            gs[0, 0:1, :] += jnp.sum(da1 * normed, axis=0, keepdims=True)
            t_dx[slot] = (dmid[r, :].astype(F32) + norm_back(da1, normed, rescale, g1)).astype(BF16)
            dx_copy(g, slot).start()
            go_at(t, plan)
            return carry

        lax.fori_loop(0, tiles, body, 0)

    kv_part(0, p0_ref, {0: (u2,), 1: (d1, q), 2: ()})
    kv_sum.finish()
    kv_part(1, p_full, {1: (d1, d2, q)})
    small(tr[...], dk[...], k, 0)
    small(tr[...], dv[...], k, 1)
    k.core_send()
    go(u1, d2, d1)
    need("wq", "wk", "wv", "x")
    x_part(0, {1: (k, q), 2: (u1, u2)})
    x_part(1, {0: (d2,), 2: (q, d1)})
    def gain_copy(level, j, peer):
        return ex.copy(gs.at[level], gr.at[j], n_send.at[j], n_recv.at[j], peer)

    def gain_level(level, jobs):
        for j, peer in jobs:
            gain_copy(level, j, peer).start()
        return jobs

    def gain_sum(level, jobs):
        total = gs[level]
        for j, peer in jobs:
            gain_copy(level, j, peer).wait_recv()
            total = total + gr[j]
        return total

    jobs0 = gain_level(0, [(0, (ex.s, ex.partner))])
    go(k, u2, u1)
    gs[1] = gain_sum(0, jobs0)
    jobs1 = gain_level(1, [(k, (ex.s, ex.y_to(k))) for k in range(1, ex.ny)])
    go(d1, d2, k, u2)
    gs[2] = gain_sum(1, jobs1)
    jobs2 = gain_level(2, [(ex.ny - 1 + k, ex.seq_peer(k)) for k in range(1, ex.ns)])
    go(d2, u1, k, u1, u2)
    gains = gain_sum(2, jobs2)
    mine = jnp.zeros((gains.shape[0], shard), F32)
    for f in range(ex.nf):
        mine = mine + jnp.where(ex.f == f, gains[:, f * shard : f * shard + shard], 0.0)
    g1_o[...] = mine[0:1]
    g2_o[...] = mine[1:2]
    go(k, u2, k)
    for piece in pieces:
        assert next(piece.steps, None) is None
    last = micro * tiles - 1
    for g in (last - 1, last):
        dx_copy(g, g % 2).wait()
    for level, jobs in enumerate((jobs0, jobs1, jobs2)):
        for j, peer in jobs:
            gain_copy(level, j, peer).wait_send()
    kv_sum.scatter_settle()
    kv_sum.spread_settle()
    ex.drain()


def back(big, small, *, micro, seqs, nf, ns, shard, factor):
    x, _, hid = big[:3]
    rand = small[1]
    total, width = x.shape
    heads, _, feats = rand.shape
    rows = 128 + PAD
    hidden = hid.shape[1]
    ny = nf // 2
    slow = 4
    fast = ns // slow
    chunk = 4 * shard // ns
    hbm = pl.BlockSpec(memory_space=pl.ANY)
    vmem = pl.BlockSpec(memory_space=pltpu.VMEM)
    v = pltpu.VMEM
    dma = pltpu.SemaphoreType.DMA

    def f32(*shape):
        return jax.ShapeDtypeStruct(shape, F32)

    out_shape = [jax.ShapeDtypeStruct((total, width), BF16), f32(1, shard), f32(1, shard)]
    out_shape += [jax.ShapeDtypeStruct((PIECES, ns, chunk, 256), BF16)]
    token = v((total, width), BF16)
    scratch = [token, token, v((hidden // 512, total, 512), BF16), token, token, token, token, token, token, token]
    scratch += [v((total, heads * feats), BF16)] + [v((width, width), BF16)] * 3 + [token, token, v((width, total), BF16)]
    scratch += [v((2, TILE, width), BF16), v((heads // 4, 256, 4 * feats), BF16), v((heads // 2, 2 * feats, 256), BF16)]
    scratch += [v((heads, 256, feats), BF16), v((ns, rows, feats), BF16), v((ns, rows, feats), BF16)]
    for lead in ((nf, ns), (ny, ns), (ny - 1, ns), (ns,), (fast - 1, slow), (slow,), (slow - 1,)):
        scratch.append(v((PIECES, *lead, chunk, 256), BF16))
    jobs = 1 + (ny - 1) + (ns - 1)
    scratch += [v((3, 8, width), F32), v((jobs, 8, width), F32)]
    peers = max(fast, slow) - 1
    scratch += [dma((13,)), dma((hidden // 512,)), dma((2,)), *([dma((ns,))] * 4)]
    scratch += [dma((PIECES, 2 * ny - 1))] * 2 + [dma((PIECES, 4, peers))] * 2 + [dma((jobs,))] * 2
    return pl.pallas_call(
        functools.partial(back_kernel, micro=micro, seqs=seqs, factor=factor),
        in_specs=[hbm] * len(big) + [vmem] * len(small),
        out_specs=[hbm] + [vmem] * 3,
        out_shape=out_shape,
        scratch_shapes=scratch,
        compiler_params=pltpu.CompilerParams(collective_id=1, has_side_effects=True, vmem_limit_bytes=63 << 20),
        name="back",
    )(*big, *small)


def results_kernel(out, dx, q, d1, d2, u1, u2, k, g1, g2, out_o, dx_o, wq, wo, wk, wv, wu, wd, g1_o, g2_o):
    out_o[...] = out[...]
    dx_o[...] = dx[...]
    g1_o[...] = g1[...]
    g2_o[...] = g2[...]

    def wide(a):
        a = a.astype(F32)
        return a.reshape(a.shape[0] * a.shape[1], a.shape[2])

    wd[:, :256] = wide(d1[...])
    wd[:, 256:] = wide(d2[...])
    step = pl.program_id(0)

    def up(piece):
        half = piece.shape[0] // 2
        wu[:, :256] = wide(piece[:half])
        wu[:, 256:] = wide(piece[half:])

    @pl.when(step < 2)
    def _():
        wq[...] = wide(q[...])
        wk[...] = wide(k[...])
        up(u1)

    @pl.when(step >= 2)
    def _():
        wo[...] = wide(q[...])
        wv[...] = wide(k[...])
        up(u2)


def results(out, dx, res, g1, g2, shard):
    total, width = out.shape
    _, ns, chunk, cols = res.shape
    quarter = ns // 4
    rows = pl.BlockSpec((total // 4, width), lambda i: (i, 0))
    gain = pl.BlockSpec((1, shard), lambda i: (0, 0))

    def piece(g):
        return pl.BlockSpec((None, quarter, chunk, cols), lambda i: (g, i, 0, 0))

    def low(i):
        return jnp.minimum(i, 1)

    def high(i):
        return jnp.maximum(i - 2, 0)

    def wider(g, of):
        return pl.BlockSpec((None, 2 * quarter, chunk, cols), lambda i: (g, of(i), 0, 0))

    first = pl.BlockSpec((shard, cols), lambda i: (0, low(i)))
    second = pl.BlockSpec((shard, cols), lambda i: (0, high(i)))
    half = jax.ShapeDtypeStruct((shard, 2 * cols), F32)
    token = jax.ShapeDtypeStruct((total, width), BF16)
    gain_shape = jax.ShapeDtypeStruct((1, shard), F32)
    return pl.pallas_call(
        results_kernel,
        grid=(4,),
        in_specs=[rows, rows, piece(0), piece(1), piece(2), wider(3, low), wider(4, high), piece(5), gain, gain],
        out_specs=[rows, rows, first, second, first, second]
        + [pl.BlockSpec((shard, 2 * cols), lambda i: (0, i)), pl.BlockSpec((shard, 2 * cols), lambda i: (i, 0)), gain, gain],
        out_shape=[token, token, half, half, half, half]
        + [jax.ShapeDtypeStruct((shard, 8 * cols), F32), jax.ShapeDtypeStruct((4 * shard, 2 * cols), F32), gain_shape, gain_shape],
        name="results",
    )(out, dx, res, res, res, res, res, res, g1, g2)


def per_device(block_input, seq_ids, rand, ln1_gain, w_query, w_key, w_value, w_out, ln2_gain, w_up, w_down, cotangent):
    micro, _, toks, width = block_input.shape
    heads, dim, feats = rand.shape
    factor = dim ** (-0.25)
    ns, nf = lax.axis_size("seq"), lax.axis_size("fsdp")
    seqs = max(2, ns // 4)
    x = block_input.reshape(micro * toks, width)
    dy = cotangent.reshape(micro * toks, width)
    shard = ln1_gain.shape[0]
    out, att, a2, hid, dpre, dmid, dq, a1, ks, vv, fk, wq, wk, wv, part, total, gains, gg = front(
        x, dy, seq_ids, rand, ln1_gain.reshape(1, shard), ln2_gain.reshape(1, shard), w_key, w_value, w_query, w_out, w_up, w_down,
        micro=micro, seqs=seqs, nf=nf, ns=ns, factor=factor,
    )
    dx, g1g, g2g, res = back(
        [x, dy, hid, dpre, a2, att, dmid, dq, a1, ks, vv, fk, wq, wk, wv],
        [seq_ids, rand, gains, gg, total, part[0]],
        micro=micro, seqs=seqs, nf=nf, ns=ns, shard=shard, factor=factor,
    )
    shape = block_input.shape
    out, dx, wqg, wog, wkg, wvg, wug, wdg, g1g, g2g = results(out, dx, res, g1g, g2g, shard)
    return (out.reshape(shape), dx.reshape(shape), g1g[0], wqg, wkg, wvg, wog, g2g[0], wug, wdg)


def solution(mesh):
    tok = P(None, "fsdp", "seq", None)
    vec, mat = P("fsdp"), P("fsdp", None)
    return jax.shard_map(
        per_device,
        mesh=mesh,
        in_specs=(tok, P(None, "fsdp", "seq"), P(), vec, mat, mat, mat, mat, vec, mat, mat, tok),
        out_specs=(tok, tok, vec, mat, mat, mat, mat, vec, mat, mat),
        check_vma=False,
    )
```

```python
import functools
import math

import jax
import jax.numpy as jnp
from jax import lax
from jax.experimental import pallas as pl
from jax.experimental.pallas import tpu as pltpu
from jax.sharding import PartitionSpec as P

EPS = 1e-05
TILE = 256
F32 = jnp.float32
BF16 = jnp.bfloat16
PAD = 16
SCATTER_AT = 5
AR2_AT = 1


def dot(a, b):
    return lax.dot_general(a, b, (((1,), (0,)), ((), ())), preferred_element_type=F32)


def dot_nt(a, b):
    return lax.dot_general(a, b, (((1,), (1,)), ((), ())), preferred_element_type=F32)


def norm_parts(v):
    c = v - jnp.mean(v, axis=-1, keepdims=True)
    r = lax.rsqrt(jnp.mean(c * c, axis=-1, keepdims=True) + EPS)
    return c * r, r


def norm_back(grad, normed, rescale, gain):
    e = grad * gain
    return rescale * (
        e
        - jnp.mean(e, axis=-1, keepdims=True)
        - normed * jnp.mean(e * normed, axis=-1, keepdims=True)
    )


def features(scaled, rbd_ref, feat_ref, feats):
    lane = lax.broadcasted_iota(jnp.int32, (scaled.shape[0], 128), 1)
    low = lane < 64
    log_scale = 0.5 * math.log(feats)
    as_float = scaled.astype(F32)
    for quad in range(scaled.shape[1] // 256):
        u = dot(scaled[:, 256 * quad : 256 * quad + 256], rbd_ref[quad])
        for pair in range(2):
            s = as_float[:, 256 * quad + 128 * pair : 256 * quad + 128 * pair + 128]
            s = s * s
            sq_a = jnp.sum(jnp.where(low, s, 0.0), axis=-1, keepdims=True)
            sq_b = jnp.sum(jnp.where(low, 0.0, s), axis=-1, keepdims=True)
            for k, sq in enumerate((sq_a, sq_b)):
                col = feats * (2 * pair + k)
                f = jnp.exp(u[:, col : col + feats] - (0.5 * sq + log_scale))
                base = feats * (4 * quad + 2 * pair + k)
                feat_ref[:, base : base + feats] = f.astype(BF16)


def summary_rows(rows, zrow, mask_t):
    z = mask_t if zrow is None else (mask_t.astype(F32) * zrow).astype(BF16)
    return jnp.concatenate([rows * mask_t[0:1], z, rows * mask_t[1:2]], axis=0)


MESH_ID = pl.DeviceIdType.MESH


def rows_at(index, size):
    return pl.ds(pl.multiple_of(index * size, size), size)


class Exchange:
    def __init__(self):
        self.s, self.f = lax.axis_index("seq"), lax.axis_index("fsdp")
        self.ns, self.nf = lax.axis_size("seq"), lax.axis_size("fsdp")
        self.ny = self.nf // 2
        self.y, self.c = self.f // 2, self.f % 2
        self.partner = self.y * 2 + (1 - self.c)
        self.pending = []

    def seq_peer(self, k):
        return ((self.s + k) % self.ns, self.f)

    def y_from(self, k):
        return ((self.y + self.ny - k) % self.ny) * 2 + self.c

    def y_to(self, k):
        return ((self.y + k) % self.ny) * 2 + self.c

    def greet(self):
        sem = pltpu.get_barrier_semaphore()
        peers = [self.seq_peer(k) for k in range(1, self.ns)]
        peers += [(self.s, self.partner)] + [(self.s, self.y_to(k)) for k in range(1, self.ny)]
        for peer in peers:
            pl.semaphore_signal(sem, inc=1, device_id=peer, device_id_type=MESH_ID)
        self.peers = len(peers)

    def meet(self):
        pl.semaphore_wait(pltpu.get_barrier_semaphore(), self.peers)

    def barrier(self):
        self.greet()
        self.meet()

    def copy(self, src, dst, send, recv, peer):
        return pltpu.make_async_remote_copy(
            src_ref=src, dst_ref=dst, send_sem=send, recv_sem=recv, device_id=peer, device_id_type=MESH_ID
        )

    def start(self, *args):
        self.launch(lambda: self.copy(*args))

    def launch(self, make):
        make().start()
        self.pending.append(make)

    def drain(self):
        for make in self.pending:
            make().wait_send()
        self.pending = []


class Gather:
    def __init__(self, ex, shard, full, send, recv, local):
        self.ex, self.shard, self.full, self.send, self.recv = ex, shard, full, send, recv
        self.rows = shard.shape[0]
        self.own = pltpu.make_async_copy(shard, self.part(ex.f), local)

    def part(self, f):
        return self.full.at[rows_at(f, self.rows), :]

    def begin(self):
        ex = self.ex
        for k in range(1, ex.ny):
            ex.start(self.shard, self.part(ex.f), self.send.at[k], self.recv.at[k], (ex.s, ex.y_to(k)))
        ex.start(self.shard, self.part(ex.f), self.send.at[0], self.recv.at[0], (ex.s, ex.partner))
        self.own.start()

    def forward(self):
        ex = self.ex
        for k in range(1, ex.ny):
            part = self.part(ex.y_from(k))
            ex.copy(part, part, self.send.at[k], self.recv.at[k], (ex.s, ex.f)).wait_recv()
            j = ex.ny - 1 + k
            ex.start(part, part, self.send.at[j], self.recv.at[j], (ex.s, ex.partner))

    def finish(self):
        ex = self.ex
        part = self.part(ex.partner)
        ex.copy(part, part, self.send.at[0], self.recv.at[0], (ex.s, ex.f)).wait_recv()
        for k in range(1, ex.ny):
            j = ex.ny - 1 + k
            part = self.part(((ex.y + ex.ny - k) % ex.ny) * 2 + 1 - ex.c)
            ex.copy(part, part, self.send.at[j], self.recv.at[j], (ex.s, ex.f)).wait_recv()
        self.own.wait()


class Sum:
    def __init__(self, ex, out, got, full, sems, seqs):
        self.ex, self.out, self.got, self.full = ex, out, got, full
        self.s1, self.r1, self.s2, self.r2 = sems
        self.sparse = seqs == 2
        self.edge = ex.ns // (2 * seqs)
        if self.sparse:
            got[...] = jnp.zeros_like(got)
            full[...] = jnp.zeros_like(full)

    def holds(self, chunk, device):
        return device < self.ex.ns - self.edge if chunk < self.ex.ns // 2 else device >= self.edge

    def chunks_of(self, device):
        return self.order(device, [o for o in range(self.ex.ns) if o != device and self.holds(o, device)])

    def devices_of(self, chunk):
        return self.order(chunk, [d for d in range(self.ex.ns) if d != chunk and self.holds(chunk, d)])

    def order(self, device, others):
        return sorted(others, key=lambda d: (-abs(d // 2 - device // 2), (d - device) % self.ex.ns))

    def each(self, peers, body):
        ex = self.ex
        if not self.sparse:
            for k in range(1, ex.ns):
                body((ex.s + k) % ex.ns)
            return
        for device in range(ex.ns):

            @pl.when(ex.s == device)
            def _(device=device):
                for peer in peers(device):
                    body(peer)

    def out_copy(self, peer):
        ex = self.ex
        return ex.copy(self.out.at[peer], self.got.at[ex.s], self.s1.at[peer], self.r1.at[ex.s], (peer, ex.f))

    def got_copy(self, peer):
        ref = self.got.at[peer]
        return self.ex.copy(ref, ref, self.s1.at[peer], self.r1.at[peer], (peer, self.ex.f))

    def spread_copy(self, peer):
        ex = self.ex
        ref = self.full.at[ex.s]
        return ex.copy(ref, ref, self.s2.at[peer], self.r2.at[ex.s], (peer, ex.f))

    def full_copy(self, peer):
        ref = self.full.at[peer]
        return self.ex.copy(ref, ref, self.s2.at[peer], self.r2.at[peer], (peer, self.ex.f))

    def scatter(self):
        self.each(self.chunks_of, lambda p: self.out_copy(p).start())

    def scatter_settle(self):
        self.each(self.chunks_of, lambda p: self.out_copy(p).wait_send())

    def reduce(self):
        ex = self.ex
        self.each(self.devices_of, lambda p: self.got_copy(p).wait_recv())
        total = self.out[ex.s].astype(F32)
        for k in range(ex.ns) if self.sparse else range(1, ex.ns):
            total = total + self.got[k if self.sparse else (ex.s + k) % ex.ns].astype(F32)
        return total.astype(BF16)

    def spread(self, total):
        self.full[self.ex.s] = total
        self.each(self.devices_of, lambda p: self.spread_copy(p).start())

    def spread_settle(self):
        self.each(self.devices_of, lambda p: self.spread_copy(p).wait_send())

    def finish(self):
        self.each(self.chunks_of, lambda p: self.full_copy(p).wait_recv())


def mask_rows(ids, last_id):
    last = (ids == last_id).astype(F32)
    row = lax.broadcasted_iota(jnp.int32, (PAD, ids.shape[1]), 0)
    return jnp.where(row == 0, 1.0 - last, jnp.where(row == 1, last, 0.0)).astype(BF16)


def last_lanes(ids, last_id):
    last = (ids == last_id).astype(F32)
    return jnp.broadcast_to(last, (128, ids.shape[1])).T > 0.5


def put_chunks(acc_ref, out_ref, first_id, last_id, seqs):
    heads = acc_ref.shape[0]
    if seqs == 2:
        owners = out_ref.shape[0] // 2
        per = heads // owners
        row = lax.broadcasted_iota(jnp.int32, (PAD, acc_ref.shape[2]), 0)
        for i in range(out_ref.shape[0]):
            slot, base = i // owners, per * (i % owners)
            at = (64 + PAD) * slot
            z = jnp.zeros(row.shape, F32)
            for j in range(per):
                z = jnp.where(row == j, acc_ref[base + j, 64 + slot : 65 + slot], z)
            rows = [acc_ref[base + j, at : at + 64] for j in range(per)]
            out_ref[i] = jnp.concatenate([*rows, z], axis=0).astype(BF16)
        return
    groups = seqs // 2

    def body(h, carry):
        a = acc_ref[h]
        v1, v2, z1, z2 = a[:64], a[64 + PAD :], a[64:65], a[65:66]
        row = lax.broadcasted_iota(jnp.int32, (PAD, a.shape[1]), 0)
        for g in range(groups):
            f0, f1 = (jnp.where(first_id == 2 * g + k, 1.0, 0.0) for k in range(2))
            l0, l1 = (jnp.where(last_id == 2 * g + k, 1.0, 0.0) for k in range(2))
            z = jnp.where(row == 0, f0 * z1 + l0 * z2, jnp.where(row == 1, f1 * z1 + l1 * z2, 0.0))
            out_ref[h * groups + g] = jnp.concatenate([f0 * v1 + l0 * v2, z, f1 * v1 + l1 * v2], axis=0).astype(BF16)
        return carry

    lax.fori_loop(0, heads, body, 0)


def take_slots(full_ref, h, heads, first_id, last_id, seqs):
    if seqs == 2:
        owners = full_ref.shape[0] // 2
        per = heads // owners
        j = h % per
        a, b = (full_ref[k * owners + h // per].astype(F32) for k in range(2))
        z = 64 * per + j
        return a[64 * j : 64 * j + 64], b[64 * j : 64 * j + 64], a[z : z + 1], b[z : z + 1]
    groups = seqs // 2
    picks = [None] * 4
    for g in range(groups):
        a = full_ref[h * groups + g].astype(F32)
        for k in range(2):
            rows, z = a[(64 + PAD) * k : (64 + PAD) * k + 64], a[64 + k : 65 + k]
            for which, ident in enumerate((first_id, last_id)):
                hit = ident == 2 * g + k
                for slot, v in ((which, rows), (2 + which, z)):
                    term = jnp.where(hit, v, 0.0)
                    picks[slot] = term if picks[slot] is None else picks[slot] + term
    return picks


def build_b(full_ref, b_ref, first_id, last_id, seqs, repeat):
    for h in range(b_ref.shape[0]):
        r1, r2, z1, z2 = take_slots(full_ref, h, b_ref.shape[0], first_id, last_id, seqs)
        if h % 2:
            r1, r2, z1, z2 = r2, r1, z2, z1
        shape = r1.shape
        if repeat:
            z1, z2 = (jnp.broadcast_to(z, shape) for z in (z1, z2))
        else:
            top = lax.broadcasted_iota(jnp.int32, shape, 0) == 0
            z1, z2 = (jnp.where(top, jnp.broadcast_to(z, shape), 0.0) for z in (z1, z2))
        b_ref[h] = jnp.concatenate([r1, r2, z1, z2], axis=0).astype(BF16)


def build_features(rand_ref, rbd_ref, rt_ref):
    heads, dim, feats = rand_ref.shape
    rbd_ref[...] = jnp.zeros_like(rbd_ref)
    lane = lax.broadcasted_iota(jnp.int32, (feats, 128), 1)
    for h in range(heads):
        q, k = h // 4, h % 4
        rbd_ref[q, dim * k : dim * k + dim, feats * k : feats * k + feats] = rand_ref[h]
    for p in range(heads // 2):
        both = jnp.concatenate([rand_ref[2 * p], rand_ref[2 * p + 1]], axis=0).astype(F32).T
        for k in range(2):
            mine = (lane < 64) if k == 0 else (lane >= 64)
            left = jnp.where(mine, both, 0.0)
            right = jnp.where(mine, 1.0, 0.0)
            rt_ref[p, feats * k : feats * k + feats, :] = jnp.concatenate([left, right], axis=1).astype(BF16)


TILED_OUT = ("out", "att", "a2", "hid", "dpre", "dmid", "dq")


def front_kernel(
    x_in, dy_in, ids_ref, rand_ref, g1_in, g2_in, wk_in, wv_in, wq_in, wo_in, wu_in, wd_in,
    out_o, att_o, a2_o, hid_o, dpre_o, dmid_o, dq_o, a1_o, ks_o, vv_o, fk_o, wq_o, wk_o, wv_o, p_o, s_o, gain_o, gg_o,
    x_ref, dy_ref,
    a1, ks, vv, fk, qs, fq, t_out, t_att, t_a2, t_hid, t_dpre, t_dmid, t_dq, att_s, inv_s, mix_s,
    gains_in, gains, wk, wv, wq, wo, wu, wd, rbd, rt, b_ref, acc, p_out, p_got, p_full,
    w_send, w_recv, w_local, r_send, r_recv, g_send, g_recv, o_sem, t_sem,
    *, micro, seqs, factor,
):
    ex = Exchange()
    heads, _, feats = rand_ref.shape
    total, width = x_in.shape
    x_load = pltpu.make_async_copy(x_in, x_ref, o_sem.at[8])
    dy_load = pltpu.make_async_copy(dy_in, dy_ref, o_sem.at[9])
    x_load.start()
    dy_load.start()
    toks = total // micro
    tiles = toks // TILE
    pairs = width // 128
    sums = [
        Sum(ex, p_out.at[mb], p_got.at[mb], p_full.at[mb], (r_send.at[mb], r_recv.at[mb], g_send.at[mb], g_recv.at[mb]), seqs)
        for mb in range(micro)
    ]
    ex.greet()
    place = lax.broadcasted_iota(jnp.int32, (1, width), 1) // g1_in.shape[1] == ex.f
    gains_in[...] = jnp.zeros_like(gains_in)
    for i, g in enumerate((g1_in, g2_in)):
        wide = jnp.concatenate([g[...].astype(F32)] * ex.nf, axis=1)
        gains_in[i : i + 1, :] = jnp.where(place, wide, 0.0).astype(BF16)
    ex.meet()
    pieces = []
    for i, (shard, full) in enumerate(
        ((gains_in, gains), (wk_in, wk), (wv_in, wv), (wq_in, wq), (wo_in, wo), (wd_in, wd), (wu_in, wu))
    ):
        pieces.append(Gather(ex, shard, full, w_send.at[i], w_recv.at[i], w_local.at[i]))
    for piece in pieces:
        piece.begin()
    build_features(rand_ref, rbd, rt)
    for piece in pieces[:2]:
        piece.forward()
    for piece in pieces[:2]:
        piece.finish()
    gain_rows = gains.shape[0] // ex.nf
    both = gains[0:gain_rows, :].astype(F32)
    for f in range(1, ex.nf):
        both = both + gains[gain_rows * f : gain_rows * f + gain_rows, :].astype(F32)
    gain_o[...] = both.astype(BF16)
    g1, g2 = both[0:1], both[1:2]
    gg_o[...] = jnp.zeros_like(gg_o)
    x_load.wait()

    def ident(mb):
        if seqs == 2:
            return 0, 1
        return ids_ref[mb, :, 0:1], ids_ref[mb, :, toks - 1 : toks]

    def ids_of(mb, t):
        return ids_ref[mb, :, pl.ds(pl.multiple_of(t * TILE, TILE), TILE)]

    outs = []

    def emit(src, dst, sem):
        c = pltpu.make_async_copy(src, dst, sem)
        c.start()
        outs.append(c)

    for mb in range(micro):
        acc[...] = jnp.zeros_like(acc)
        first_id, last_id = ident(mb)

        def keys(t, carry, mb=mb):
            r = rows_at(t + mb * tiles, TILE)
            normed, _ = norm_parts(x_ref[r, :].astype(F32))
            low = (normed * g1).astype(BF16)
            a1[r, :] = low
            k = (dot(low, wk[...]) * factor).astype(BF16)
            ks[r, :] = k
            features(k, rbd, fk.at[r, :], feats)
            return carry

        lax.fori_loop(0, tiles, keys, 0)
        if mb == 0:
            pieces[2].forward()
            pieces[2].finish()

        def values(t, carry, mb=mb, last_id=last_id):
            r = rows_at(t + mb * tiles, TILE)
            v = dot(a1[r, :], wv[...]).astype(BF16)
            vv[r, :] = v
            vt = v.T
            mask_t = mask_rows(ids_of(mb, t), last_id)
            for h in range(heads):
                lt = summary_rows(vt[64 * h : 64 * h + 64], None, mask_t)
                acc[h] += dot(lt, fk[r, feats * h : feats * h + feats])
            return carry

        lax.fori_loop(0, tiles, values, 0)
        put_chunks(acc, p_out.at[mb], first_id, last_id, seqs)
        if mb == 0:
            sums[mb].scatter()
    for i, (src, dst) in enumerate(((a1, a1_o), (ks, ks_o), (vv, vv_o), (fk, fk_o))):
        emit(src, dst, o_sem.at[i])
    fk_out = outs.pop()
    pieces[3].forward()
    pieces[3].finish()
    sums[0].spread(sums[0].reduce())

    def queries(t, carry):
        r = rows_at(t, TILE)
        q = (dot(a1[r, :], wq[...]) * factor).astype(BF16)
        qs[r, :] = q
        features(q, rbd, fq.at[r, :], feats)
        return carry

    def queries_and_sums(t, carry):
        @pl.when(t == SCATTER_AT)
        def _():
            for other in sums[1:]:
                other.scatter()

        return queries(t, carry)

    lax.fori_loop(0, micro * tiles, queries_and_sums, 0)
    for piece in pieces[4:6]:
        piece.forward()
    for piece in pieces[4:6]:
        piece.finish()

    dy_load.wait()
    fk_out.wait()
    dh = fk

    def hidden_grads(t, carry):
        r = rows_at(t, TILE)
        dy = dy_ref[r, :]
        for j in range(wd.shape[0] // 256):
            js = slice(256 * j, 256 * j + 256)
            dh[r, js] = dot_nt(dy, wd[js, :]).astype(BF16)
        return carry

    lax.fori_loop(0, micro * tiles, hidden_grads, 0)
    for i, (src, dst) in enumerate(((wq, wq_o), (wk, wk_o), (wv, wv_o))):
        emit(src, dst, o_sem.at[4 + i])
    tiled = ((t_out, out_o), (t_att, att_o), (t_a2, a2_o), (t_hid, hid_o), (t_dpre, dpre_o), (t_dmid, dmid_o), (t_dq, dq_o))

    def tile_copies(t, slot):
        r = rows_at(t, TILE)
        return [pltpu.make_async_copy(src.at[slot], dst.at[r, :], t_sem.at[slot, i]) for i, (src, dst) in enumerate(tiled)]

    for mb in range(micro):
        first_id, last_id = ident(mb)
        sums[mb].finish()
        build_b(p_full.at[mb], b_ref, first_id, last_id, seqs, True)
        acc[...] = jnp.zeros_like(acc)

        def attend(t, carry, mb=mb, last_id=last_id):
            r = rows_at(t + mb * tiles, TILE)
            own = rows_at(t, TILE)
            last = last_lanes(ids_of(mb, t), last_id)
            lane = lax.broadcasted_iota(jnp.int32, (TILE, 128), 1)
            sel = jnp.logical_xor(lane < 64, last)

            def swap(v):
                return jnp.where(last, pltpu.roll(v, 64, 1), v)

            for p in range(pairs):
                base = 2 * feats * p
                ps = slice(128 * p, 128 * p + 128)
                a = dot_nt(fq[r, base : base + feats], b_ref[2 * p])
                b = dot_nt(fq[r, base + feats : base + 2 * feats], b_ref[2 * p + 1])
                inv = 1.0 / jnp.where(sel, a[:, 128:], b[:, 128:])
                att_s[own, ps] = swap(jnp.where(sel, a[:, :128], b[:, :128]) * inv)
                inv_s[own, ps] = swap(inv)
            mix_s[own, :] = x_ref[r, :].astype(F32) + dot(att_s[own, :].astype(BF16), wo[...])
            return carry

        def mid(t, carry, mb=mb, last_id=last_id):
            g = t + mb * tiles
            slot = g % 2
            r = rows_at(g, TILE)

            @pl.when(g >= 2)
            def _():
                for c in tile_copies(g - 2, slot):
                    c.wait()

            if mb == 1:

                @pl.when(t == AR2_AT)
                def _():
                    sums[0].spread_settle()
                    sums[0].spread(sums[0].reduce())

            ids = ids_of(mb, t)
            last = last_lanes(ids, last_id)
            mask_t = mask_rows(ids, last_id)
            lane = lax.broadcasted_iota(jnp.int32, (TILE, 128), 1)
            sel = jnp.logical_xor(lane < 64, last)

            def swap(v):
                return jnp.where(last, pltpu.roll(v, 64, 1), v)

            own = rows_at(t, TILE)
            att, inv, mixed = att_s[own, :], inv_s[own, :], mix_s[own, :]
            t_att[slot] = att.astype(BF16)
            normed, rescale = norm_parts(mixed)
            a2 = (normed * g2).astype(BF16)
            t_a2[slot] = a2
            dy = dy_ref[r, :]
            for j in range(wu.shape[1] // 256):
                js = slice(256 * j, 256 * j + 256)
                pre = dot(a2, wu[:, js])
                cdf = 0.5 * (1.0 + lax.erf(pre * 0.7071067811865476))
                slope = cdf + pre * jnp.exp(-0.5 * pre * pre) * 0.3989422804014327
                t_hid[slot, :, js] = (pre * cdf).astype(BF16)
                t_dpre[slot, :, js] = (dh[r, js].astype(F32) * slope).astype(BF16)
            t_out[slot] = (mixed + dot(t_hid[slot], wd[...])).astype(BF16)
            da2 = dot_nt(t_dpre[slot], wu[...])
            gg_o[...] += jnp.sum(da2 * normed, axis=0, keepdims=True)
            dmid = dy.astype(F32) + norm_back(da2, normed, rescale, g2)
            dmid_low = dmid.astype(BF16)
            t_dmid[slot] = dmid_low
            dnum = dot_nt(dmid_low, wo[...]) * inv
            dpart = -dnum * att
            for p in range(pairs):
                ps = slice(128 * p, 128 * p + 128)
                d, q = dnum[:, ps], dpart[:, ps]
                ds, dp = swap(d), swap(q)
                la = jnp.concatenate([jnp.where(sel, ds, 0.0), jnp.where(sel, dp, 0.0)], axis=1).astype(BF16)
                lb = jnp.concatenate([jnp.where(sel, 0.0, ds), jnp.where(sel, 0.0, dp)], axis=1).astype(BF16)
                base = 2 * feats * p
                fa = fq[r, base : base + feats]
                fb = fq[r, base + feats : base + 2 * feats]
                ga = (dot(la, b_ref[2 * p]) * fa.astype(F32)).astype(BF16)
                gb = (dot(lb, b_ref[2 * p + 1]) * fb.astype(F32)).astype(BF16)
                o = dot(jnp.concatenate([ga, gb], axis=1), rt[p])
                t_dq[slot, :, ps] = (factor * (o[:, :128] - qs[r, ps].astype(F32) * o[:, 128:])).astype(BF16)
                dt = d.astype(BF16).T
                qt = q.T
                for k, f in enumerate((fa, fb)):
                    z = jnp.sum(qt[64 * k : 64 * k + 64], axis=0, keepdims=True)
                    lt = summary_rows(dt[64 * k : 64 * k + 64], z, mask_t)
                    acc[2 * p + k] += dot(lt, f)
            for c in tile_copies(g, slot):
                c.start()
            return carry

        lax.fori_loop(0, tiles, attend, 0)
        if mb == 0:
            for other in sums[1:]:
                other.spread(other.reduce())
            pieces[6].forward()
            pieces[6].finish()
        lax.fori_loop(0, tiles, mid, 0)
        if mb == 0:
            sums[0].scatter_settle()
            put_chunks(acc, p_out.at[0], first_id, last_id, seqs)
            sums[0].scatter()
        else:
            put_chunks(acc, p_o.at[mb - 1], first_id, last_id, seqs)
    sums[0].finish()
    emit(p_full.at[0], s_o, o_sem.at[7])
    last_tile = micro * tiles - 1
    for g in (last_tile - 1, last_tile):
        for c in tile_copies(g, g % 2):
            c.wait()
    for c in outs:
        c.wait()
    for one in sums:
        one.scatter_settle()
        one.spread_settle()
    ex.drain()


def front(x, dy, ids, rand, g1, g2, wk, wv, wq, wo, wu, wd, *, micro, seqs, nf, ns, factor):
    total, width = x.shape
    heads, _, feats = rand.shape
    hidden = wu.shape[1]
    rows = 128 + PAD
    chunks = heads * (seqs // 2)

    def bf(*shape):
        return jax.ShapeDtypeStruct(shape, BF16)

    hbm = pl.BlockSpec(memory_space=pl.ANY)
    vmem = pl.BlockSpec(memory_space=pltpu.VMEM)
    out_shape = [
        bf(total, width), bf(total, width), bf(total, width), bf(total, hidden), bf(total, hidden), bf(total, width),
        bf(total, width), bf(total, width), bf(total, width), bf(total, width), bf(total, heads * feats),
        bf(width, width), bf(width, width), bf(width, width), bf(micro - 1, chunks, rows, feats), bf(ns, rows, feats),
        bf(PAD, width), jax.ShapeDtypeStruct((1, width), F32),
    ]
    v = pltpu.VMEM
    dma = pltpu.SemaphoreType.DMA
    scratch = [v((total, width), BF16)] * 5 + [v((total, heads * feats), BF16), v((total, width), BF16), v((total, heads * feats), BF16)]
    scratch += [v((2, TILE, width), BF16)] * 3 + [v((2, TILE, hidden), BF16)] * 2 + [v((2, TILE, width), BF16)] * 2
    scratch += [v((total // micro, width), F32)] * 3
    scratch += [v((PAD, width), BF16), v((nf * PAD, width), BF16)] + [v((width, width), BF16)] * 4 + [v((width, hidden), BF16), v((hidden, width), BF16)]
    scratch += [v((heads // 4, 256, 4 * feats), BF16), v((heads // 2, 2 * feats, 256), BF16), v((heads, 256, feats), BF16)]
    scratch += [v((heads, rows, feats), F32), v((micro, chunks, rows, feats), BF16)]
    scratch += [v((micro, ns, rows, feats), BF16), v((micro, ns, rows, feats), BF16)]
    kinds = nf - 1
    scratch += [dma((7, kinds)), dma((7, kinds)), dma((7,))] + [dma((micro, ns))] * 4 + [dma((10,)), dma((2, 7))]
    return pl.pallas_call(
        functools.partial(front_kernel, micro=micro, seqs=seqs, factor=factor),
        in_specs=[hbm] * 2 + [vmem] * 4 + [hbm] * 6,
        out_specs=[hbm] * 14 + [vmem, hbm, vmem, vmem],
        out_shape=out_shape,
        scratch_shapes=scratch,
        compiler_params=pltpu.CompilerParams(collective_id=0, has_side_effects=True, vmem_limit_bytes=63 << 20),
        name="front",
    )(x, dy, ids, rand, g1, g2, wk, wv, wq, wo, wu, wd)


class SeqSum:
    def __init__(self, ex, refs, send, recv):
        self.ex, self.send, self.recv = ex, send, recv
        self.out, self.got1, self.mid, self.got2, self.full = refs
        self.fast = ex.ns // 4
        self.z, self.x = ex.s // self.fast, ex.s % self.fast

    def copy(self, phase, k, src, dst, z, x):
        return self.ex.copy(src, dst, self.send.at[phase, k - 1], self.recv.at[phase, k - 1], (z * self.fast + x, self.ex.f))

    def fast_copy(self, phase, k, src, dst):
        return self.copy(phase, k, src, dst, self.z, (self.x + k) % self.fast)

    def slow_copy(self, phase, k, src, dst):
        return self.copy(phase, k, src, dst, (self.z + k) % 4, self.x)

    def block(self, x):
        return pl.ds(x * 4, 4)

    def send1(self):
        for k in range(1, self.fast):

            def make(k=k):
                src = self.out.at[self.block((self.x + k) % self.fast)]
                return self.fast_copy(0, k, src, self.got1.at[k - 1])

            self.ex.launch(make)

    def sum1(self):
        for k in range(1, self.fast):
            self.fast_copy(0, k, self.got1.at[k - 1], self.got1.at[k - 1]).wait_recv()
        total = self.out[self.block(self.x)].astype(F32)
        for k in range(1, self.fast):
            total = total + self.got1[k - 1].astype(F32)
        self.mid[...] = total.astype(BF16)
        for k in (2, 1, 3):
            self.ex.launch(lambda k=k: self.slow_copy(1, k, self.mid.at[(self.z + k) % 4], self.got2.at[k - 1]))

    def sum2(self):
        for k in range(1, 4):
            self.slow_copy(1, k, self.got2.at[k - 1], self.got2.at[k - 1]).wait_recv()
        total = self.mid[self.z].astype(F32)
        for k in range(1, 4):
            total = total + self.got2[k - 1].astype(F32)
        self.full[self.x * 4 + self.z] = total.astype(BF16)
        for k in (2, 1, 3):

            def make(k=k):
                mine = self.full.at[self.x * 4 + self.z]
                return self.slow_copy(2, k, mine, mine)

            self.ex.launch(make)

    def send_fast(self):
        for k in range(1, 4):
            part = self.full.at[self.x * 4 + (self.z + 4 - k) % 4]
            self.slow_copy(2, k, part, part).wait_recv()
        for k in range(1, self.fast):

            def make(k=k):
                mine = self.full.at[self.block(self.x)]
                return self.fast_copy(3, k, mine, mine)

            self.ex.launch(make)

    def finish(self):
        for k in range(1, self.fast):
            part = self.full.at[self.block((self.x + self.fast - k) % self.fast)]
            self.fast_copy(3, k, part, part).wait_recv()


class Reduce:
    def __init__(self, ex, part, rc, ry, seq, send, recv):
        self.ex, self.part, self.rc, self.ry, self.seq, self.send, self.recv = ex, part, rc, ry, seq, send, recv
        self.steps = iter([self.core_sum, self.y_sum, seq.sum1, seq.sum2, seq.send_fast, seq.finish])

    def core_copy(self, yy):
        ex = self.ex
        f = yy * 2 + (1 - ex.c)
        return ex.copy(self.part.at[f], self.rc.at[yy], self.send.at[yy], self.recv.at[yy], (ex.s, ex.partner))

    def core_send(self):
        for yy in range(self.ex.ny):
            self.ex.launch(lambda yy=yy: self.core_copy(yy))

    def y_copy(self, k):
        ex = self.ex
        f = ex.y_to(k)
        j = ex.ny + k - 1
        return ex.copy(self.part.at[f], self.ry.at[k - 1], self.send.at[j], self.recv.at[j], (ex.s, f))

    def core_sum(self):
        ex = self.ex
        for k in range(1, ex.ny):
            yy = (ex.y + k) % ex.ny
            f = ex.y_to(k)
            self.core_copy(yy).wait_recv()
            self.part[f] = (self.part[f].astype(F32) + self.rc[yy].astype(F32)).astype(BF16)
            ex.launch(lambda k=k: self.y_copy(k))

    def y_sum(self):
        ex = self.ex
        self.core_copy(ex.y).wait_recv()
        total = self.part[ex.f].astype(F32) + self.rc[ex.y].astype(F32)
        for k in range(1, ex.ny):
            self.y_copy(k).wait_recv()
            total = total + self.ry[k - 1].astype(F32)
        self.seq.out[...] = total.astype(BF16)
        self.seq.send1()


PIECES = 6


def back_kernel(
    x_in, dy_in, hid_in, dpre_in, a2_in, att_in, dmid_in, dq_in, a1_in, ks_in, vv_in, fk_in, wq_in, wk_in, wv_in,
    ids_ref, rand_ref, gain_ref, gg_ref, p0_ref, p1_ref,
    dx_o, g1_o, g2_o, res_o,
    x, dy, blk, a2, att, dmid, dq, a1, ks, vv, fk, wq, wk, wv, dk, dv, tr, t_dx, rbd, rt, b_ref,
    p_got, p_full, part, rc, ry, s_out, s_got1, s_mid, s_got2,
    gs, gr,
    l_sem, b_sem, x_sem, r_send, r_recv, g_send, g_recv, c_send, c_recv, t_send, t_recv, n_send, n_recv,
    *, micro, seqs, factor,
):
    ex = Exchange()
    heads, _, feats = rand_ref.shape
    total_rows, width = x.shape
    toks = total_rows // micro
    tiles = toks // TILE
    pairs = width // 128
    hidden = hid_in.shape[1]
    blocks = hidden // 512
    quarter = ex.ns // 4
    chunk = res_o.shape[2]
    shard = quarter * chunk
    kv_sum = Sum(ex, p1_ref, p_got, p_full, (r_send, r_recv, g_send, g_recv), seqs)

    ex.greet()
    loads = {}
    order = (
        ("att", att_in, att), ("dmid", dmid_in, dmid), ("a1", a1_in, a1), ("dq", dq_in, dq), ("dy", dy_in, dy), ("a2", a2_in, a2),
        ("vv", vv_in, vv), ("fk", fk_in, fk), ("ks", ks_in, ks), ("wq", wq_in, wq), ("wk", wk_in, wk), ("wv", wv_in, wv),
        ("x", x_in, x),
    )

    def block_copy(src, b):
        return pltpu.make_async_copy(src.at[:, pl.ds(pl.multiple_of(b * 512, 512), 512)], blk.at[b], b_sem.at[b])

    for i, (name, src, dst) in enumerate(order):
        loads[name] = pltpu.make_async_copy(src, dst, l_sem.at[i])
        loads[name].start()
        if name == "dy":
            for b in range(blocks):
                block_copy(hid_in, b).start()

    def need(*names):
        for name in names:
            loads.pop(name).wait()

    pieces = []
    for i in range(PIECES):
        seq = SeqSum(ex, (s_out.at[i], s_got1.at[i], s_mid.at[i], s_got2.at[i], res_o.at[i]), t_send.at[i], t_recv.at[i])
        pieces.append(Reduce(ex, part.at[i], rc.at[i], ry.at[i], seq, c_send.at[i], c_recv.at[i]))
    q, d1, d2, u1, u2, k = pieces

    def go(*which):
        for one in which:
            next(one.steps)()

    def go_at(t, plan):
        for when, which in plan.items():

            @pl.when(t == when)
            def _(which=which):
                go(*which)

    def small(left_t, right, piece, which):
        v = dot(left_t, right)
        for half in range(2):
            for f in range(ex.nf):
                one = v[f * shard : (f + 1) * shard, 256 * half : 256 * half + 256].reshape(quarter, chunk, 256)
                piece.part[f, quarter * (2 * which + half) : quarter * (2 * which + half + 1)] = one.astype(BF16)

    need("att", "dmid")
    small(att[...].T, dmid[...], q, 1)
    ex.meet()
    kv_sum.scatter()
    need("a1", "dq")
    small(a1[...].T, dq[...], q, 0)
    q.core_send()
    need("dy")
    tr[...] = dy[...].T
    per = 512 // chunk // ex.ns

    def down_block(i, carry):
        b = (i + (ex.y + 1) % ex.ny * (blocks // ex.ny)) % blocks
        block_copy(hid_in, b).wait()
        v = dot(tr[...], blk[b]).T
        block_copy(dpre_in, b).start()
        for half, piece in enumerate((d1, d2)):
            one = v[:, 256 * half : 256 * half + 256].reshape(512 // chunk, chunk, 256).astype(BF16)
            for j in range(per):
                f = b * per + j
                piece.part[f] = one[j * ex.ns : (j + 1) * ex.ns]

                @pl.when(f % 2 != ex.c)
                def _(f=f, piece=piece):
                    piece.core_copy(f // 2).start()

        go_at(i, {1: (q,)})
        return carry

    lax.fori_loop(0, blocks, down_block, 0)
    for piece in (d1, d2):
        ex.pending += [lambda yy=yy, piece=piece: piece.core_copy(yy) for yy in range(ex.ny)]
    kv_sum.spread(kv_sum.reduce())
    go(d1, d2)
    build_features(rand_ref, rbd, rt)
    need("a2")
    tr[...] = a2[...].T

    def up_block(b, carry):
        block_copy(dpre_in, b).wait()
        v = dot(tr[...], blk[b])
        for half in range(2):
            for f in range(ex.nf):
                one = v[f * shard : (f + 1) * shard, 256 * half : 256 * half + 256].reshape(quarter, chunk, 256)
                part[3 + b // 2, f, pl.ds((b % 2 * 2 + half) * quarter, quarter)] = one.astype(BF16)

        @pl.when(b == 1)
        def _():
            u1.core_send()

        go_at(b, {2: (q,), 3: (u1,)})
        return carry

    lax.fori_loop(0, blocks, up_block, 0)
    u2.core_send()
    tr[...] = a1[...].T
    need("vv", "fk", "ks")

    def ident(mb):
        if seqs == 2:
            return 0, 1
        return ids_ref[mb, :, 0:1], ids_ref[mb, :, toks - 1 : toks]

    def kv_part(mb, full, plan):
        first_id, last_id = ident(mb)
        build_b(full, b_ref, first_id, last_id, seqs, False)

        def body(t, carry):
            r = rows_at(t + mb * tiles, TILE)
            ids = ids_ref[mb, :, pl.ds(pl.multiple_of(t * TILE, TILE), TILE)]
            last = last_lanes(ids, last_id)
            lane = lax.broadcasted_iota(jnp.int32, (TILE, 128), 1)
            sel = jnp.logical_xor(lane < 64, last)
            ones_a = jnp.where(sel, 1.0, 0.0).astype(BF16)
            ones_b = jnp.where(sel, 0.0, 1.0).astype(BF16)

            def swap(v):
                return jnp.where(last, pltpu.roll(v, 64, 1), v)

            for p in range(pairs):
                ps = slice(128 * p, 128 * p + 128)
                v = swap(vv[r, ps].astype(F32))
                la = jnp.concatenate([jnp.where(sel, v, 0.0).astype(BF16), ones_a], axis=1)
                lb = jnp.concatenate([jnp.where(sel, 0.0, v).astype(BF16), ones_b], axis=1)
                base = 2 * feats * p
                fa = fk[r, base : base + feats]
                fb = fk[r, base + feats : base + 2 * feats]
                ga = (dot(la, b_ref[2 * p]) * fa.astype(F32)).astype(BF16)
                gb = (dot(lb, b_ref[2 * p + 1]) * fb.astype(F32)).astype(BF16)
                o = dot(jnp.concatenate([ga, gb], axis=1), rt[p])
                dk[r, ps] = (factor * (o[:, :128] - ks[r, ps].astype(F32) * o[:, 128:])).astype(BF16)
                va = dot_nt(fa, b_ref[2 * p, :128])
                vb = dot_nt(fb, b_ref[2 * p + 1, :128])
                dv[r, ps] = swap(jnp.where(sel, va, vb)).astype(BF16)
            go_at(t, plan)
            return carry

        lax.fori_loop(0, tiles, body, 0)

    g1 = gain_ref[0:1].astype(F32)
    gs[...] = jnp.zeros_like(gs)
    gs[0, 1:2, :] = gg_ref[...]

    def dx_copy(g, slot):
        return pltpu.make_async_copy(t_dx.at[slot], dx_o.at[rows_at(g, TILE), :], x_sem.at[slot])

    def x_part(mb, plan):
        def body(t, carry):
            g = t + mb * tiles
            slot = g % 2
            r = rows_at(g, TILE)

            @pl.when(g >= 2)
            def _():
                dx_copy(g - 2, slot).wait()

            da1 = dot_nt(dq[r, :], wq[...]) + dot_nt(dk[r, :], wk[...]) + dot_nt(dv[r, :], wv[...])
            normed, rescale = norm_parts(x[r, :].astype(F32))
            gs[0, 0:1, :] += jnp.sum(da1 * normed, axis=0, keepdims=True)
            t_dx[slot] = (dmid[r, :].astype(F32) + norm_back(da1, normed, rescale, g1)).astype(BF16)
            dx_copy(g, slot).start()
            go_at(t, plan)
            return carry

        lax.fori_loop(0, tiles, body, 0)

    kv_part(0, p0_ref, {0: (u2,), 1: (d1, q), 2: ()})
    kv_sum.finish()
    kv_part(1, p_full, {1: (d1, d2, q)})
    small(tr[...], dk[...], k, 0)
    small(tr[...], dv[...], k, 1)
    k.core_send()
    go(u1, d2, d1)
    need("wq", "wk", "wv", "x")
    x_part(0, {1: (k, q), 2: (u1, u2)})
    x_part(1, {0: (d2,), 2: (q, d1)})
    def gain_copy(level, j, peer):
        return ex.copy(gs.at[level], gr.at[j], n_send.at[j], n_recv.at[j], peer)

    def gain_level(level, jobs):
        for j, peer in jobs:
            gain_copy(level, j, peer).start()
        return jobs

    def gain_sum(level, jobs):
        total = gs[level]
        for j, peer in jobs:
            gain_copy(level, j, peer).wait_recv()
            total = total + gr[j]
        return total

    jobs0 = gain_level(0, [(0, (ex.s, ex.partner))])
    go(k, u2, u1)
    gs[1] = gain_sum(0, jobs0)
    jobs1 = gain_level(1, [(k, (ex.s, ex.y_to(k))) for k in range(1, ex.ny)])
    go(d1, d2, k, u2)
    gs[2] = gain_sum(1, jobs1)
    jobs2 = gain_level(2, [(ex.ny - 1 + k, ex.seq_peer(k)) for k in range(1, ex.ns)])
    go(d2, u1, k, u1, u2)
    gains = gain_sum(2, jobs2)
    mine = jnp.zeros((gains.shape[0], shard), F32)
    for f in range(ex.nf):
        mine = mine + jnp.where(ex.f == f, gains[:, f * shard : f * shard + shard], 0.0)
    g1_o[...] = mine[0:1]
    g2_o[...] = mine[1:2]
    go(k, u2, k)
    for piece in pieces:
        assert next(piece.steps, None) is None
    last = micro * tiles - 1
    for g in (last - 1, last):
        dx_copy(g, g % 2).wait()
    for level, jobs in enumerate((jobs0, jobs1, jobs2)):
        for j, peer in jobs:
            gain_copy(level, j, peer).wait_send()
    kv_sum.scatter_settle()
    kv_sum.spread_settle()
    ex.drain()


def back(big, small, *, micro, seqs, nf, ns, shard, factor):
    x, _, hid = big[:3]
    rand = small[1]
    total, width = x.shape
    heads, _, feats = rand.shape
    rows = 128 + PAD
    hidden = hid.shape[1]
    ny = nf // 2
    slow = 4
    fast = ns // slow
    chunk = 4 * shard // ns
    hbm = pl.BlockSpec(memory_space=pl.ANY)
    vmem = pl.BlockSpec(memory_space=pltpu.VMEM)
    v = pltpu.VMEM
    dma = pltpu.SemaphoreType.DMA

    def f32(*shape):
        return jax.ShapeDtypeStruct(shape, F32)

    out_shape = [jax.ShapeDtypeStruct((total, width), BF16), f32(1, shard), f32(1, shard)]
    out_shape += [jax.ShapeDtypeStruct((PIECES, ns, chunk, 256), BF16)]
    token = v((total, width), BF16)
    scratch = [token, token, v((hidden // 512, total, 512), BF16), token, token, token, token, token, token, token]
    scratch += [v((total, heads * feats), BF16)] + [v((width, width), BF16)] * 3 + [token, token, v((width, total), BF16)]
    scratch += [v((2, TILE, width), BF16), v((heads // 4, 256, 4 * feats), BF16), v((heads // 2, 2 * feats, 256), BF16)]
    scratch += [v((heads, 256, feats), BF16), v((ns, rows, feats), BF16), v((ns, rows, feats), BF16)]
    for lead in ((nf, ns), (ny, ns), (ny - 1, ns), (ns,), (fast - 1, slow), (slow,), (slow - 1,)):
        scratch.append(v((PIECES, *lead, chunk, 256), BF16))
    jobs = 1 + (ny - 1) + (ns - 1)
    scratch += [v((3, 8, width), F32), v((jobs, 8, width), F32)]
    peers = max(fast, slow) - 1
    scratch += [dma((13,)), dma((hidden // 512,)), dma((2,)), *([dma((ns,))] * 4)]
    scratch += [dma((PIECES, 2 * ny - 1))] * 2 + [dma((PIECES, 4, peers))] * 2 + [dma((jobs,))] * 2
    return pl.pallas_call(
        functools.partial(back_kernel, micro=micro, seqs=seqs, factor=factor),
        in_specs=[hbm] * len(big) + [vmem] * len(small),
        out_specs=[hbm] + [vmem] * 3,
        out_shape=out_shape,
        scratch_shapes=scratch,
        compiler_params=pltpu.CompilerParams(collective_id=1, has_side_effects=True, vmem_limit_bytes=63 << 20),
        name="back",
    )(*big, *small)


def results_kernel(out, dx, q, d1, d2, u1, u2, k, g1, g2, out_o, dx_o, wq, wo, wk, wv, wu, wd, g1_o, g2_o):
    out_o[...] = out[...]
    dx_o[...] = dx[...]
    g1_o[...] = g1[...]
    g2_o[...] = g2[...]

    def wide(a):
        a = a.astype(F32)
        return a.reshape(a.shape[0] * a.shape[1], a.shape[2])

    wd[:, :256] = wide(d1[...])
    wd[:, 256:] = wide(d2[...])
    step = pl.program_id(0)

    def up(piece):
        half = piece.shape[0] // 2
        wu[:, :256] = wide(piece[:half])
        wu[:, 256:] = wide(piece[half:])

    @pl.when(step < 2)
    def _():
        wq[...] = wide(q[...])
        wk[...] = wide(k[...])
        up(u1)

    @pl.when(step >= 2)
    def _():
        wo[...] = wide(q[...])
        wv[...] = wide(k[...])
        up(u2)


def results(out, dx, res, g1, g2, shard):
    total, width = out.shape
    _, ns, chunk, cols = res.shape
    quarter = ns // 4
    rows = pl.BlockSpec((total // 4, width), lambda i: (i, 0))
    gain = pl.BlockSpec((1, shard), lambda i: (0, 0))

    def piece(g):
        return pl.BlockSpec((None, quarter, chunk, cols), lambda i: (g, i, 0, 0))

    def low(i):
        return jnp.minimum(i, 1)

    def high(i):
        return jnp.maximum(i - 2, 0)

    def wider(g, of):
        return pl.BlockSpec((None, 2 * quarter, chunk, cols), lambda i: (g, of(i), 0, 0))

    first = pl.BlockSpec((shard, cols), lambda i: (0, low(i)))
    second = pl.BlockSpec((shard, cols), lambda i: (0, high(i)))
    half = jax.ShapeDtypeStruct((shard, 2 * cols), F32)
    token = jax.ShapeDtypeStruct((total, width), BF16)
    gain_shape = jax.ShapeDtypeStruct((1, shard), F32)
    return pl.pallas_call(
        results_kernel,
        grid=(4,),
        in_specs=[rows, rows, piece(0), piece(1), piece(2), wider(3, low), wider(4, high), piece(5), gain, gain],
        out_specs=[rows, rows, first, second, first, second]
        + [pl.BlockSpec((shard, 2 * cols), lambda i: (0, i)), pl.BlockSpec((shard, 2 * cols), lambda i: (i, 0)), gain, gain],
        out_shape=[token, token, half, half, half, half]
        + [jax.ShapeDtypeStruct((shard, 8 * cols), F32), jax.ShapeDtypeStruct((4 * shard, 2 * cols), F32), gain_shape, gain_shape],
        name="results",
    )(out, dx, res, res, res, res, res, res, g1, g2)


def per_device(block_input, seq_ids, rand, ln1_gain, w_query, w_key, w_value, w_out, ln2_gain, w_up, w_down, cotangent):
    micro, _, toks, width = block_input.shape
    heads, dim, feats = rand.shape
    factor = dim ** (-0.25)
    ns, nf = lax.axis_size("seq"), lax.axis_size("fsdp")
    seqs = max(2, ns // 4)
    x = block_input.reshape(micro * toks, width)
    dy = cotangent.reshape(micro * toks, width)
    shard = ln1_gain.shape[0]
    out, att, a2, hid, dpre, dmid, dq, a1, ks, vv, fk, wq, wk, wv, part, total, gains, gg = front(
        x, dy, seq_ids, rand, ln1_gain.reshape(1, shard), ln2_gain.reshape(1, shard), w_key, w_value, w_query, w_out, w_up, w_down,
        micro=micro, seqs=seqs, nf=nf, ns=ns, factor=factor,
    )
    dx, g1g, g2g, res = back(
        [x, dy, hid, dpre, a2, att, dmid, dq, a1, ks, vv, fk, wq, wk, wv],
        [seq_ids, rand, gains, gg, total, part[0]],
        micro=micro, seqs=seqs, nf=nf, ns=ns, shard=shard, factor=factor,
    )
    shape = block_input.shape
    out, dx, wqg, wog, wkg, wvg, wug, wdg, g1g, g2g = results(out, dx, res, g1g, g2g, shard)
    return (out.reshape(shape), dx.reshape(shape), g1g[0], wqg, wkg, wvg, wog, g2g[0], wug, wdg)


def solution(mesh):
    tok = P(None, "fsdp", "seq", None)
    vec, mat = P("fsdp"), P("fsdp", None)
    return jax.shard_map(
        per_device,
        mesh=mesh,
        in_specs=(tok, P(None, "fsdp", "seq"), P(), vec, mat, mat, mat, mat, vec, mat, mat, tok),
        out_specs=(tok, tok, vec, mat, mat, mat, mat, vec, mat, mat),
        check_vma=False,
    )
```
